256 devices in a mesh: mem: 8 (over z), space: 32 (over x, y, core).
Axes of the slice: x: 4, y: 4, z: 8, core: 2. Of those that a mesh axis runs over, the one named last changes fastest.
Arguments:
- ensemble: float32 [256, 64, 2048], P('mem', 'space'), may hold values from -6 to 6
- forcing: float32 [64, 2048], P('space'), may hold values from 2 to 8
- obs_cell: int32 [4096], P('space'), may hold values from 0 to 131071, as said below
- obs_value: float32 [4096], P('space'), may hold values from -8 to 8
- obs_var: float32 [4096], P('space'), may hold values from 0.5 to 2
- obs_noise: float32 [256, 4096], P('mem', 'space'), may hold values from -5 to 5
Outputs:
- analysis: float32 [256, 64, 2048], P('mem', 'space')
The draws below stay inside these ranges and needn't reach their ends.
Inputs may be any that keep to these rules, and one draw needn't show every extreme that they name: `obs_cell`: entries 128 * s to 128 * (s + 1) - 1 name cells of planes 2 * s to 2 * (s + 1) - 1, a cell of plane x and position p having index x * 2048 + p.
All inputs are finite; a program needn't handle non-finite values.
Results may differ from the reference program's by a relative error of at most 0.00018.
Values sent between devices are 32-bit elements; how exact they have to be, the bound alone decides.
A program may use at most 64 MiB of HBM per device.

```python
import math
import jax
import jax.numpy as jnp
from jax import lax

PLANES_DEV = 2
PLANE = 2048
OBS_DEV = 128
FSTEPS = 4
ITERS = 6
MEMBERS = 256
NX = 64
NOBS = 4096
LOC = 16


def draw_obs_cell(key, part):
    blocks = NOBS // OBS_DEV
    slab_cells = PLANES_DEV * PLANE
    local_cells = jax.random.randint(key, (blocks, OBS_DEV), 0, slab_cells)
    starts = slab_cells * jnp.arange(blocks, dtype=jnp.int32)[:, None]
    return (local_cells + starts).reshape(NOBS).astype(jnp.int32)


def level_of(stream_key, dims, cuts, least, largest):
    factor_of = 1.0
    for dim, blocks in cuts:
        draws = jax.random.uniform(jax.random.fold_in(jax.random.fold_in(stream_key, 6), dim), (blocks,), jnp.float32, least / len(cuts), largest / len(cuts))
        factor_of = factor_of * jnp.repeat(jnp.exp(draws), dims[dim] // blocks).reshape((-1,) + (1,) * (len(dims) - 1 - dim))
    return factor_of


def scatter_about(key, dims, deviation, limit, cuts=(), held_as=jnp.bfloat16):
    entries = deviation * jax.random.normal(key, dims, jnp.float32)
    if cuts:
        entries = entries * level_of(key, dims, cuts, -0.22, 0.18)
    return jnp.clip(entries, -limit, limit).astype(held_as)


def setup_inputs(seed: int = 0) -> dict:
    keys = jax.random.split(jax.random.key(seed), 7)
    return {
        "ensemble": scatter_about(keys[0], (MEMBERS, NX, PLANE), 1.0, 6.0, ((0, 8), (1, 32)), jnp.float32),
        "forcing": jnp.clip(2.0 + 6.0 * jax.random.uniform(keys[1], (NX, PLANE), jnp.float32) ** level_of(keys[1], (NX, PLANE), ((0, 32),), -0.2, 0.2), 2.0, 8.0),
        "obs_cell": draw_obs_cell(jax.random.fold_in(keys[6], 71), 0),
        "obs_value": scatter_about(keys[3], (NOBS,), 2.0, 8.0, ((0, 32),), jnp.float32),
        "obs_var": jnp.clip(jnp.exp(math.log(2.0) - 1.3862944 * jax.random.uniform(keys[4], (NOBS,), jnp.float32) ** level_of(keys[4], (NOBS,), ((0, 32),), -0.2, 0.2)), 0.5, 2.0),
        "obs_noise": scatter_about(keys[5], (MEMBERS, NOBS), 1.0, 5.0, ((0, 8), (1, 32)), jnp.float32),
    }


time_step = 0.05
highest = lax.Precision.HIGHEST

def advance(states, forcing):
    forward_one = jnp.roll(states, -1, axis=1)
    back_one = jnp.roll(states, 1, axis=1)
    back_two = jnp.roll(states, 2, axis=1)
    return states + time_step * ((forward_one - back_two) * back_one - states + forcing)

def taper_of(planes_a, planes_b):
    spread = jnp.abs(planes_a[:, None] - planes_b[None, :])
    spread = jnp.minimum(spread, NX - spread)
    return jnp.maximum(0.0, 1.0 - spread.astype(jnp.float32) / LOC)

def chebyshev(covariance, rhs, lower_bound, upper_bound):
    center = (upper_bound + lower_bound) / 2.0
    radius = (upper_bound - lower_bound) / 2.0
    sigma_ratio = center / radius
    rho_now = 1.0 / sigma_ratio
    residual = rhs
    direction = rhs / center
    solution = jnp.zeros_like(rhs)
    for iteration in range(ITERS):
        solution = solution + direction
        if iteration < ITERS - 1:
            residual = residual - jnp.dot(covariance, direction, precision=highest)
            rho_next = 1.0 / (2.0 * sigma_ratio - rho_now)
            direction = rho_next * rho_now * direction + 2.0 * rho_next / radius * residual
            rho_now = rho_next
    return solution

def reference(ensemble, forcing, obs_cell, obs_value, obs_var, obs_noise):
    states = ensemble
    for counter in range(FSTEPS):
        states = advance(states, forcing)
    flattened = states.reshape(MEMBERS, NX * PLANE)
    observed = jnp.take(flattened, obs_cell, axis=1)
    obs_mean = lax.optimization_barrier(jnp.sum(observed, axis=0)) / MEMBERS
    obs_anom = observed - obs_mean
    obs_planes = (obs_cell // PLANE).astype(jnp.int32)
    taper_block = taper_of(obs_planes, obs_planes)
    gram_block = jnp.dot(obs_anom.T, obs_anom, precision=highest) / (MEMBERS - 1)
    covariance = taper_block * gram_block + jnp.diag(obs_var)
    lower_bound = jnp.min(obs_var)
    upper_bound = jnp.max(lax.optimization_barrier(jnp.sum(jnp.abs(covariance), axis=1)))
    mean_weight = chebyshev(covariance, obs_value - obs_mean, lower_bound, upper_bound)
    anom_rhs = (jnp.sqrt(obs_var)[None, :] * obs_noise - obs_anom).T
    anom_weight = chebyshev(covariance, anom_rhs, lower_bound, upper_bound)
    weight = anom_weight + mean_weight[:, None]
    state_mean = lax.optimization_barrier(jnp.sum(states, axis=0)) / MEMBERS
    state_anom = states - state_mean
    plane_taper = taper_of(jnp.arange(NX, dtype=jnp.int32), obs_planes)

    def plane_gain(taper_row):
        return jnp.dot(obs_anom * taper_row[None, :], weight, precision=highest)
    gain_blocks = lax.map(plane_gain, plane_taper)
    update = jnp.einsum('jxp,xjk->kxp', state_anom, gain_blocks, precision=highest) / (MEMBERS - 1)
    return states + update
```

```python
import jax
import jax.numpy as jnp
from jax import lax
from jax.experimental import pallas as pl
from jax.experimental.pallas import tpu as pltpu
from jax.sharding import PartitionSpec as P

FSTEPS = 4
ITERS = 6
LOC = 16
REACH = 8
SLOTS = 2 * REACH + 1
MESH = pl.DeviceIdType.MESH
f32 = jnp.float32
bf16 = jnp.bfloat16

R_OUT, R_FORC, R_BACK, R_OBS, R_RHS, R_BAND, R_BOUND = range(7)
R_DIR = 7
R_RIGHT = 12
R_LEFT = 16
RECVS = 20
S_OUT, S_FORC, S_BACK, S_OBS, S_RHS, S_BAND, S_BOUND = range(7)
S_DIR = 7
S_RIGHT = 12
S_LEFT = 16
SENDS = 20

NT = (((1,), (1,)), ((), ()))


def nn(a, b):
    return jnp.dot(a, b, preferred_element_type=f32)


def nt(a, b):
    return lax.dot_general(a, b, NT, preferred_element_type=f32)


def halves(x):
    high = x.astype(bf16)
    return high, (x - high.astype(f32)).astype(bf16)


def awaited(ref, sem):
    pltpu.make_async_copy(ref, ref, sem).wait()


def kernel(
    space_count, mem_count,
    ens, forc, cell, value, var, noise, plane,
    out,
    r, t, fr, zs, oh, ao, ab, ah, al, e0, ex, bb, ch, cl, dh,
    ssem, rsem, lsem,
):
    me_s = lax.axis_index("space")
    me_m = lax.axis_index("mem")
    members = ao.shape[0]
    mdev = noise.shape[0]
    planes = r.shape[0]
    half = mdev // 2
    odev = cell.shape[1]
    slab = ens.shape[2]

    def chunk_of(index):
        return lax.div(index, 2), lax.rem(index, 2)

    def other(base, step, count):
        return lax.rem(base + step, count)

    barrier = pltpu.get_barrier_semaphore()

    def greet_space(i, c):
        pl.semaphore_signal(barrier, inc=1, device_id={"space": other(me_s, i, space_count)}, device_id_type=MESH)
        return c

    def greet_mem(i, c):
        pl.semaphore_signal(barrier, inc=1, device_id={"mem": other(me_m, i, mem_count)}, device_id_type=MESH)
        return c

    lax.fori_loop(1, space_count, greet_space, 0)
    lax.fori_loop(1, mem_count, greet_mem, 0)

    my_c, my_h = chunk_of(me_s)
    own_out = pltpu.make_async_copy(
        ens.at[:, pl.ds(pl.multiple_of(my_h * half, half), half), pl.ds(pl.multiple_of(my_c * 128, 128), 128)],
        r.at[pl.ds(me_s * 2, 2)], lsem.at[0])
    own_forc = pltpu.make_async_copy(
        forc.at[:, pl.ds(pl.multiple_of(my_c * 128, 128), 128)], fr.at[me_s], lsem.at[1])
    own_out.start()
    own_forc.start()

    pl.semaphore_wait(barrier, space_count + mem_count - 2)

    def send_out(i, c):
        to = other(me_s, i, space_count)
        tc, th = chunk_of(to)
        cells = pl.ds(pl.multiple_of(tc * 128, 128), 128)
        pltpu.make_async_remote_copy(
            src_ref=forc.at[:, cells], dst_ref=fr.at[me_s],
            send_sem=ssem.at[S_FORC], recv_sem=rsem.at[R_FORC],
            device_id={"space": to}, device_id_type=MESH).start()
        pltpu.make_async_remote_copy(
            src_ref=ens.at[:, pl.ds(pl.multiple_of(th * half, half), half), cells],
            dst_ref=r.at[pl.ds(me_s * 2, 2)],
            send_sem=ssem.at[S_OUT], recv_sem=rsem.at[R_OUT],
            device_id={"space": to}, device_id_type=MESH).start()
        return c

    lax.fori_loop(1, space_count, send_out, 0)

    cells_here = cell[...]

    def one_hot(i, c):
        rows = lax.broadcasted_iota(jnp.int32, (256, odev), 0) + i * 256
        oh[pl.ds(pl.multiple_of(i * 256, 256), 256), :] = jnp.where(rows == cells_here, 1.0, 0.0).astype(bf16)
        return c

    lax.fori_loop(0, 2 * slab // 256, one_hot, 0)

    own_out.wait()
    own_forc.wait()
    awaited(r.at[pl.ds(0, planes - 2)], rsem.at[R_OUT])
    awaited(fr.at[pl.ds(0, space_count - 1)], rsem.at[R_FORC])

    def advance(src, dst):
        def group(g, carry):
            two, one, now = carry
            for i in range(8):
                x = g * 8 + i
                ahead = src[lax.rem(x + 1, planes)]
                force = fr[g * 4 + i // 2, pl.ds(i % 2, 1), :]
                dst[x] = now + 0.05 * ((ahead - two) * one - now + force)
                two, one, now = one, now, ahead
            return two, one, now

        lax.fori_loop(0, planes // 8, group, (src[planes - 2], src[planes - 1], src[0]))

    for step in range(FSTEPS // 2):
        advance(r, t)
        advance(t, r)

    mine = pl.ds(pl.multiple_of(me_m * mdev, mdev), mdev)
    my_rows = pl.ds(pl.multiple_of(me_m * mdev + my_h * half, half), half)
    my_cells = pl.ds(pl.multiple_of(my_c * 128, 128), 128)

    def send_back(i, c):
        to = other(me_s, i, space_count)
        pltpu.make_async_remote_copy(
            src_ref=r.at[pl.ds(to * 2, 2)], dst_ref=zs.at[:, my_rows, my_cells],
            send_sem=ssem.at[S_BACK], recv_sem=rsem.at[R_BACK],
            device_id={"space": to}, device_id_type=MESH).start()
        return c

    lax.fori_loop(1, space_count, send_back, 0)
    own_back = pltpu.make_async_copy(r.at[pl.ds(me_s * 2, 2)], zs.at[:, my_rows, my_cells], lsem.at[2])
    own_back.start()
    own_back.wait()
    awaited(r.at[pl.ds(0, planes - 2)], rsem.at[R_BACK])

    observed = jnp.zeros((3 * mdev, odev), f32)
    for x in range(2):
        block = zs[x, mine, :]
        first = block.astype(bf16)
        rest = block - first.astype(f32)
        second = rest.astype(bf16)
        third = (rest - second.astype(f32)).astype(bf16)
        pieces = jnp.concatenate([first, second, third], axis=0)
        observed = observed + nn(pieces, oh[x * slab:(x + 1) * slab, :])
    observed = observed[:mdev] + observed[mdev:2 * mdev] + observed[2 * mdev:]
    ao[mine, :] = observed

    def send_obs(i, c):
        pltpu.make_async_remote_copy(
            src_ref=ao.at[mine], dst_ref=ao.at[mine],
            send_sem=ssem.at[S_OBS], recv_sem=rsem.at[R_OBS],
            device_id={"mem": other(me_m, i, mem_count)}, device_id_type=MESH).start()
        return c

    lax.fori_loop(1, mem_count, send_obs, 0)

    plane_row = plane[...]
    rhs = jnp.sqrt(var[...]) * noise[...] + value[...] - observed
    e0[REACH, :mdev, :] = rhs
    e0[REACH, mdev:, :] = jnp.broadcast_to(plane_row, (8, odev))

    def band_send(src, dst_of, send, recv):
        def one(i, c):
            away = (REACH - lax.div(i, 2)) * (1 - 2 * lax.rem(i, 2))
            to = lax.rem(me_s + away + space_count, space_count)
            pltpu.make_async_remote_copy(
                src_ref=src, dst_ref=dst_of(REACH - away),
                send_sem=ssem.at[send], recv_sem=rsem.at[recv],
                device_id={"space": to}, device_id_type=MESH).start()
            return c

        lax.fori_loop(0, 2 * REACH, one, 0)

    band_send(e0.at[REACH], lambda j: e0.at[j], S_RHS, R_RHS)

    awaited(ao.at[pl.ds(0, members - mdev)], rsem.at[R_OBS])
    all_obs = ao[...]
    anom = all_obs - jnp.sum(all_obs, axis=0, keepdims=True) / members
    centre = pl.ds(REACH * odev, odev)
    ab[:, centre] = anom
    band_send(ab.at[:, centre], lambda j: ab.at[:, pl.ds(pl.multiple_of(j * odev, odev), odev)], S_BAND, R_BAND)

    right = other(me_m, 1, mem_count)
    left = other(me_m, mem_count - 1, mem_count)

    def relay(step, way, only=None):
        origin = lax.rem(me_m + mem_count - (step if way > 0 else -step), mem_count)
        rows = pl.ds(pl.multiple_of(origin * mdev, mdev), mdev)
        which = slice(None) if only is None else pl.ds(only, 1)
        ref = zs.at[which, rows, :]
        return pltpu.make_async_remote_copy(
            src_ref=ref, dst_ref=ref,
            send_sem=ssem.at[(S_RIGHT if way > 0 else S_LEFT) + step],
            recv_sem=rsem.at[(R_RIGHT if way > 0 else R_LEFT) + step],
            device_id={"mem": right if way > 0 else left}, device_id_type=MESH)

    def relay_wait(step, only=None):
        for base in (R_RIGHT, R_LEFT):
            if only is None:
                awaited(zs.at[:, pl.ds(0, mdev), :], rsem.at[base + step])
            else:
                awaited(zs.at[pl.ds(0, 1), pl.ds(0, mdev), :], rsem.at[base + step])

    relay(0, 1).start()
    relay(0, -1).start()

    anom_t = anom.T
    th, tl = halves(anom_t)
    both_t = jnp.concatenate([th, tl], axis=0)
    own_plane = jnp.broadcast_to(plane_row, (odev, odev)).T
    own_var = jnp.broadcast_to(var[...], (odev, odev)).T
    diagonal = (lax.broadcasted_iota(jnp.int32, (odev, odev), 0) == lax.broadcasted_iota(jnp.int32, (odev, odev), 1))
    diag_var = jnp.where(diagonal, own_var, 0.0)

    def taper(a, b):
        spread = jnp.abs(a - b)
        spread = jnp.minimum(spread, planes - spread)
        return jnp.maximum(0.0, 1.0 - spread / LOC)

    awaited(e0.at[pl.ds(0, 2 * REACH)], rsem.at[R_RHS])
    awaited(ab.at[:, pl.ds(0, 2 * REACH * odev)], rsem.at[R_BAND])
    relay_wait(0)
    relay(1, 1).start()
    relay(1, -1).start()

    def rows_of(j, total):
        lanes = pl.ds(pl.multiple_of(j * odev, odev), odev)
        high, low = halves(ab[:, lanes])
        ah[:, lanes] = high
        al[:, lanes] = low
        gram = nn(both_t, high)
        gram = gram[:odev] + gram[odev:] + nn(th, low)
        shape = taper(own_plane, e0[j, pl.ds(mdev, 1), :])
        block = shape * gram / (members - 1)
        block = block + jnp.where(j == REACH, 1.0, 0.0) * diag_var
        chigh, clow = halves(block)
        ch[:, lanes] = chigh
        cl[:, lanes] = clow
        dhigh, dlow = halves(e0[j, pl.ds(0, mdev), :])
        dh[:mdev, lanes] = dhigh
        dh[mdev:, lanes] = dlow
        return total + jnp.abs(block)

    total = lax.fori_loop(0, SLOTS, rows_of, jnp.zeros((odev, odev), f32))

    def image_of():
        top = nt(dh[...], ch[...])
        return top[:mdev] + top[mdev:] + nt(dh[:mdev, :], cl[...])

    def load(e):
        def one(j, c):
            lanes = pl.ds(pl.multiple_of(j * odev, odev), odev)
            dhigh, dlow = halves(ex[e, j])
            dh[:mdev, lanes] = dhigh
            dh[mdev:, lanes] = dlow
            return c

        lax.fori_loop(0, SLOTS, one, 0)

    def exchange(e, block):
        ex[e, REACH] = block
        band_send(ex.at[e, REACH], lambda j: ex.at[e, j], S_DIR + e, R_DIR + e)

    def arrived(e):
        awaited(ex.at[e, pl.ds(0, 2 * REACH)], rsem.at[R_DIR + e])

    first_image = image_of()
    exchange(0, first_image)

    row_max = jnp.max(jnp.sum(total, axis=1, keepdims=True), axis=0, keepdims=True)
    var_min = jnp.min(var[...], axis=1, keepdims=True)
    is_upper = lax.broadcasted_iota(jnp.int32, (8, odev), 0) < 4
    bb[me_s] = jnp.where(is_upper, row_max, -var_min)

    def send_bound(i, c):
        pltpu.make_async_remote_copy(
            src_ref=bb.at[me_s], dst_ref=bb.at[me_s],
            send_sem=ssem.at[S_BOUND], recv_sem=rsem.at[R_BOUND],
            device_id={"space": other(me_s, i, space_count)}, device_id_type=MESH).start()
        return c

    lax.fori_loop(1, space_count, send_bound, 0)

    arrived(0)
    load(0)
    second_image = image_of()

    awaited(bb.at[pl.ds(0, space_count - 1)], rsem.at[R_BOUND])
    bounds = jnp.max(bb[...], axis=0)
    upper = bounds[0:1, :]
    lower = -bounds[4:5, :]
    center = (upper + lower) / 2.0
    radius = (upper - lower) / 2.0
    sigma = center / radius
    rho = 1.0 / sigma
    direction = rhs / center
    weight = direction
    residual = rhs - first_image / center
    rho_next = 1.0 / (2.0 * sigma - rho)
    keep, take = rho_next * rho, 2.0 * rho_next / radius
    image = keep * (first_image / center) + take * (first_image - second_image / center)
    direction = keep * direction + take * residual
    rho = rho_next
    weight = weight + direction

    for e in range(1, ITERS - 2):
        residual = residual - image
        rho_next = 1.0 / (2.0 * sigma - rho)
        direction = rho_next * rho * direction + 2.0 * rho_next / radius * residual
        rho = rho_next
        weight = weight + direction
        exchange(e, direction)
        if e == 1:
            relay_wait(1)
            relay(2, 1).start()
            relay(2, -1).start()
        if e == 3:
            relay_wait(2)
            relay(3, 1, 0).start()
            relay(3, -1, 1).start()
        arrived(e)
        load(e)
        image = image_of()
    residual = residual - image
    rho_next = 1.0 / (2.0 * sigma - rho)
    direction = rho_next * rho * direction + 2.0 * rho_next / radius * residual
    weight = weight + direction
    last = ITERS - 2
    exchange(last, weight)
    arrived(last)

    gain = jnp.zeros((2 * mdev, members), f32)
    base = me_s.astype(f32) * 2.0

    def gains(j, total):
        lanes = pl.ds(pl.multiple_of(j * odev, odev), odev)
        row = e0[j, pl.ds(mdev, 1), :]
        block = ex[last, j]
        wide = jnp.concatenate([block * taper(base, row), block * taper(base + 1.0, row)], axis=0)
        high, low = halves(wide)
        top = nt(jnp.concatenate([high, low], axis=0), ah[:, lanes])
        return total + top[:2 * mdev] + top[2 * mdev:] + nt(high, al[:, lanes])

    gain = lax.fori_loop(0, SLOTS, gains, gain) / (members - 1)

    relay_wait(3, 0)

    width = 512
    for x in range(2):
        ghigh, glow = halves(gain[x * mdev:(x + 1) * mdev])
        gboth = jnp.concatenate([ghigh, glow], axis=0)

        def update(i, c, x=x, ghigh=ghigh, gboth=gboth):
            lanes = pl.ds(pl.multiple_of(i * width, width), width)
            states = zs[x, :, lanes]
            states = states - jnp.sum(states, axis=0, keepdims=True) / members
            high, low = halves(states)
            top = nn(gboth, high)
            out[x, :, lanes] = zs[x, mine, lanes] + (top[:mdev] + top[mdev:] + nn(ghigh, low))
            return c

        lax.fori_loop(0, slab // width, update, 0)

    awaited(r.at[pl.ds(0, planes - 2)], ssem.at[S_OUT])
    awaited(fr.at[pl.ds(0, space_count - 1)], ssem.at[S_FORC])
    awaited(r.at[pl.ds(0, planes - 2)], ssem.at[S_BACK])
    awaited(ao.at[pl.ds(0, members - mdev)], ssem.at[S_OBS])
    awaited(e0.at[pl.ds(0, 2 * REACH)], ssem.at[S_RHS])
    awaited(ab.at[:, pl.ds(0, 2 * REACH * odev)], ssem.at[S_BAND])
    awaited(bb.at[pl.ds(0, space_count - 1)], ssem.at[S_BOUND])
    for e in range(ITERS - 1):
        awaited(ex.at[e, pl.ds(0, 2 * REACH)], ssem.at[S_DIR + e])
    for step in range(3):
        for at in (S_RIGHT, S_LEFT):
            awaited(zs.at[:, pl.ds(0, mdev), :], ssem.at[at + step])
    for at in (S_RIGHT, S_LEFT):
        awaited(zs.at[pl.ds(0, 1), pl.ds(0, mdev), :], ssem.at[at + 3])


def shards(ensemble, forcing, obs_cell, obs_value, obs_var, obs_noise):
    mdev, pdev, slab = ensemble.shape
    odev = obs_cell.shape[0]
    space_count = lax.axis_size("space")
    mem_count = lax.axis_size("mem")
    members = mdev * mem_count
    planes = pdev * space_count
    cell = obs_cell - lax.axis_index("space") * (pdev * slab)
    plane = (obs_cell // slab).astype(f32)
    band = SLOTS * odev

    def call(*args):
        return kernel(space_count, mem_count, *args)

    vmem = pl.BlockSpec(memory_space=pltpu.VMEM)
    analysis = pl.pallas_call(
        call,
        out_shape=jax.ShapeDtypeStruct((pdev, mdev, slab), f32),
        in_specs=[vmem] * 7,
        out_specs=vmem,
        scratch_shapes=[
            pltpu.VMEM((planes, mdev // 2, 128), f32),
            pltpu.VMEM((planes, mdev // 2, 128), f32),
            pltpu.VMEM((space_count, pdev, 128), f32),
            pltpu.VMEM((pdev, members, slab), f32),
            pltpu.VMEM((pdev * slab, odev), bf16),
            pltpu.VMEM((members, odev), f32),
            pltpu.VMEM((members, band), f32),
            pltpu.VMEM((members, band), bf16),
            pltpu.VMEM((members, band), bf16),
            pltpu.VMEM((SLOTS, mdev + 8, odev), f32),
            pltpu.VMEM((ITERS - 1, SLOTS, mdev, odev), f32),
            pltpu.VMEM((space_count, 8, odev), f32),
            pltpu.VMEM((odev, band), bf16),
            pltpu.VMEM((odev, band), bf16),
            pltpu.VMEM((2 * mdev, band), bf16),
            pltpu.SemaphoreType.DMA((SENDS,)),
            pltpu.SemaphoreType.DMA((RECVS,)),
            pltpu.SemaphoreType.DMA((3,)),
        ],
        compiler_params=pltpu.CompilerParams(collective_id=0, has_side_effects=True),
        name="cycle",
    )(
        jnp.transpose(ensemble, (1, 0, 2)), forcing, cell[None, :], obs_value[None, :], obs_var[None, :],
        obs_noise, plane[None, :],
    )
    return jnp.transpose(analysis, (1, 0, 2))


def solution(mesh):
    placed = (
        P("mem", "space", None),
        P("space", None),
        P("space"),
        P("space"),
        P("space"),
        P("mem", "space"),
    )
    return jax.shard_map(
        shards, mesh=mesh, in_specs=placed, out_specs=P("mem", "space", None), check_vma=False
    )
```

```python
import jax
import jax.numpy as jnp
from jax import lax
from jax.experimental import pallas as pl
from jax.experimental.pallas import tpu as pltpu
from jax.sharding import PartitionSpec as P

FSTEPS = 4
ITERS = 6
LOC = 16
REACH = 8
SLOTS = 2 * REACH + 1
MESH = pl.DeviceIdType.MESH
f32 = jnp.float32
bf16 = jnp.bfloat16

R_OUT, R_FORC, R_BACK, R_RHS, R_BOUND = range(5)
R_DIR = 5
R_OBS = 10
R_BAND = 18
R_RIGHT = 35
R_LEFT = 42
RECVS = 49
S_OUT, S_FORC, S_BACK, S_OBS, S_RHS, S_BAND, S_PAIR, S_BOUND = range(8)
S_DIR = 8
S_RIGHT = 13
S_LEFT = 20
SENDS = 27
HOPS = 7

NT = (((1,), (1,)), ((), ()))


def nn(a, b):
    return jnp.dot(a, b, preferred_element_type=f32)


def nt(a, b):
    return lax.dot_general(a, b, NT, preferred_element_type=f32)


def halves(x):
    high = x.astype(bf16)
    return high, (x - high.astype(f32)).astype(bf16)


def awaited(ref, sem):
    pltpu.make_async_copy(ref, ref, sem).wait()


def kernel(
    space_count, mem_count,
    ens, forc, cell, value, var, noise, plane,
    out,
    r, t, fr, zs, sh, sl, oh, ab, ah, al, e0, ex, bb, ch, cl, dh, gh,
    ssem, rsem, lsem,
):
    me_s = lax.axis_index("space")
    me_m = lax.axis_index("mem")
    members = ab.shape[1]
    mdev = noise.shape[0]
    planes = r.shape[0]
    half = mdev // 2
    odev = cell.shape[1]
    slab = ens.shape[2]

    def chunk_of(index):
        return lax.div(index, 2), lax.rem(index, 2)

    def other(base, step, count):
        return lax.rem(base + step, count)

    barrier = pltpu.get_barrier_semaphore()

    def greet_space(i, c):
        pl.semaphore_signal(barrier, inc=1, device_id={"space": other(me_s, i, space_count)}, device_id_type=MESH)
        return c

    def greet_mem(i, c):
        pl.semaphore_signal(barrier, inc=1, device_id={"mem": other(me_m, i, mem_count)}, device_id_type=MESH)
        return c

    lax.fori_loop(1, space_count, greet_space, 0)
    lax.fori_loop(1, mem_count, greet_mem, 0)

    my_c, my_h = chunk_of(me_s)
    own_out = pltpu.make_async_copy(
        ens.at[:, pl.ds(pl.multiple_of(my_h * half, half), half), pl.ds(pl.multiple_of(my_c * 128, 128), 128)],
        r.at[pl.ds(me_s * 2, 2)], lsem.at[0])
    own_forc = pltpu.make_async_copy(
        forc.at[:, pl.ds(pl.multiple_of(my_c * 128, 128), 128)], fr.at[me_s], lsem.at[1])
    own_out.start()
    own_forc.start()

    pl.semaphore_wait(barrier, space_count + mem_count - 2)

    def send_out(i, c):
        to = other(me_s, i, space_count)
        tc, th = chunk_of(to)
        cells = pl.ds(pl.multiple_of(tc * 128, 128), 128)
        pltpu.make_async_remote_copy(
            src_ref=forc.at[:, cells], dst_ref=fr.at[me_s],
            send_sem=ssem.at[S_FORC], recv_sem=rsem.at[R_FORC],
            device_id={"space": to}, device_id_type=MESH).start()
        pltpu.make_async_remote_copy(
            src_ref=ens.at[:, pl.ds(pl.multiple_of(th * half, half), half), cells],
            dst_ref=r.at[pl.ds(me_s * 2, 2)],
            send_sem=ssem.at[S_OUT], recv_sem=rsem.at[R_OUT],
            device_id={"space": to}, device_id_type=MESH).start()
        return c

    lax.fori_loop(1, space_count, send_out, 0)

    cells_here = cell[...]

    def one_hot(i, c):
        rows = lax.broadcasted_iota(jnp.int32, (256, odev), 0) + i * 256
        oh[pl.ds(pl.multiple_of(i * 256, 256), 256), :] = jnp.where(rows == cells_here, 1.0, 0.0).astype(bf16)
        return c

    lax.fori_loop(0, 2 * slab // 256, one_hot, 0)

    own_out.wait()
    own_forc.wait()
    awaited(r.at[pl.ds(0, planes - 2)], rsem.at[R_OUT])
    awaited(fr.at[pl.ds(0, space_count - 1)], rsem.at[R_FORC])

    def advance(src, dst):
        def group(g, carry):
            two, one, now = carry
            for i in range(8):
                x = g * 8 + i
                ahead = src[lax.rem(x + 1, planes)]
                force = fr[g * 4 + i // 2, pl.ds(i % 2, 1), :]
                dst[x] = now + 0.05 * ((ahead - two) * one - now + force)
                two, one, now = one, now, ahead
            return two, one, now

        lax.fori_loop(0, planes // 8, group, (src[planes - 2], src[planes - 1], src[0]))

    for step in range(FSTEPS // 2):
        advance(r, t)
        advance(t, r)

    mine = pl.ds(pl.multiple_of(me_m * mdev, mdev), mdev)
    my_rows = pl.ds(pl.multiple_of(me_m * mdev + my_h * half, half), half)
    my_cells = pl.ds(pl.multiple_of(my_c * 128, 128), 128)

    def send_back(i, c):
        to = other(me_s, i, space_count)
        pltpu.make_async_remote_copy(
            src_ref=r.at[pl.ds(to * 2, 2)], dst_ref=zs.at[:, my_rows, my_cells],
            send_sem=ssem.at[S_BACK], recv_sem=rsem.at[R_BACK],
            device_id={"space": to}, device_id_type=MESH).start()
        return c

    lax.fori_loop(1, space_count, send_back, 0)
    own_back = pltpu.make_async_copy(r.at[pl.ds(me_s * 2, 2)], zs.at[:, my_rows, my_cells], lsem.at[2])
    own_back.start()
    own_back.wait()
    awaited(r.at[pl.ds(0, planes - 2)], rsem.at[R_BACK])

    observed = jnp.zeros((3 * mdev, odev), f32)
    for x in range(2):
        block = zs[x, mine, :]
        first = block.astype(bf16)
        rest = block - first.astype(f32)
        second = rest.astype(bf16)
        third = (rest - second.astype(f32)).astype(bf16)
        pieces = jnp.concatenate([first, second, third], axis=0)
        observed = observed + nn(pieces, oh[x * slab:(x + 1) * slab, :])
    observed = observed[:mdev] + observed[mdev:2 * mdev] + observed[2 * mdev:]
    ab[REACH, mine, :] = observed

    def send_obs(i, c):
        pltpu.make_async_remote_copy(
            src_ref=ab.at[REACH, mine], dst_ref=ab.at[REACH, mine],
            send_sem=ssem.at[S_OBS], recv_sem=rsem.at[R_OBS + i],
            device_id={"mem": other(me_m, i, mem_count)}, device_id_type=MESH).start()
        return c

    lax.fori_loop(1, mem_count, send_obs, 0)

    right = other(me_m, 1, mem_count)
    left = other(me_m, mem_count - 1, mem_count)

    def relay(hop):
        for way in (1, -1):
            origin = lax.rem(me_m + mem_count - way * (hop // 2), mem_count)
            x = hop % 2 if way > 0 else 1 - hop % 2
            ref = zs.at[x, pl.ds(pl.multiple_of(origin * mdev, mdev), mdev), :]
            pltpu.make_async_remote_copy(
                src_ref=ref, dst_ref=ref,
                send_sem=ssem.at[(S_RIGHT if way > 0 else S_LEFT) + hop],
                recv_sem=rsem.at[(R_RIGHT if way > 0 else R_LEFT) + hop],
                device_id={"mem": right if way > 0 else left}, device_id_type=MESH).start()

    def relayed(hop):
        for base in (R_RIGHT, R_LEFT):
            awaited(zs.at[0, pl.ds(0, mdev), :], rsem.at[base + hop])

    plane_row = plane[...]
    rhs = jnp.sqrt(var[...]) * noise[...] + value[...] - observed
    e0[REACH, :mdev, :] = rhs
    e0[REACH, mdev:, :] = jnp.broadcast_to(plane_row, (8, odev))

    def spread_of(n, unit):
        at = lax.div(n, 2)
        far = lax.div(at + 1, 2) * (1 - 2 * lax.rem(at + 1, 2))
        return (REACH // (2 * unit) + far) * unit * (1 - 2 * lax.rem(n, 2))

    def band_send(src, dst_of, send, recv):
        def one(i, c):
            away = spread_of(i, 1)
            to = lax.rem(me_s + away + space_count, space_count)
            pltpu.make_async_remote_copy(
                src_ref=src, dst_ref=dst_of(REACH - away),
                send_sem=ssem.at[send], recv_sem=rsem.at[recv],
                device_id={"space": to}, device_id_type=MESH).start()
            return c

        lax.fori_loop(0, 2 * REACH, one, 0)

    band_send(e0.at[REACH], lambda j: e0.at[j], S_RHS, R_RHS)

    def piece_to(step, i):
        away = spread_of(i, 2)
        origin = lax.rem(me_m + mem_count - step, mem_count)
        rows = pl.ds(pl.multiple_of(origin * mdev, mdev), mdev)
        pltpu.make_async_remote_copy(
            src_ref=ab.at[REACH, rows], dst_ref=ab.at[REACH - away, rows],
            send_sem=ssem.at[S_BAND], recv_sem=rsem.at[R_BAND + REACH - away],
            device_id={"space": lax.rem(me_s + away + space_count, space_count)}, device_id_type=MESH).start()

    def piece_here(step):
        awaited(ab.at[REACH, pl.ds(0, mdev)], rsem.at[R_OBS + step])

    def to_chips(step):
        def one(i, c):
            piece_to(step, i)
            return c

        lax.fori_loop(0, REACH, one, 0)

    to_chips(0)
    relay(0)
    relay(1)
    early = (1, mem_count - 1)
    for step in early:
        piece_here(step)
        to_chips(step)
    for step in range(2, mem_count - 1):
        piece_here(step)

    def late(i, c):
        def one(step, d):
            piece_to(step, i)
            return d

        return lax.fori_loop(2, mem_count - 1, one, c)

    lax.fori_loop(0, REACH, late, 0)

    turn = 1 - 2 * my_h
    partner = me_s + turn

    def pair_send(e):
        pltpu.make_async_remote_copy(
            src_ref=ab.at[REACH + turn * e], dst_ref=ab.at[REACH + turn * (e - 1)],
            send_sem=ssem.at[S_PAIR], recv_sem=rsem.at[R_BAND + REACH + turn * (e - 1)],
            device_id={"space": partner}, device_id_type=MESH).start()

    def slot_here(j):
        awaited(ab.at[0], rsem.at[R_BAND + j])

    pair_send(0)

    def anomalies(j):
        raw = ab[j]
        return raw - jnp.sum(raw, axis=0, keepdims=True) / members

    anom_t = anomalies(REACH).T
    th, tl = halves(anom_t)
    both_t = jnp.concatenate([th, tl], axis=0)
    own_plane = jnp.broadcast_to(plane_row, (odev, odev)).T
    own_var = jnp.broadcast_to(var[...], (odev, odev)).T
    diagonal = (lax.broadcasted_iota(jnp.int32, (odev, odev), 0) == lax.broadcasted_iota(jnp.int32, (odev, odev), 1))
    diag_var = jnp.where(diagonal, own_var, 0.0)

    def taper(a, b):
        spread = jnp.abs(a - b)
        spread = jnp.minimum(spread, planes - spread)
        return jnp.maximum(0.0, 1.0 - spread / LOC)

    def rows_of(j, total, more=None):
        lanes = pl.ds(pl.multiple_of(j * odev, odev), odev)
        high, low = halves(anomalies(j))
        ah[:, lanes] = high
        al[:, lanes] = low
        gram = nn(both_t, high)
        gram = gram[:odev] + gram[odev:] + nn(th, low)
        block = taper(own_plane, e0[j, pl.ds(mdev, 1), :]) * gram / (members - 1)
        if more is not None:
            block = block + more
        chigh, clow = halves(block)
        ch[:, lanes] = chigh
        cl[:, lanes] = clow
        dhigh, dlow = halves(e0[j, pl.ds(0, mdev), :])
        dh[:mdev, lanes] = dhigh
        dh[mdev:, lanes] = dlow
        return total + jnp.abs(block)

    total = rows_of(REACH, jnp.zeros((odev, odev), f32), diag_var)
    awaited(e0.at[pl.ds(0, 2 * REACH)], rsem.at[R_RHS])
    relayed(0)
    relay(2)

    def from_partner(e, total):
        j = REACH + turn * (1 - e)
        slot_here(j)
        return rows_of(j, total)

    def two_slots(i, total):
        e = spread_of(i, 2)
        j = REACH + turn * e
        slot_here(j)
        pair_send(e)
        total = rows_of(j, total)
        return from_partner(jnp.where(i == 0, 0, spread_of(lax.max(i - 1, 0), 2)), total)

    total = lax.fori_loop(0, REACH - 1, two_slots, total)
    final = REACH - turn * REACH
    slot_here(final)
    total = rows_of(final, total)
    total = from_partner(spread_of(REACH - 2, 2), total)
    relayed(1)
    relay(3)

    def image_of():
        top = nt(dh[...], ch[...])
        return top[:mdev] + top[mdev:] + nt(dh[:mdev, :], cl[...])

    def load(e):
        def one(j, c):
            lanes = pl.ds(pl.multiple_of(j * odev, odev), odev)
            dhigh, dlow = halves(ex[e, j])
            dh[:mdev, lanes] = dhigh
            dh[mdev:, lanes] = dlow
            return c

        lax.fori_loop(0, SLOTS, one, 0)

    def exchange(e, block):
        ex[e, REACH] = block
        band_send(ex.at[e, REACH], lambda j: ex.at[e, j], S_DIR + e, R_DIR + e)

    def arrived(e):
        awaited(ex.at[e, pl.ds(0, 2 * REACH)], rsem.at[R_DIR + e])

    first_image = image_of()
    exchange(0, first_image)

    row_max = jnp.max(jnp.sum(total, axis=1, keepdims=True), axis=0, keepdims=True)
    var_min = jnp.min(var[...], axis=1, keepdims=True)
    is_upper = lax.broadcasted_iota(jnp.int32, (8, odev), 0) < 4
    bb[me_s] = jnp.where(is_upper, row_max, -var_min)

    def send_bound(i, c):
        pltpu.make_async_remote_copy(
            src_ref=bb.at[me_s], dst_ref=bb.at[me_s],
            send_sem=ssem.at[S_BOUND], recv_sem=rsem.at[R_BOUND],
            device_id={"space": other(me_s, i, space_count)}, device_id_type=MESH).start()
        return c

    lax.fori_loop(1, space_count, send_bound, 0)

    arrived(0)
    relayed(2)
    relay(4)
    load(0)
    second_image = image_of()

    awaited(bb.at[pl.ds(0, space_count - 1)], rsem.at[R_BOUND])
    bounds = jnp.max(bb[...], axis=0)
    upper = bounds[0:1, :]
    lower = -bounds[4:5, :]
    center = (upper + lower) / 2.0
    radius = (upper - lower) / 2.0
    sigma = center / radius
    rho = 1.0 / sigma
    direction = rhs / center
    weight = direction
    residual = rhs - first_image / center
    rho_next = 1.0 / (2.0 * sigma - rho)
    keep, take = rho_next * rho, 2.0 * rho_next / radius
    image = keep * (first_image / center) + take * (first_image - second_image / center)
    direction = keep * direction + take * residual
    rho = rho_next
    weight = weight + direction

    for e in range(1, ITERS - 2):
        residual = residual - image
        rho_next = 1.0 / (2.0 * sigma - rho)
        direction = rho_next * rho * direction + 2.0 * rho_next / radius * residual
        rho = rho_next
        weight = weight + direction
        exchange(e, direction)
        arrived(e)
        if e < 3:
            relayed(e + 2)
            relay(e + 4)
        load(e)
        image = image_of()
    residual = residual - image
    rho_next = 1.0 / (2.0 * sigma - rho)
    direction = rho_next * rho * direction + 2.0 * rho_next / radius * residual
    weight = weight + direction
    last = ITERS - 2
    exchange(last, weight)

    relayed(HOPS - 2)
    relayed(HOPS - 1)
    width = 512

    def split_states(i, c):
        x = lax.div(i, slab // width)
        lanes = pl.ds(pl.multiple_of(lax.rem(i, slab // width) * width, width), width)
        states = zs[x, :, lanes]
        high, low = halves(states - jnp.sum(states, axis=0, keepdims=True) / members)
        sh[x, :, lanes] = high
        sl[x, :, lanes] = low
        return c

    lax.fori_loop(0, 2 * slab // width, split_states, 0)
    arrived(last)

    base = me_s.astype(f32) * 2.0

    def tapered(j, c):
        lanes = pl.ds(pl.multiple_of(j * odev, odev), odev)
        row = e0[j, pl.ds(mdev, 1), :]
        block = ex[last, j]
        for x in range(2):
            high, low = halves(block * taper(base + x, row))
            gh[x * mdev:(x + 1) * mdev, lanes] = high
            gh[(2 + x) * mdev:(3 + x) * mdev, lanes] = low
        return c

    lax.fori_loop(0, SLOTS, tapered, 0)
    top = nt(gh[...], ah[...])
    gain = (top[:2 * mdev] + top[2 * mdev:] + nt(gh[:2 * mdev, :], al[...])) / (members - 1)

    for x in range(2):
        ghigh, glow = halves(gain[x * mdev:(x + 1) * mdev])
        gboth = jnp.concatenate([ghigh, glow], axis=0)

        def update(i, c, x=x, ghigh=ghigh, gboth=gboth):
            lanes = pl.ds(pl.multiple_of(i * width, width), width)
            top = nn(gboth, sh[x, :, lanes])
            out[x, :, lanes] = zs[x, mine, lanes] + (top[:mdev] + top[mdev:] + nn(ghigh, sl[x, :, lanes]))
            return c

        lax.fori_loop(0, slab // width, update, 0)

    awaited(r.at[pl.ds(0, planes - 2)], ssem.at[S_OUT])
    awaited(fr.at[pl.ds(0, space_count - 1)], ssem.at[S_FORC])
    awaited(r.at[pl.ds(0, planes - 2)], ssem.at[S_BACK])
    awaited(ab.at[0, pl.ds(0, members - mdev)], ssem.at[S_OBS])
    awaited(e0.at[pl.ds(0, 2 * REACH)], ssem.at[S_RHS])
    awaited(ab.at[pl.ds(0, REACH)], ssem.at[S_BAND])
    awaited(ab.at[pl.ds(0, REACH)], ssem.at[S_PAIR])
    awaited(bb.at[pl.ds(0, space_count - 1)], ssem.at[S_BOUND])
    for e in range(ITERS - 1):
        awaited(ex.at[e, pl.ds(0, 2 * REACH)], ssem.at[S_DIR + e])
    for hop in range(HOPS):
        for at in (S_RIGHT, S_LEFT):
            awaited(zs.at[0, pl.ds(0, mdev), :], ssem.at[at + hop])


def shards(ensemble, forcing, obs_cell, obs_value, obs_var, obs_noise):
    mdev, pdev, slab = ensemble.shape
    odev = obs_cell.shape[0]
    space_count = lax.axis_size("space")
    mem_count = lax.axis_size("mem")
    members = mdev * mem_count
    planes = pdev * space_count
    cell = obs_cell - lax.axis_index("space") * (pdev * slab)
    plane = (obs_cell // slab).astype(f32)
    band = SLOTS * odev

    def call(*args):
        return kernel(space_count, mem_count, *args)

    vmem = pl.BlockSpec(memory_space=pltpu.VMEM)
    analysis = pl.pallas_call(
        call,
        out_shape=jax.ShapeDtypeStruct((pdev, mdev, slab), f32),
        in_specs=[vmem] * 7,
        out_specs=vmem,
        scratch_shapes=[
            pltpu.VMEM((planes, mdev // 2, 128), f32),
            pltpu.VMEM((planes, mdev // 2, 128), f32),
            pltpu.VMEM((space_count, pdev, 128), f32),
            pltpu.VMEM((pdev, members, slab), f32),
            pltpu.VMEM((pdev, members, slab), bf16),
            pltpu.VMEM((pdev, members, slab), bf16),
            pltpu.VMEM((pdev * slab, odev), bf16),
            pltpu.VMEM((SLOTS, members, odev), f32),
            pltpu.VMEM((members, band), bf16),
            pltpu.VMEM((members, band), bf16),
            pltpu.VMEM((SLOTS, mdev + 8, odev), f32),
            pltpu.VMEM((ITERS - 1, SLOTS, mdev, odev), f32),
            pltpu.VMEM((space_count, 8, odev), f32),
            pltpu.VMEM((odev, band), bf16),
            pltpu.VMEM((odev, band), bf16),
            pltpu.VMEM((2 * mdev, band), bf16),
            pltpu.VMEM((2 * pdev * mdev, band), bf16),
            pltpu.SemaphoreType.DMA((SENDS,)),
            pltpu.SemaphoreType.DMA((RECVS,)),
            pltpu.SemaphoreType.DMA((3,)),
        ],
        compiler_params=pltpu.CompilerParams(collective_id=0, has_side_effects=True),
        name="cycle",
    )(
        jnp.transpose(ensemble, (1, 0, 2)), forcing, cell[None, :], obs_value[None, :], obs_var[None, :],
        obs_noise, plane[None, :],
    )
    return jnp.transpose(analysis, (1, 0, 2))


def solution(mesh):
    placed = (
        P("mem", "space", None),
        P("space", None),
        P("space"),
        P("space"),
        P("space"),
        P("mem", "space"),
    )
    return jax.shard_map(
        shards, mesh=mesh, in_specs=placed, out_specs=P("mem", "space", None), check_vma=False
    )
```

```python
import jax
import jax.numpy as jnp
from jax import lax
from jax.experimental import pallas as pl
from jax.experimental.pallas import tpu as pltpu
from jax.sharding import PartitionSpec as P

FSTEPS = 4
ITERS = 6
LOC = 16
REACH = 8
SLOTS = 2 * REACH + 1
MESH = pl.DeviceIdType.MESH
f32 = jnp.float32
bf16 = jnp.bfloat16

GROUP = 4
GROUPS = 2 * REACH // GROUP
HOPS = 7
R_OUT, R_FORC, R_BACK, R_RHS, R_BOUND = range(5)
R_DIR = 5
R_OBS = R_DIR + GROUPS * (ITERS - 1)
R_BAND = R_OBS + 8
R_RIGHT = R_BAND + SLOTS
R_LEFT = R_RIGHT + HOPS
RECVS = R_LEFT + HOPS
S_OUT, S_FORC, S_BACK, S_OBS, S_RHS, S_BAND, S_PAIR, S_BOUND = range(8)
S_DIR = 8
S_RIGHT = S_DIR + ITERS - 1
S_LEFT = S_RIGHT + HOPS
SENDS = S_LEFT + HOPS

NT = (((1,), (1,)), ((), ()))


def nn(a, b):
    return jnp.dot(a, b, preferred_element_type=f32)


def nt(a, b):
    return lax.dot_general(a, b, NT, preferred_element_type=f32)


def halves(x):
    high = x.astype(bf16)
    return high, (x - high.astype(f32)).astype(bf16)


def awaited(ref, sem):
    pltpu.make_async_copy(ref, ref, sem).wait()


def kernel(
    space_count, mem_count,
    ens, forc, cell, value, var, noise,
    out,
    r, t, fr, zs, sh, sl, oh, ab, ah, al, e0, ex, bb, ch, cl,
    ssem, rsem, lsem,
):
    me_s = lax.axis_index("space")
    me_m = lax.axis_index("mem")
    members = ab.shape[1]
    mdev = noise.shape[0]
    planes = r.shape[0]
    half = mdev // 2
    odev = cell.shape[1]
    slab = ens.shape[2]

    def chunk_of(index):
        return lax.div(index, 2), lax.rem(index, 2)

    def other(base, step, count):
        return lax.rem(base + step, count)

    barrier = pltpu.get_barrier_semaphore()

    def greet_space(i, c):
        pl.semaphore_signal(barrier, inc=1, device_id={"space": other(me_s, i, space_count)}, device_id_type=MESH)
        return c

    def greet_mem(i, c):
        pl.semaphore_signal(barrier, inc=1, device_id={"mem": other(me_m, i, mem_count)}, device_id_type=MESH)
        return c

    lax.fori_loop(1, space_count, greet_space, 0)
    lax.fori_loop(1, mem_count, greet_mem, 0)

    my_c, my_h = chunk_of(me_s)
    own_out = pltpu.make_async_copy(
        ens.at[:, pl.ds(pl.multiple_of(my_h * half, half), half), pl.ds(pl.multiple_of(my_c * 128, 128), 128)],
        r.at[pl.ds(me_s * 2, 2)], lsem.at[0])
    own_forc = pltpu.make_async_copy(
        forc.at[:, pl.ds(pl.multiple_of(my_c * 128, 128), 128)], fr.at[me_s], lsem.at[1])
    own_out.start()
    own_forc.start()

    pl.semaphore_wait(barrier, space_count + mem_count - 2)

    def send_out(i, c):
        to = other(me_s, i, space_count)
        tc, th = chunk_of(to)
        cells = pl.ds(pl.multiple_of(tc * 128, 128), 128)
        pltpu.make_async_remote_copy(
            src_ref=forc.at[:, cells], dst_ref=fr.at[me_s],
            send_sem=ssem.at[S_FORC], recv_sem=rsem.at[R_FORC],
            device_id={"space": to}, device_id_type=MESH).start()
        pltpu.make_async_remote_copy(
            src_ref=ens.at[:, pl.ds(pl.multiple_of(th * half, half), half), cells],
            dst_ref=r.at[pl.ds(me_s * 2, 2)],
            send_sem=ssem.at[S_OUT], recv_sem=rsem.at[R_OUT],
            device_id={"space": to}, device_id_type=MESH).start()
        return c

    lax.fori_loop(1, space_count, send_out, 0)

    cells_here = cell[...] - me_s * (2 * slab)

    def one_hot(i, c):
        rows = lax.broadcasted_iota(jnp.int32, (256, odev), 0) + i * 256
        oh[pl.ds(pl.multiple_of(i * 256, 256), 256), :] = jnp.where(rows == cells_here, 1.0, 0.0).astype(bf16)
        return c

    lax.fori_loop(0, 2 * slab // 256, one_hot, 0)

    own_out.wait()
    own_forc.wait()
    awaited(r.at[pl.ds(0, planes - 2)], rsem.at[R_OUT])
    awaited(fr.at[pl.ds(0, space_count - 1)], rsem.at[R_FORC])

    def advance(src, dst):
        def group(g, carry):
            two, one, now = carry
            for i in range(8):
                x = g * 8 + i
                ahead = src[lax.rem(x + 1, planes)]
                force = fr[g * 4 + i // 2, pl.ds(i % 2, 1), :]
                dst[x] = now + 0.05 * ((ahead - two) * one - now + force)
                two, one, now = one, now, ahead
            return two, one, now

        lax.fori_loop(0, planes // 8, group, (src[planes - 2], src[planes - 1], src[0]))

    for step in range(FSTEPS // 2):
        advance(r, t)
        advance(t, r)

    mine = pl.ds(pl.multiple_of(me_m * mdev, mdev), mdev)
    my_rows = pl.ds(pl.multiple_of(me_m * mdev + my_h * half, half), half)
    my_cells = pl.ds(pl.multiple_of(my_c * 128, 128), 128)

    def send_back(i, c):
        to = other(me_s, i, space_count)
        pltpu.make_async_remote_copy(
            src_ref=r.at[pl.ds(to * 2, 2)], dst_ref=zs.at[:, my_rows, my_cells],
            send_sem=ssem.at[S_BACK], recv_sem=rsem.at[R_BACK],
            device_id={"space": to}, device_id_type=MESH).start()
        return c

    lax.fori_loop(1, space_count, send_back, 0)
    own_back = pltpu.make_async_copy(r.at[pl.ds(me_s * 2, 2)], zs.at[:, my_rows, my_cells], lsem.at[2])
    own_back.start()
    own_back.wait()
    awaited(r.at[pl.ds(0, planes - 2)], rsem.at[R_BACK])

    observed = jnp.zeros((3 * mdev, odev), f32)
    for x in range(2):
        block = zs[x, mine, :]
        first = block.astype(bf16)
        rest = block - first.astype(f32)
        second = rest.astype(bf16)
        third = (rest - second.astype(f32)).astype(bf16)
        pieces = jnp.concatenate([first, second, third], axis=0)
        observed = observed + nn(pieces, oh[x * slab:(x + 1) * slab, :])
    observed = observed[:mdev] + observed[mdev:2 * mdev] + observed[2 * mdev:]
    ab[REACH, mine, :] = observed

    def send_obs(i, c):
        pltpu.make_async_remote_copy(
            src_ref=ab.at[REACH, mine], dst_ref=ab.at[REACH, mine],
            send_sem=ssem.at[S_OBS], recv_sem=rsem.at[R_OBS + i],
            device_id={"mem": other(me_m, i, mem_count)}, device_id_type=MESH).start()
        return c

    lax.fori_loop(1, mem_count, send_obs, 0)

    right = other(me_m, 1, mem_count)
    left = other(me_m, mem_count - 1, mem_count)

    def relay(hop):
        for way in (1, -1):
            origin = lax.rem(me_m + mem_count - way * (hop // 2), mem_count)
            x = hop % 2 if way > 0 else 1 - hop % 2
            ref = zs.at[x, pl.ds(pl.multiple_of(origin * mdev, mdev), mdev), :]
            pltpu.make_async_remote_copy(
                src_ref=ref, dst_ref=ref,
                send_sem=ssem.at[(S_RIGHT if way > 0 else S_LEFT) + hop],
                recv_sem=rsem.at[(R_RIGHT if way > 0 else R_LEFT) + hop],
                device_id={"mem": right if way > 0 else left}, device_id_type=MESH).start()

    def relayed(hop):
        for base in (R_RIGHT, R_LEFT):
            awaited(zs.at[0, pl.ds(0, mdev), :], rsem.at[base + hop])

    plane_row = jnp.floor(cell[...].astype(f32) / slab)
    rhs = jnp.sqrt(var[...]) * noise[...] + value[...] - observed
    own = 2 * REACH
    e0[own, :mdev, :] = rhs
    e0[own, mdev:, :] = jnp.broadcast_to(plane_row, (8, odev))

    def away_at(n):
        at = lax.div(n, 2)
        far = lax.div(at + 1, 2) * (1 - 2 * lax.rem(at + 1, 2))
        return (REACH // 2 + far) * (1 - 2 * lax.rem(n, 2))

    def place_of(away):
        past = lax.max(away, -away) - REACH // 2
        rank = 2 * lax.max(past, -past) - jnp.where(past > 0, 1, 0)
        return 2 * rank + jnp.where(away < 0, 1, 0)

    def band_send(src, dst_of, send, recv_of):
        def one(i, c):
            away = away_at(i)
            to = lax.rem(me_s + away + space_count, space_count)
            there = i + 1 - 2 * lax.rem(i, 2)
            pltpu.make_async_remote_copy(
                src_ref=src, dst_ref=dst_of(there),
                send_sem=ssem.at[send], recv_sem=rsem.at[recv_of(there)],
                device_id={"space": to}, device_id_type=MESH).start()
            return c

        lax.fori_loop(0, 2 * REACH, one, 0)

    band_send(e0.at[own], lambda j: e0.at[j], S_RHS, lambda j: R_RHS)

    def space_at(chips):
        return {"space": lax.rem(me_s + 2 * chips + space_count, space_count)}

    def piece_to(step, i):
        chips = (1 + 3 * lax.div(i, 2)) * (1 - 2 * lax.rem(i, 2))
        origin = lax.rem(me_m + mem_count - step, mem_count)
        rows = pl.ds(pl.multiple_of(origin * mdev, mdev), mdev)
        pltpu.make_async_remote_copy(
            src_ref=ab.at[REACH, rows], dst_ref=ab.at[REACH - 2 * chips, rows],
            send_sem=ssem.at[S_BAND], recv_sem=rsem.at[R_BAND + REACH - 2 * chips],
            device_id=space_at(chips), device_id_type=MESH).start()

    def piece_here(step):
        awaited(ab.at[REACH, pl.ds(0, mdev)], rsem.at[R_OBS + step])

    def to_chips(step):
        def one(i, c):
            piece_to(step, i)
            return c

        lax.fori_loop(0, 4, one, 0)

    to_chips(0)
    relay(0)
    relay(1)
    for away in range(1, mem_count // 2 + 1):
        for step in sorted({away, mem_count - away}):
            piece_here(step)
            to_chips(step)

    turn = 1 - 2 * my_h
    partner = me_s + turn

    def pair_send(e):
        pltpu.make_async_remote_copy(
            src_ref=ab.at[REACH + turn * e], dst_ref=ab.at[REACH + turn * (e - 1)],
            send_sem=ssem.at[S_PAIR], recv_sem=rsem.at[R_BAND + REACH + turn * (e - 1)],
            device_id={"space": partner}, device_id_type=MESH).start()

    def slot_here(j):
        awaited(ab.at[0], rsem.at[R_BAND + j])

    pair_send(0)

    def anomalies(j):
        raw = ab[j]
        return raw - jnp.sum(raw, axis=0, keepdims=True) / members

    anom_t = anomalies(REACH).T
    th, tl = halves(anom_t)
    both_t = jnp.concatenate([th, tl], axis=0)
    own_plane = jnp.broadcast_to(plane_row, (odev, odev)).T
    own_var = jnp.broadcast_to(var[...], (odev, odev)).T
    diagonal = (lax.broadcasted_iota(jnp.int32, (odev, odev), 0) == lax.broadcasted_iota(jnp.int32, (odev, odev), 1))
    diag_var = jnp.where(diagonal, own_var, 0.0)

    def taper(a, b):
        spread = jnp.abs(a - b)
        spread = jnp.minimum(spread, planes - spread)
        return jnp.maximum(0.0, 1.0 - spread / LOC)

    def rows_of(j, place, total, more=None):
        lanes = pl.ds(pl.multiple_of(place * odev, odev), odev)
        high, low = halves(anomalies(j))
        ah[:, lanes] = high
        al[:, lanes] = low
        gram = nn(both_t, high)
        gram = gram[:odev] + gram[odev:] + nn(th, low)
        block = taper(own_plane, e0[place, pl.ds(mdev, 1), :]) * gram / (members - 1)
        if more is not None:
            block = block + more
        chigh, clow = halves(block)
        ch[:, lanes] = chigh
        cl[:, lanes] = clow
        return total + jnp.abs(block)

    total = rows_of(REACH, own, jnp.zeros((odev, odev), f32), diag_var)

    for side in (1, -1):
        slot = REACH + 2 * side
        slot_here(slot)
        for chips in (-side, 4 * side):
            there = REACH + 2 * (side - chips)
            pltpu.make_async_remote_copy(
                src_ref=ab.at[slot], dst_ref=ab.at[there],
                send_sem=ssem.at[S_BAND], recv_sem=rsem.at[R_BAND + there],
                device_id=space_at(chips), device_id_type=MESH).start()
    pair_send(2)
    pair_send(-2)
    awaited(e0.at[pl.ds(0, 2 * REACH)], rsem.at[R_RHS])

    def slot_rows(e, total):
        return rows_of(REACH + turn * e, place_of(turn * e), total)

    def from_partner(e, total):
        slot_here(REACH + turn * (1 - e))
        return slot_rows(1 - e, total)

    total = slot_rows(2, total)
    total = slot_rows(-2, total)
    total = from_partner(0, total)
    relayed(0)
    relay(2)

    def pick(i, table):
        value = table[0]
        for k in range(1, len(table)):
            value = jnp.where(i == k, table[k], value)
        return value

    def two_slots(i, total):
        e = pick(i, (8, 4, -4, 6, -6))
        slot_here(REACH + turn * e)
        pair_send(e)
        total = slot_rows(e, total)
        return from_partner(pick(i, (2, -2, 8, 4, -4)), total)

    total = lax.fori_loop(0, 5, two_slots, total)
    slot_here(REACH - turn * REACH)
    total = slot_rows(-REACH, total)

    def last_two(i, total):
        return from_partner(pick(i, (6, -6)), total)

    total = lax.fori_loop(0, 2, last_two, total)
    relayed(1)
    relay(3)

    def part(block, lanes):
        high, low = halves(block)
        top = nt(jnp.concatenate([high, low], axis=0), ch[:, lanes])
        return top[:mdev] + top[mdev:] + nt(high, cl[:, lanes])

    def lanes_of(g):
        return slice(g * GROUP * odev, (g + 1) * GROUP * odev)

    own_lanes = slice(own * odev, (own + 1) * odev)

    def image_of(block, group):
        image = part(block, own_lanes)
        for g in range(GROUPS):
            image = image + part(group(g), lanes_of(g))
        return image

    def rhs_group(g):
        return jnp.concatenate([e0[g * GROUP + k, :mdev, :] for k in range(GROUP)], axis=1)

    def exchange(e, block):
        ex[e, own] = block
        band_send(ex.at[e, own], lambda j: ex.at[e, j], S_DIR + e, lambda j: R_DIR + GROUPS * e + lax.div(j, GROUP))

    def arrived(e):
        def group(g):
            awaited(ex.at[e, pl.ds(g * GROUP, GROUP)], rsem.at[R_DIR + GROUPS * e + g])
            return jnp.concatenate([ex[e, g * GROUP + k] for k in range(GROUP)], axis=1)

        return group

    first_image = image_of(rhs, rhs_group)
    exchange(0, first_image)

    row_max = jnp.max(jnp.sum(total, axis=1, keepdims=True), axis=0, keepdims=True)
    var_min = jnp.min(var[...], axis=1, keepdims=True)
    is_upper = lax.broadcasted_iota(jnp.int32, (8, odev), 0) < 4
    bb[me_s] = jnp.where(is_upper, row_max, -var_min)

    def send_bound(i, c):
        pltpu.make_async_remote_copy(
            src_ref=bb.at[me_s], dst_ref=bb.at[me_s],
            send_sem=ssem.at[S_BOUND], recv_sem=rsem.at[R_BOUND],
            device_id={"space": other(me_s, i, space_count)}, device_id_type=MESH).start()
        return c

    lax.fori_loop(1, space_count, send_bound, 0)

    second_image = image_of(first_image, arrived(0))
    relayed(2)
    relay(4)

    awaited(bb.at[pl.ds(0, space_count - 1)], rsem.at[R_BOUND])
    bounds = jnp.max(bb[...], axis=0)
    upper = bounds[0:1, :]
    lower = -bounds[4:5, :]
    center = (upper + lower) / 2.0
    radius = (upper - lower) / 2.0
    sigma = center / radius
    rho = 1.0 / sigma
    direction = rhs / center
    weight = direction
    residual = rhs - first_image / center
    rho_next = 1.0 / (2.0 * sigma - rho)
    keep, take = rho_next * rho, 2.0 * rho_next / radius
    image = keep * (first_image / center) + take * (first_image - second_image / center)
    direction = keep * direction + take * residual
    rho = rho_next
    weight = weight + direction

    for e in range(1, ITERS - 2):
        residual = residual - image
        rho_next = 1.0 / (2.0 * sigma - rho)
        direction = rho_next * rho * direction + 2.0 * rho_next / radius * residual
        rho = rho_next
        weight = weight + direction
        exchange(e, direction)
        image = image_of(direction, arrived(e))
        if e < 3:
            relayed(e + 2)
            relay(e + 4)
    residual = residual - image
    rho_next = 1.0 / (2.0 * sigma - rho)
    direction = rho_next * rho * direction + 2.0 * rho_next / radius * residual
    weight = weight + direction
    last = ITERS - 2
    exchange(last, weight)

    relayed(HOPS - 2)
    relayed(HOPS - 1)
    width = 512

    def split_states(i, c):
        x = lax.div(i, slab // width)
        lanes = pl.ds(pl.multiple_of(lax.rem(i, slab // width) * width, width), width)
        states = zs[x, :, lanes]
        high, low = halves(states - jnp.sum(states, axis=0, keepdims=True) / members)
        sh[x, :, lanes] = high
        sl[x, :, lanes] = low
        return c

    lax.fori_loop(0, 2 * slab // width, split_states, 0)

    base = me_s.astype(f32) * 2.0

    def gain_part(block, row, lanes):
        wide = jnp.concatenate([block * taper(base, row), block * taper(base + 1.0, row)], axis=0)
        high, low = halves(wide)
        top = nt(jnp.concatenate([high, low], axis=0), ah[:, lanes])
        return top[:2 * mdev] + top[2 * mdev:] + nt(high, al[:, lanes])

    gain = gain_part(weight, plane_row, own_lanes)
    group = arrived(last)
    for g in range(GROUPS):
        rows = jnp.concatenate([e0[g * GROUP + k, pl.ds(mdev, 1), :] for k in range(GROUP)], axis=1)
        gain = gain + gain_part(group(g), rows, lanes_of(g))
    gain = gain / (members - 1)

    for x in range(2):
        ghigh, glow = halves(gain[x * mdev:(x + 1) * mdev])
        gboth = jnp.concatenate([ghigh, glow], axis=0)

        def update(i, c, x=x, ghigh=ghigh, gboth=gboth):
            lanes = pl.ds(pl.multiple_of(i * width, width), width)
            top = nn(gboth, sh[x, :, lanes])
            out[x, :, lanes] = zs[x, mine, lanes] + (top[:mdev] + top[mdev:] + nn(ghigh, sl[x, :, lanes]))
            return c

        lax.fori_loop(0, slab // width, update, 0)

    awaited(r.at[pl.ds(0, planes - 2)], ssem.at[S_OUT])
    awaited(fr.at[pl.ds(0, space_count - 1)], ssem.at[S_FORC])
    awaited(r.at[pl.ds(0, planes - 2)], ssem.at[S_BACK])
    awaited(ab.at[0, pl.ds(0, members - mdev)], ssem.at[S_OBS])
    awaited(e0.at[pl.ds(0, 2 * REACH)], ssem.at[S_RHS])
    awaited(ab.at[pl.ds(0, REACH)], ssem.at[S_BAND])
    awaited(ab.at[pl.ds(0, REACH)], ssem.at[S_PAIR])
    awaited(bb.at[pl.ds(0, space_count - 1)], ssem.at[S_BOUND])
    for e in range(ITERS - 1):
        awaited(ex.at[e, pl.ds(0, 2 * REACH)], ssem.at[S_DIR + e])
    for hop in range(HOPS):
        for at in (S_RIGHT, S_LEFT):
            awaited(zs.at[0, pl.ds(0, mdev), :], ssem.at[at + hop])


def shards(ensemble, forcing, obs_cell, obs_value, obs_var, obs_noise):
    mdev, pdev, slab = ensemble.shape
    odev = obs_cell.shape[0]
    space_count = lax.axis_size("space")
    mem_count = lax.axis_size("mem")
    members = mdev * mem_count
    planes = pdev * space_count
    band = SLOTS * odev

    def call(*args):
        return kernel(space_count, mem_count, *args)

    vmem = pl.BlockSpec(memory_space=pltpu.VMEM)
    analysis = pl.pallas_call(
        call,
        out_shape=jax.ShapeDtypeStruct((pdev, mdev, slab), f32),
        in_specs=[vmem] * 6,
        out_specs=vmem,
        scratch_shapes=[
            pltpu.VMEM((planes, mdev // 2, 128), f32),
            pltpu.VMEM((planes, mdev // 2, 128), f32),
            pltpu.VMEM((space_count, pdev, 128), f32),
            pltpu.VMEM((pdev, members, slab), f32),
            pltpu.VMEM((pdev, members, slab), bf16),
            pltpu.VMEM((pdev, members, slab), bf16),
            pltpu.VMEM((pdev * slab, odev), bf16),
            pltpu.VMEM((SLOTS, members, odev), f32),
            pltpu.VMEM((members, band), bf16),
            pltpu.VMEM((members, band), bf16),
            pltpu.VMEM((SLOTS, mdev + 8, odev), f32),
            pltpu.VMEM((ITERS - 1, SLOTS, mdev, odev), f32),
            pltpu.VMEM((space_count, 8, odev), f32),
            pltpu.VMEM((odev, band), bf16),
            pltpu.VMEM((odev, band), bf16),
            pltpu.SemaphoreType.DMA((SENDS,)),
            pltpu.SemaphoreType.DMA((RECVS,)),
            pltpu.SemaphoreType.DMA((3,)),
        ],
        compiler_params=pltpu.CompilerParams(
            collective_id=0, has_side_effects=True, vmem_limit_bytes=32 * 1024 * 1024),
        name="cycle",
    )(
        jnp.transpose(ensemble, (1, 0, 2)), forcing, obs_cell[None, :], obs_value[None, :], obs_var[None, :],
        obs_noise,
    )
    return jnp.transpose(analysis, (1, 0, 2))


def solution(mesh):
    placed = (
        P("mem", "space", None),
        P("space", None),
        P("space"),
        P("space"),
        P("space"),
        P("mem", "space"),
    )
    return jax.shard_map(
        shards, mesh=mesh, in_specs=placed, out_specs=P("mem", "space", None), check_vma=False
    )
```

```python
import jax
import jax.numpy as jnp
from jax import lax
from jax.experimental import pallas as pl
from jax.experimental.pallas import tpu as pltpu
from jax.sharding import PartitionSpec as P

FSTEPS = 4
ITERS = 6
LOC = 16
REACH = 8
SLOTS = 2 * REACH + 1
MESH = pl.DeviceIdType.MESH
AWAY = (4, -4, 6, -6, 2, -2, 8, -8)
STEPS = (
    (2, 2), (2, 1), (1, 2), (2, 3), (3, 2), (1, 1), (3, 3), (1, 3),
    (3, 1), (2, 0), (0, 2), (1, 0), (0, 1), (3, 0), (0, 3), (0, 0),
)
f32 = jnp.float32
bf16 = jnp.bfloat16

HOPS = 7
R_OUT, R_FORC, R_BACK, R_BOUND = range(4)
R_RHS = 4
R_DIR = R_RHS + 2 * REACH
R_OBS = R_DIR + 2 * REACH * (ITERS - 1)
R_BAND = R_OBS + 8
R_RIGHT = R_BAND + SLOTS
R_LEFT = R_RIGHT + HOPS
RECVS = R_LEFT + HOPS
S_OUT, S_FORC, S_BACK, S_OBS, S_RHS, S_BAND, S_PAIR, S_BOUND = range(8)
S_DIR = 8
S_RIGHT = S_DIR + ITERS - 1
S_LEFT = S_RIGHT + HOPS
SENDS = S_LEFT + HOPS

NT = (((1,), (1,)), ((), ()))


def nn(a, b):
    return jnp.dot(a, b, preferred_element_type=f32)


def nt(a, b):
    return lax.dot_general(a, b, NT, preferred_element_type=f32)


def halves(x):
    high = x.astype(bf16)
    return high, (x - high.astype(f32)).astype(bf16)


def awaited(ref, sem):
    pltpu.make_async_copy(ref, ref, sem).wait()


def kernel(
    space_count, mem_count,
    ens, forc, cell, value, var, noise,
    out,
    r, t, fr, zs, sh, sl, oh, ab, ah, al, e0, ex, bb, ch, cl,
    ssem, rsem, lsem,
):
    me_s = lax.axis_index("space")
    me_m = lax.axis_index("mem")
    members = ab.shape[1]
    mdev = noise.shape[0]
    planes = r.shape[0]
    half = mdev // 2
    odev = cell.shape[1]
    slab = ens.shape[2]

    def chunk_of(index):
        return lax.div(index, 2), lax.rem(index, 2)

    def other(base, step, count):
        return lax.rem(base + step, count)

    my_c, my_h = chunk_of(me_s)
    side_y = 4
    side_x = space_count // 2 // side_y
    others = []
    for dx, dy in STEPS:
        chip = lax.rem(lax.div(my_c, side_y) + dx, side_x) * side_y + lax.rem(lax.rem(my_c, side_y) + dy, side_y)
        others.append(2 * chip + (1 - my_h))
        if (dx, dy) != (0, 0):
            others.append(2 * chip + my_h)

    barrier = pltpu.get_barrier_semaphore()

    def greet_space(i, c):
        pl.semaphore_signal(barrier, inc=1, device_id={"space": other(me_s, i, space_count)}, device_id_type=MESH)
        return c

    def greet_mem(i, c):
        pl.semaphore_signal(barrier, inc=1, device_id={"mem": other(me_m, i, mem_count)}, device_id_type=MESH)
        return c

    lax.fori_loop(1, space_count, greet_space, 0)
    lax.fori_loop(1, mem_count, greet_mem, 0)

    own_out = pltpu.make_async_copy(
        ens.at[:, pl.ds(pl.multiple_of(my_h * half, half), half), pl.ds(pl.multiple_of(my_c * 128, 128), 128)],
        r.at[pl.ds(me_s * 2, 2)], lsem.at[0])
    own_forc = pltpu.make_async_copy(
        forc.at[:, pl.ds(pl.multiple_of(my_c * 128, 128), 128)], fr.at[me_s], lsem.at[1])
    own_out.start()
    own_forc.start()

    pl.semaphore_wait(barrier, space_count + mem_count - 2)

    for to in others:
        tc, th = chunk_of(to)
        cells = pl.ds(pl.multiple_of(tc * 128, 128), 128)
        pltpu.make_async_remote_copy(
            src_ref=forc.at[:, cells], dst_ref=fr.at[me_s],
            send_sem=ssem.at[S_FORC], recv_sem=rsem.at[R_FORC],
            device_id={"space": to}, device_id_type=MESH).start()
        pltpu.make_async_remote_copy(
            src_ref=ens.at[:, pl.ds(pl.multiple_of(th * half, half), half), cells],
            dst_ref=r.at[pl.ds(me_s * 2, 2)],
            send_sem=ssem.at[S_OUT], recv_sem=rsem.at[R_OUT],
            device_id={"space": to}, device_id_type=MESH).start()

    cells_here = cell[...] - me_s * (2 * slab)

    def one_hot(i, c):
        rows = lax.broadcasted_iota(jnp.int32, (256, odev), 0) + i * 256
        oh[pl.ds(pl.multiple_of(i * 256, 256), 256), :] = jnp.where(rows == cells_here, 1.0, 0.0).astype(bf16)
        return c

    lax.fori_loop(0, 2 * slab // 256, one_hot, 0)

    own_out.wait()
    own_forc.wait()
    awaited(r.at[pl.ds(0, planes - 2)], rsem.at[R_OUT])
    awaited(fr.at[pl.ds(0, space_count - 1)], rsem.at[R_FORC])

    def advance(src, dst):
        def group(g, carry):
            two, one, now = carry
            for i in range(8):
                x = g * 8 + i
                ahead = src[lax.rem(x + 1, planes)]
                force = fr[g * 4 + i // 2, pl.ds(i % 2, 1), :]
                dst[x] = now + 0.05 * ((ahead - two) * one - now + force)
                two, one, now = one, now, ahead
            return two, one, now

        lax.fori_loop(0, planes // 8, group, (src[planes - 2], src[planes - 1], src[0]))

    for step in range(FSTEPS // 2):
        advance(r, t)
        advance(t, r)

    mine = pl.ds(pl.multiple_of(me_m * mdev, mdev), mdev)
    my_rows = pl.ds(pl.multiple_of(me_m * mdev + my_h * half, half), half)
    my_cells = pl.ds(pl.multiple_of(my_c * 128, 128), 128)

    for to in others:
        pltpu.make_async_remote_copy(
            src_ref=r.at[pl.ds(to * 2, 2)], dst_ref=zs.at[:, my_rows, my_cells],
            send_sem=ssem.at[S_BACK], recv_sem=rsem.at[R_BACK],
            device_id={"space": to}, device_id_type=MESH).start()
    own_back = pltpu.make_async_copy(r.at[pl.ds(me_s * 2, 2)], zs.at[:, my_rows, my_cells], lsem.at[2])
    own_back.start()
    own_back.wait()
    awaited(r.at[pl.ds(0, planes - 2)], rsem.at[R_BACK])

    observed = jnp.zeros((3 * mdev, odev), f32)
    for x in range(2):
        block = zs[x, mine, :]
        first = block.astype(bf16)
        rest = block - first.astype(f32)
        second = rest.astype(bf16)
        third = (rest - second.astype(f32)).astype(bf16)
        pieces = jnp.concatenate([first, second, third], axis=0)
        observed = observed + nn(pieces, oh[x * slab:(x + 1) * slab, :])
    observed = observed[:mdev] + observed[mdev:2 * mdev] + observed[2 * mdev:]
    ab[REACH, mine, :] = observed

    def send_obs(i, c):
        pltpu.make_async_remote_copy(
            src_ref=ab.at[REACH, mine], dst_ref=ab.at[REACH, mine],
            send_sem=ssem.at[S_OBS], recv_sem=rsem.at[R_OBS + i],
            device_id={"mem": other(me_m, i, mem_count)}, device_id_type=MESH).start()
        return c

    lax.fori_loop(1, mem_count, send_obs, 0)

    right = other(me_m, 1, mem_count)
    left = other(me_m, mem_count - 1, mem_count)

    def relay(hop):
        for way in (1, -1):
            origin = lax.rem(me_m + mem_count - way * (hop // 2), mem_count)
            x = hop % 2 if way > 0 else 1 - hop % 2
            ref = zs.at[x, pl.ds(pl.multiple_of(origin * mdev, mdev), mdev), :]
            pltpu.make_async_remote_copy(
                src_ref=ref, dst_ref=ref,
                send_sem=ssem.at[(S_RIGHT if way > 0 else S_LEFT) + hop],
                recv_sem=rsem.at[(R_RIGHT if way > 0 else R_LEFT) + hop],
                device_id={"mem": right if way > 0 else left}, device_id_type=MESH).start()

    def relayed(hop):
        for base in (R_RIGHT, R_LEFT):
            awaited(zs.at[0, pl.ds(0, mdev), :], rsem.at[base + hop])

    plane_row = jnp.floor(cell[...].astype(f32) / slab)
    rhs = jnp.sqrt(var[...]) * noise[...] + value[...] - observed
    own = 2 * REACH
    e0[own, :mdev, :] = rhs
    e0[own, mdev:, :] = jnp.broadcast_to(plane_row, (8, odev))

    turn = 1 - 2 * my_h
    partner = {"space": me_s + turn}
    out_of_reach = REACH - 1 - my_h
    band_to = [{"space": lax.rem(me_s + away + space_count, space_count)} for away in AWAY]

    def spread(at, send, recv):
        def copy(there, to):
            pltpu.make_async_remote_copy(
                src_ref=at(own), dst_ref=at(there), send_sem=ssem.at[send], recv_sem=rsem.at[recv + there],
                device_id=to, device_id_type=MESH).start()

        for i, to in enumerate(band_to):
            copy(i ^ 1, to)
        copy(REACH + out_of_reach, partner)

    def hand_over(at, send, recv):
        def copy(i):
            pltpu.make_async_remote_copy(
                src_ref=at(i), dst_ref=at(REACH + i), send_sem=ssem.at[send], recv_sem=rsem.at[recv + REACH + i],
                device_id=partner, device_id_type=MESH).start()

        for i in range(REACH - 2):
            awaited(at(i), rsem.at[recv + i])
            copy(i)
        for i in range(REACH - 2, REACH):
            awaited(at(i), rsem.at[recv + i])
        copy(2 * REACH - 3 - out_of_reach)

    def handed(at, recv):
        for i in range(REACH, 2 * REACH):
            awaited(at(i), rsem.at[recv + i])

    def rhs_at(i):
        return e0.at[i]

    spread(rhs_at, S_RHS, R_RHS)

    near = (1, -1, 4, -4)
    chips_at = {chips: {"space": lax.rem(me_s + 2 * chips + space_count, space_count)}
                for chips in near}

    def piece_rows(step):
        origin = lax.rem(me_m + mem_count - step, mem_count)
        return pl.ds(pl.multiple_of(origin * mdev, mdev), mdev)

    def piece_send(slot, there, rows, chips):
        pltpu.make_async_remote_copy(
            src_ref=ab.at[slot, rows], dst_ref=ab.at[there, rows],
            send_sem=ssem.at[S_BAND], recv_sem=rsem.at[R_BAND + there],
            device_id=chips_at[chips], device_id_type=MESH).start()

    def to_chips(step):
        rows = piece_rows(step)
        for chips in near:
            piece_send(REACH, REACH - 2 * chips, rows, chips)

    def piece_here(step):
        awaited(ab.at[REACH, pl.ds(0, mdev)], rsem.at[R_OBS + step])

    to_chips(0)
    relay(0)
    relay(1)
    for step in (1, 7, 2, 6, 3, 5, 4):
        piece_here(step)
        to_chips(step)
    hand_over(rhs_at, S_RHS, R_RHS)

    def pair_send(e):
        pltpu.make_async_remote_copy(
            src_ref=ab.at[REACH + turn * e], dst_ref=ab.at[REACH + turn * (e - 1)],
            send_sem=ssem.at[S_PAIR], recv_sem=rsem.at[R_BAND + REACH + turn * (e - 1)],
            device_id=partner, device_id_type=MESH).start()

    def slot_here(j):
        awaited(ab.at[0], rsem.at[R_BAND + j])

    pair_send(0)

    def anomalies(j):
        raw = ab[j]
        return raw - jnp.sum(raw, axis=0, keepdims=True) / members

    anom_t = anomalies(REACH).T
    th, tl = halves(anom_t)
    both_t = jnp.concatenate([th, tl], axis=0)
    own_plane = jnp.broadcast_to(plane_row, (odev, odev)).T
    own_var = jnp.broadcast_to(var[...], (odev, odev)).T
    diagonal = (lax.broadcasted_iota(jnp.int32, (odev, odev), 0) == lax.broadcasted_iota(jnp.int32, (odev, odev), 1))
    diag_var = jnp.where(diagonal, own_var, 0.0)

    def taper(a, b):
        spread = jnp.abs(a - b)
        spread = jnp.minimum(spread, planes - spread)
        return jnp.maximum(0.0, 1.0 - spread / LOC)

    def rows_of(j, place, carry, more=None):
        total, image = carry
        lanes = pl.ds(pl.multiple_of(place * odev, odev), odev)
        high, low = halves(anomalies(j))
        ah[:, lanes] = high
        al[:, lanes] = low
        gram = nn(both_t, high)
        gram = gram[:odev] + gram[odev:] + nn(th, low)
        block = taper(own_plane, e0[place, pl.ds(mdev, 1), :]) * gram / (members - 1)
        if more is not None:
            block = block + more
        chigh, clow = halves(block)
        ch[:, lanes] = chigh
        cl[:, lanes] = clow
        dhigh, dlow = halves(e0[place, pl.ds(0, mdev), :])
        top = nt(jnp.concatenate([dhigh, dlow], axis=0), chigh)
        return total + jnp.abs(block), image + (top[:mdev] + top[mdev:] + nt(dhigh, clow))

    total = rows_of(REACH, own, (jnp.zeros((odev, odev), f32), jnp.zeros((mdev, odev), f32)), diag_var)

    for side in (1, -1):
        slot = REACH + 2 * side
        slot_here(slot)
        for chips in (-side, 4 * side):
            piece_send(slot, slot - 2 * chips, slice(None), chips)
    pair_send(2)
    pair_send(-2)
    relayed(0)
    relay(2)
    handed(rhs_at, R_RHS)

    def pick(i, table):
        value = table[0]
        for k in range(1, len(table)):
            value = jnp.where(i == k, table[k], value)
        return value

    def place(rank, negative):
        return 2 * rank + my_h + negative - 2 * my_h * negative

    def slot_rows(e, rank, negative, total):
        return rows_of(REACH + turn * e, place(rank, negative), total)

    def from_partner(e, rank, negative, total):
        slot_here(REACH + turn * (1 - e))
        return rows_of(REACH + turn * (1 - e), REACH + place(rank, 1 - negative), total)

    total = slot_rows(2, 2, 0, total)
    total = slot_rows(-2, 2, 1, total)
    total = from_partner(0, 3, 1, total)

    def two_slots(i, total):
        e = pick(i, (8, 4, -4, 6, -6))
        slot_here(REACH + turn * e)
        pair_send(e)
        total = slot_rows(e, pick(i, (3, 0, 0, 1, 1)), pick(i, (0, 0, 1, 0, 1)), total)
        return from_partner(
            pick(i, (2, -2, 8, 4, -4)), pick(i, (2, 2, 3, 0, 0)), pick(i, (0, 1, 0, 0, 1)), total)

    total = lax.fori_loop(0, 2, two_slots, total)
    relayed(1)
    relay(3)
    total = lax.fori_loop(2, 5, two_slots, total)
    slot_here(REACH - turn * REACH)
    total = slot_rows(-REACH, 3, 1, total)

    def last_two(i, total):
        return from_partner(pick(i, (6, -6)), 1, i, total)

    total, first_image = lax.fori_loop(0, 2, last_two, total)

    def part(block, lanes):
        high, low = halves(block)
        top = nt(jnp.concatenate([high, low], axis=0), ch[:, lanes])
        return top[:mdev] + top[mdev:] + nt(high, cl[:, lanes])

    own_lanes = slice(own * odev, (own + 1) * odev)
    halves_of_band = ((0, REACH), (REACH, 2 * REACH))

    def at_of(e):
        return lambda i: ex.at[e, i]

    def exchange(e, block):
        ex[e, own] = block
        spread(at_of(e), S_DIR + e, R_DIR + 2 * REACH * e)

    def arrived(e):
        def group(g):
            recv = R_DIR + 2 * REACH * e
            if g == 0:
                hand_over(at_of(e), S_DIR + e, recv)
            else:
                handed(at_of(e), recv)
            return jnp.concatenate([ex[e, i] for i in range(*halves_of_band[g])], axis=1)

        return group

    def lanes_of(g):
        return slice(halves_of_band[g][0] * odev, halves_of_band[g][1] * odev)

    def image_of(block, group):
        image = part(block, own_lanes)
        for g in range(2):
            image = image + part(group(g), lanes_of(g))
        return image

    exchange(0, first_image)

    row_max = jnp.max(jnp.sum(total, axis=1, keepdims=True), axis=0, keepdims=True)
    var_min = jnp.min(var[...], axis=1, keepdims=True)
    is_upper = lax.broadcasted_iota(jnp.int32, (8, odev), 0) < 4
    bb[me_s] = jnp.where(is_upper, row_max, -var_min)

    for to in others:
        pltpu.make_async_remote_copy(
            src_ref=bb.at[me_s], dst_ref=bb.at[me_s],
            send_sem=ssem.at[S_BOUND], recv_sem=rsem.at[R_BOUND],
            device_id={"space": to}, device_id_type=MESH).start()
    relayed(2)
    relay(4)

    second_image = image_of(first_image, arrived(0))
    relayed(3)
    relay(5)

    awaited(bb.at[pl.ds(0, space_count - 1)], rsem.at[R_BOUND])
    bounds = jnp.max(bb[...], axis=0)
    upper = bounds[0:1, :]
    lower = -bounds[4:5, :]
    center = (upper + lower) / 2.0
    radius = (upper - lower) / 2.0
    sigma = center / radius
    rho = 1.0 / sigma
    direction = rhs / center
    weight = direction
    residual = rhs - first_image / center
    rho_next = 1.0 / (2.0 * sigma - rho)
    keep, take = rho_next * rho, 2.0 * rho_next / radius
    image = keep * (first_image / center) + take * (first_image - second_image / center)
    direction = keep * direction + take * residual
    rho = rho_next
    weight = weight + direction

    for e in range(1, ITERS - 2):
        residual = residual - image
        rho_next = 1.0 / (2.0 * sigma - rho)
        direction = rho_next * rho * direction + 2.0 * rho_next / radius * residual
        rho = rho_next
        weight = weight + direction
        exchange(e, direction)
        image = image_of(direction, arrived(e))
        if e == 1:
            relayed(4)
            relay(6)
    residual = residual - image
    rho_next = 1.0 / (2.0 * sigma - rho)
    direction = rho_next * rho * direction + 2.0 * rho_next / radius * residual
    weight = weight + direction
    last = ITERS - 2
    exchange(last, weight)

    relayed(HOPS - 2)
    relayed(HOPS - 1)
    width = 512

    def split_states(i, c):
        x = lax.div(i, slab // width)
        lanes = pl.ds(pl.multiple_of(lax.rem(i, slab // width) * width, width), width)
        states = zs[x, :, lanes]
        high, low = halves(states - jnp.sum(states, axis=0, keepdims=True) / members)
        sh[x, :, lanes] = high
        sl[x, :, lanes] = low
        return c

    lax.fori_loop(0, 2 * slab // width, split_states, 0)

    base = me_s.astype(f32) * 2.0

    def gain_part(block, row, lanes):
        wide = jnp.concatenate([block * taper(base, row), block * taper(base + 1.0, row)], axis=0)
        high, low = halves(wide)
        top = nt(jnp.concatenate([high, low], axis=0), ah[:, lanes])
        return top[:2 * mdev] + top[2 * mdev:] + nt(high, al[:, lanes])

    gain = gain_part(weight, plane_row, own_lanes)
    group = arrived(last)
    for g in range(2):
        rows = jnp.concatenate([e0[i, pl.ds(mdev, 1), :] for i in range(*halves_of_band[g])], axis=1)
        gain = gain + gain_part(group(g), rows, lanes_of(g))
    gain = gain / (members - 1)

    for x in range(2):
        ghigh, glow = halves(gain[x * mdev:(x + 1) * mdev])
        gboth = jnp.concatenate([ghigh, glow], axis=0)

        def update(i, c, x=x, ghigh=ghigh, gboth=gboth):
            lanes = pl.ds(pl.multiple_of(i * width, width), width)
            top = nn(gboth, sh[x, :, lanes])
            out[x, :, lanes] = zs[x, mine, lanes] + (top[:mdev] + top[mdev:] + nn(ghigh, sl[x, :, lanes]))
            return c

        lax.fori_loop(0, slab // width, update, 0)

    awaited(r.at[pl.ds(0, planes - 2)], ssem.at[S_OUT])
    awaited(fr.at[pl.ds(0, space_count - 1)], ssem.at[S_FORC])
    awaited(r.at[pl.ds(0, planes - 2)], ssem.at[S_BACK])
    awaited(ab.at[0, pl.ds(0, members - mdev)], ssem.at[S_OBS])
    awaited(e0.at[pl.ds(0, 2 * REACH)], ssem.at[S_RHS])
    awaited(ab.at[pl.ds(0, REACH)], ssem.at[S_BAND])
    awaited(ab.at[pl.ds(0, REACH)], ssem.at[S_PAIR])
    awaited(bb.at[pl.ds(0, space_count - 1)], ssem.at[S_BOUND])
    for e in range(ITERS - 1):
        awaited(ex.at[e, pl.ds(0, 2 * REACH)], ssem.at[S_DIR + e])
    for hop in range(HOPS):
        for at in (S_RIGHT, S_LEFT):
            awaited(zs.at[0, pl.ds(0, mdev), :], ssem.at[at + hop])


def shards(ensemble, forcing, obs_cell, obs_value, obs_var, obs_noise):
    mdev, pdev, slab = ensemble.shape
    odev = obs_cell.shape[0]
    space_count = lax.axis_size("space")
    mem_count = lax.axis_size("mem")
    members = mdev * mem_count
    planes = pdev * space_count
    band = SLOTS * odev

    def call(*args):
        return kernel(space_count, mem_count, *args)

    vmem = pl.BlockSpec(memory_space=pltpu.VMEM)
    analysis = pl.pallas_call(
        call,
        out_shape=jax.ShapeDtypeStruct((pdev, mdev, slab), f32),
        in_specs=[vmem] * 6,
        out_specs=vmem,
        scratch_shapes=[
            pltpu.VMEM((planes, mdev // 2, 128), f32),
            pltpu.VMEM((planes, mdev // 2, 128), f32),
            pltpu.VMEM((space_count, pdev, 128), f32),
            pltpu.VMEM((pdev, members, slab), f32),
            pltpu.VMEM((pdev, members, slab), bf16),
            pltpu.VMEM((pdev, members, slab), bf16),
            pltpu.VMEM((pdev * slab, odev), bf16),
            pltpu.VMEM((SLOTS, members, odev), f32),
            pltpu.VMEM((members, band), bf16),
            pltpu.VMEM((members, band), bf16),
            pltpu.VMEM((SLOTS, mdev + 8, odev), f32),
            pltpu.VMEM((ITERS - 1, SLOTS, mdev, odev), f32),
            pltpu.VMEM((space_count, 8, odev), f32),
            pltpu.VMEM((odev, band), bf16),
            pltpu.VMEM((odev, band), bf16),
            pltpu.SemaphoreType.DMA((SENDS,)),
            pltpu.SemaphoreType.DMA((RECVS,)),
            pltpu.SemaphoreType.DMA((3,)),
        ],
        compiler_params=pltpu.CompilerParams(
            collective_id=0, has_side_effects=True, vmem_limit_bytes=32 * 1024 * 1024),
        name="cycle",
    )(
        jnp.transpose(ensemble, (1, 0, 2)), forcing, obs_cell[None, :], obs_value[None, :], obs_var[None, :],
        obs_noise,
    )
    return jnp.transpose(analysis, (1, 0, 2))


def solution(mesh):
    placed = (
        P("mem", "space", None),
        P("space", None),
        P("space"),
        P("space"),
        P("space"),
        P("mem", "space"),
    )
    return jax.shard_map(
        shards, mesh=mesh, in_specs=placed, out_specs=P("mem", "space", None), check_vma=False
    )
```

```python
import jax
import jax.numpy as jnp
from jax import lax
from jax.experimental import pallas as pl
from jax.experimental.pallas import tpu as pltpu
from jax.sharding import PartitionSpec as P

FSTEPS = 4
ITERS = 6
LOC = 16
REACH = 8
SLOTS = 2 * REACH + 1
MESH = pl.DeviceIdType.MESH
AWAY = (4, -4, 6, -6, 2, -2, 8, -8)
STEPS = (
    (2, 2), (2, 1), (1, 2), (2, 3), (3, 2), (1, 1), (3, 3), (1, 3),
    (3, 1), (2, 0), (0, 2), (1, 0), (0, 1), (3, 0), (0, 3), (0, 0),
)
f32 = jnp.float32
bf16 = jnp.bfloat16

HOPS = 7
R_OUT, R_FORC, R_BACK, R_BOUND = range(4)
R_RHS = 4
R_DIR = R_RHS + 2 * REACH
R_OBS = R_DIR + ITERS - 1
R_BAND = R_OBS + 8
R_RIGHT = R_BAND + SLOTS
R_LEFT = R_RIGHT + HOPS
RECVS = R_LEFT + HOPS
S_OUT, S_FORC, S_BACK, S_OBS, S_RHS, S_BAND, S_PAIR, S_BOUND = range(8)
S_DIR = 8
S_RIGHT = S_DIR + ITERS - 1
S_LEFT = S_RIGHT + HOPS
SENDS = S_LEFT + HOPS

NT = (((1,), (1,)), ((), ()))


def nn(a, b):
    return jnp.dot(a, b, preferred_element_type=f32)


def nt(a, b):
    return lax.dot_general(a, b, NT, preferred_element_type=f32)


def halves(x):
    high = x.astype(bf16)
    return high, (x - high.astype(f32)).astype(bf16)


def awaited(ref, sem):
    pltpu.make_async_copy(ref, ref, sem).wait()


def kernel(
    space_count, mem_count,
    ens, forc, cell, value, var, noise,
    out,
    r, t, fr, zs, sh, sl, oh, ab, ah, al, e0, ex, bb, ch, cl, dh,
    ssem, rsem, lsem,
):
    me_s = lax.axis_index("space")
    me_m = lax.axis_index("mem")
    members = ab.shape[1]
    mdev = noise.shape[0]
    planes = r.shape[0]
    half = mdev // 2
    odev = cell.shape[1]
    slab = ens.shape[2]

    def chunk_of(index):
        return lax.div(index, 2), lax.rem(index, 2)

    def other(base, step, count):
        return lax.rem(base + step, count)

    my_c, my_h = chunk_of(me_s)
    side_y = 4
    side_x = space_count // 2 // side_y
    others = []
    for dx, dy in STEPS:
        chip = lax.rem(lax.div(my_c, side_y) + dx, side_x) * side_y + lax.rem(lax.rem(my_c, side_y) + dy, side_y)
        others.append(2 * chip + (1 - my_h))
        if (dx, dy) != (0, 0):
            others.append(2 * chip + my_h)

    barrier = pltpu.get_barrier_semaphore()

    def greet_space(i, c):
        pl.semaphore_signal(barrier, inc=1, device_id={"space": other(me_s, i, space_count)}, device_id_type=MESH)
        return c

    def greet_mem(i, c):
        pl.semaphore_signal(barrier, inc=1, device_id={"mem": other(me_m, i, mem_count)}, device_id_type=MESH)
        return c

    lax.fori_loop(1, space_count, greet_space, 0)
    lax.fori_loop(1, mem_count, greet_mem, 0)

    own_out = pltpu.make_async_copy(
        ens.at[:, pl.ds(pl.multiple_of(my_h * half, half), half), pl.ds(pl.multiple_of(my_c * 128, 128), 128)],
        r.at[pl.ds(me_s * 2, 2)], lsem.at[0])
    own_forc = pltpu.make_async_copy(
        forc.at[:, pl.ds(pl.multiple_of(my_c * 128, 128), 128)], fr.at[me_s], lsem.at[1])
    own_out.start()
    own_forc.start()

    pl.semaphore_wait(barrier, space_count + mem_count - 2)

    for to in others:
        tc, th = chunk_of(to)
        cells = pl.ds(pl.multiple_of(tc * 128, 128), 128)
        pltpu.make_async_remote_copy(
            src_ref=forc.at[:, cells], dst_ref=fr.at[me_s],
            send_sem=ssem.at[S_FORC], recv_sem=rsem.at[R_FORC],
            device_id={"space": to}, device_id_type=MESH).start()
        pltpu.make_async_remote_copy(
            src_ref=ens.at[:, pl.ds(pl.multiple_of(th * half, half), half), cells],
            dst_ref=r.at[pl.ds(me_s * 2, 2)],
            send_sem=ssem.at[S_OUT], recv_sem=rsem.at[R_OUT],
            device_id={"space": to}, device_id_type=MESH).start()

    cells_here = cell[...] - me_s * (2 * slab)

    def one_hot(i, c):
        rows = lax.broadcasted_iota(jnp.int32, (256, odev), 0) + i * 256
        oh[pl.ds(pl.multiple_of(i * 256, 256), 256), :] = jnp.where(rows == cells_here, 1.0, 0.0).astype(bf16)
        return c

    lax.fori_loop(0, 2 * slab // 256, one_hot, 0)

    own_out.wait()
    own_forc.wait()
    awaited(r.at[pl.ds(0, planes - 2)], rsem.at[R_OUT])
    awaited(fr.at[pl.ds(0, space_count - 1)], rsem.at[R_FORC])

    def advance(src, dst):
        def group(g, carry):
            two, one, now = carry
            for i in range(8):
                x = g * 8 + i
                ahead = src[lax.rem(x + 1, planes)]
                force = fr[g * 4 + i // 2, pl.ds(i % 2, 1), :]
                dst[x] = now + 0.05 * ((ahead - two) * one - now + force)
                two, one, now = one, now, ahead
            return two, one, now

        lax.fori_loop(0, planes // 8, group, (src[planes - 2], src[planes - 1], src[0]))

    for step in range(FSTEPS // 2):
        advance(r, t)
        advance(t, r)

    mine = pl.ds(pl.multiple_of(me_m * mdev, mdev), mdev)
    my_rows = pl.ds(pl.multiple_of(me_m * mdev + my_h * half, half), half)
    my_cells = pl.ds(pl.multiple_of(my_c * 128, 128), 128)

    for to in others:
        pltpu.make_async_remote_copy(
            src_ref=r.at[pl.ds(to * 2, 2)], dst_ref=zs.at[:, my_rows, my_cells],
            send_sem=ssem.at[S_BACK], recv_sem=rsem.at[R_BACK],
            device_id={"space": to}, device_id_type=MESH).start()
    own_back = pltpu.make_async_copy(r.at[pl.ds(me_s * 2, 2)], zs.at[:, my_rows, my_cells], lsem.at[2])
    own_back.start()
    own_back.wait()
    awaited(r.at[pl.ds(0, planes - 2)], rsem.at[R_BACK])

    observed = jnp.zeros((3 * mdev, odev), f32)
    for x in range(2):
        block = zs[x, mine, :]
        first = block.astype(bf16)
        rest = block - first.astype(f32)
        second = rest.astype(bf16)
        third = (rest - second.astype(f32)).astype(bf16)
        pieces = jnp.concatenate([first, second, third], axis=0)
        observed = observed + nn(pieces, oh[x * slab:(x + 1) * slab, :])
    observed = observed[:mdev] + observed[mdev:2 * mdev] + observed[2 * mdev:]
    ab[REACH, mine, :] = observed

    def send_obs(i, c):
        pltpu.make_async_remote_copy(
            src_ref=ab.at[REACH, mine], dst_ref=ab.at[REACH, mine],
            send_sem=ssem.at[S_OBS], recv_sem=rsem.at[R_OBS + i],
            device_id={"mem": other(me_m, i, mem_count)}, device_id_type=MESH).start()
        return c

    lax.fori_loop(1, mem_count, send_obs, 0)

    right = other(me_m, 1, mem_count)
    left = other(me_m, mem_count - 1, mem_count)

    def relay(hop):
        for way in (1, -1):
            origin = lax.rem(me_m + mem_count - way * (hop // 2), mem_count)
            x = hop % 2 if way > 0 else 1 - hop % 2
            ref = zs.at[x, pl.ds(pl.multiple_of(origin * mdev, mdev), mdev), :]
            pltpu.make_async_remote_copy(
                src_ref=ref, dst_ref=ref,
                send_sem=ssem.at[(S_RIGHT if way > 0 else S_LEFT) + hop],
                recv_sem=rsem.at[(R_RIGHT if way > 0 else R_LEFT) + hop],
                device_id={"mem": right if way > 0 else left}, device_id_type=MESH).start()

    def relayed(hop):
        for base in (R_RIGHT, R_LEFT):
            awaited(zs.at[0, pl.ds(0, mdev), :], rsem.at[base + hop])

    plane_row = jnp.floor(cell[...].astype(f32) / slab)
    rhs = jnp.sqrt(var[...]) * noise[...] + value[...] - observed
    own = 2 * REACH
    e0[own, :mdev, :] = rhs
    e0[own, mdev:, :] = jnp.broadcast_to(plane_row, (8, odev))

    turn = 1 - 2 * my_h
    partner = {"space": me_s + turn}
    out_of_reach = REACH - 1 - my_h
    band_to = [{"space": lax.rem(me_s + away + space_count, space_count)} for away in AWAY]

    def spread(at, send, recv):
        def copy(there, to):
            pltpu.make_async_remote_copy(
                src_ref=at(own), dst_ref=at(there), send_sem=ssem.at[send], recv_sem=rsem.at[recv + there],
                device_id=to, device_id_type=MESH).start()

        for i, to in enumerate(band_to):
            copy(i ^ 1, to)
        copy(REACH + out_of_reach, partner)

    def hand_over(at, send, recv):
        def copy(i):
            pltpu.make_async_remote_copy(
                src_ref=at(i), dst_ref=at(REACH + i), send_sem=ssem.at[send], recv_sem=rsem.at[recv + REACH + i],
                device_id=partner, device_id_type=MESH).start()

        for i in range(REACH - 2):
            awaited(at(i), rsem.at[recv + i])
            copy(i)
        for i in range(REACH - 2, REACH):
            awaited(at(i), rsem.at[recv + i])
        copy(2 * REACH - 3 - out_of_reach)

    def handed(at, recv):
        for i in range(REACH, 2 * REACH):
            awaited(at(i), rsem.at[recv + i])

    def rhs_at(i):
        return e0.at[i]

    spread(rhs_at, S_RHS, R_RHS)

    near = (1, -1, 4, -4)
    chips_at = {chips: {"space": lax.rem(me_s + 2 * chips + space_count, space_count)}
                for chips in near}

    def piece_rows(step):
        origin = lax.rem(me_m + mem_count - step, mem_count)
        return pl.ds(pl.multiple_of(origin * mdev, mdev), mdev)

    def piece_send(slot, there, rows, chips):
        pltpu.make_async_remote_copy(
            src_ref=ab.at[slot, rows], dst_ref=ab.at[there, rows],
            send_sem=ssem.at[S_BAND], recv_sem=rsem.at[R_BAND + there],
            device_id=chips_at[chips], device_id_type=MESH).start()

    def to_chips(step):
        rows = piece_rows(step)
        for chips in near:
            piece_send(REACH, REACH - 2 * chips, rows, chips)

    def piece_here(step):
        awaited(ab.at[REACH, pl.ds(0, mdev)], rsem.at[R_OBS + step])

    to_chips(0)
    relay(0)
    relay(1)
    for step in (1, 7, 2, 6, 3, 5, 4):
        piece_here(step)
        to_chips(step)
    hand_over(rhs_at, S_RHS, R_RHS)

    def pair_send(e):
        pltpu.make_async_remote_copy(
            src_ref=ab.at[REACH + turn * e], dst_ref=ab.at[REACH + turn * (e - 1)],
            send_sem=ssem.at[S_PAIR], recv_sem=rsem.at[R_BAND + REACH + turn * (e - 1)],
            device_id=partner, device_id_type=MESH).start()

    def slot_here(j):
        awaited(ab.at[0], rsem.at[R_BAND + j])

    pair_send(0)

    def anomalies(j):
        raw = ab[j]
        return raw - jnp.sum(raw, axis=0, keepdims=True) / members

    anom_t = anomalies(REACH).T
    th, tl = halves(anom_t)
    both_t = jnp.concatenate([th, tl], axis=0)
    own_plane = jnp.broadcast_to(plane_row, (odev, odev)).T
    own_var = jnp.broadcast_to(var[...], (odev, odev)).T
    diagonal = (lax.broadcasted_iota(jnp.int32, (odev, odev), 0) == lax.broadcasted_iota(jnp.int32, (odev, odev), 1))
    diag_var = jnp.where(diagonal, own_var, 0.0)

    def taper(a, b):
        spread = jnp.abs(a - b)
        spread = jnp.minimum(spread, planes - spread)
        return jnp.maximum(0.0, 1.0 - spread / LOC)

    def rows_of(j, place, total, more=None):
        lanes = pl.ds(pl.multiple_of(place * odev, odev), odev)
        high, low = halves(anomalies(j))
        ah[:, lanes] = high
        al[:, lanes] = low
        gram = nn(both_t, high)
        gram = gram[:odev] + gram[odev:] + nn(th, low)
        block = taper(own_plane, e0[place, pl.ds(mdev, 1), :]) * gram / (members - 1)
        if more is not None:
            block = block + more
        chigh, clow = halves(block)
        ch[:, lanes] = chigh
        cl[:, lanes] = clow
        return total + jnp.abs(block)

    total = rows_of(REACH, own, jnp.zeros((odev, odev), f32), diag_var)

    for side in (1, -1):
        slot = REACH + 2 * side
        slot_here(slot)
        for chips in (-side, 4 * side):
            piece_send(slot, slot - 2 * chips, slice(None), chips)
    pair_send(2)
    pair_send(-2)
    handed(rhs_at, R_RHS)

    def pick(i, table):
        value = table[0]
        for k in range(1, len(table)):
            value = jnp.where(i == k, table[k], value)
        return value

    def place(rank, negative):
        return 2 * rank + my_h + negative - 2 * my_h * negative

    def slot_rows(e, rank, negative, total):
        return rows_of(REACH + turn * e, place(rank, negative), total)

    def partner_rows(e, rank, negative, total):
        return rows_of(REACH + turn * (1 - e), REACH + place(rank, 1 - negative), total)

    total = slot_rows(2, 2, 0, total)
    total = slot_rows(-2, 2, 1, total)

    def two_slots(i, total):
        e = pick(i, (8, 4, -4, 6, -6))
        f = pick(i, (0, 2, -2, 8, 4))
        slot_here(REACH + turn * e)
        pair_send(e)
        slot_here(REACH + turn * (1 - f))
        total = slot_rows(e, pick(i, (3, 0, 0, 1, 1)), pick(i, (0, 0, 1, 0, 1)), total)
        return partner_rows(f, pick(i, (3, 2, 2, 3, 0)), pick(i, (1, 0, 1, 0, 0)), total)

    total = lax.fori_loop(0, 1, two_slots, total)
    for hop in (0, 1):
        relayed(hop)
        relay(hop + 2)
    total = lax.fori_loop(1, 5, two_slots, total)
    slot_here(REACH - turn * REACH)
    slot_here(REACH + turn * (1 + 4))
    total = slot_rows(-REACH, 3, 1, total)
    total = partner_rows(-4, 0, 1, total)
    slot_here(REACH + turn * (1 - 6))
    slot_here(REACH + turn * (1 + 6))
    total = partner_rows(6, 1, 0, total)
    total = partner_rows(-6, 1, 1, total)

    def part(block, lanes):
        high, low = halves(block)
        top = nt(jnp.concatenate([high, low], axis=0), ch[:, lanes])
        return top[:mdev] + top[mdev:] + nt(high, cl[:, lanes])

    own_lanes = slice(own * odev, (own + 1) * odev)
    lanes_out = slice(0, own * odev)

    def exchange(e, block):
        ex[e, own] = block

        def copy(there, to):
            pltpu.make_async_remote_copy(
                src_ref=ex.at[e, own], dst_ref=ex.at[e, there],
                send_sem=ssem.at[S_DIR + e], recv_sem=rsem.at[R_DIR + e],
                device_id=to, device_id_type=MESH).start()

        for i, to in enumerate(band_to):
            copy(i ^ 1, to)
            if i < REACH - 2:
                copy(REACH + (i ^ 1), {"space": lax.rem(me_s + AWAY[i] + turn + space_count, space_count)})
        copy(3 * REACH - 3 - out_of_reach,
             {"space": lax.rem(me_s - (REACH - 1) * turn + space_count, space_count)})
        copy(REACH + out_of_reach, partner)

    def arrived(e):
        awaited(ex.at[e, pl.ds(0, own)], rsem.at[R_DIR + e])
        return lambda i: ex[e, i]

    def image_of(block, values_of):
        image = part(block, own_lanes)
        values = values_of()
        for i in range(own):
            high, low = halves(values(i))
            dh[:mdev, i * odev:(i + 1) * odev] = high
            dh[mdev:, i * odev:(i + 1) * odev] = low
        top = nt(dh[...], ch[:, lanes_out])
        return image + (top[:mdev] + top[mdev:] + nt(dh[:mdev, :], cl[:, lanes_out]))

    row_max = jnp.max(jnp.sum(total, axis=1, keepdims=True), axis=0, keepdims=True)
    var_min = jnp.min(var[...], axis=1, keepdims=True)
    is_upper = lax.broadcasted_iota(jnp.int32, (8, odev), 0) < 4
    bb[me_s] = jnp.where(is_upper, row_max, -var_min)

    for to in others:
        pltpu.make_async_remote_copy(
            src_ref=bb.at[me_s], dst_ref=bb.at[me_s],
            send_sem=ssem.at[S_BOUND], recv_sem=rsem.at[R_BOUND],
            device_id={"space": to}, device_id_type=MESH).start()

    first_image = image_of(rhs, lambda: lambda i: e0[i, pl.ds(0, mdev), :])
    exchange(0, first_image)
    second_image = image_of(first_image, lambda: arrived(0))

    awaited(bb.at[pl.ds(0, space_count - 1)], rsem.at[R_BOUND])
    bounds = jnp.max(bb[...], axis=0)
    upper = bounds[0:1, :]
    lower = -bounds[4:5, :]
    center = (upper + lower) / 2.0
    radius = (upper - lower) / 2.0
    sigma = center / radius
    rho = 1.0 / sigma
    direction = rhs / center
    weight = direction
    residual = rhs - first_image / center
    rho_next = 1.0 / (2.0 * sigma - rho)
    keep, take = rho_next * rho, 2.0 * rho_next / radius
    image = keep * (first_image / center) + take * (first_image - second_image / center)
    direction = keep * direction + take * residual
    rho = rho_next
    weight = weight + direction

    for e in range(1, ITERS - 2):
        residual = residual - image
        rho_next = 1.0 / (2.0 * sigma - rho)
        direction = rho_next * rho * direction + 2.0 * rho_next / radius * residual
        rho = rho_next
        weight = weight + direction
        exchange(e, direction)
        if e == 1:
            for hop in (2, 3):
                relayed(hop)
                relay(hop + 2)
        if e == 3:
            relayed(4)
            relay(6)
        image = image_of(direction, lambda e=e: arrived(e))
    residual = residual - image
    rho_next = 1.0 / (2.0 * sigma - rho)
    direction = rho_next * rho * direction + 2.0 * rho_next / radius * residual
    weight = weight + direction
    last = ITERS - 2
    exchange(last, weight)

    relayed(HOPS - 2)
    relayed(HOPS - 1)
    width = 512

    def split_states(i, c):
        x = lax.div(i, slab // width)
        lanes = pl.ds(pl.multiple_of(lax.rem(i, slab // width) * width, width), width)
        states = zs[x, :, lanes]
        high, low = halves(states - jnp.sum(states, axis=0, keepdims=True) / members)
        sh[x, :, lanes] = high
        sl[x, :, lanes] = low
        return c

    lax.fori_loop(0, 2 * slab // width, split_states, 0)

    base = me_s.astype(f32) * 2.0

    def gain_part(block, row, lanes):
        wide = jnp.concatenate([block * taper(base, row), block * taper(base + 1.0, row)], axis=0)
        high, low = halves(wide)
        top = nt(jnp.concatenate([high, low], axis=0), ah[:, lanes])
        return top[:2 * mdev] + top[2 * mdev:] + nt(high, al[:, lanes])

    gain = gain_part(weight, plane_row, own_lanes)
    values = arrived(last)
    for g in (slice(0, REACH), slice(REACH, own)):
        span = range(g.start, g.stop)
        rows = jnp.concatenate([e0[i, pl.ds(mdev, 1), :] for i in span], axis=1)
        block = jnp.concatenate([values(i) for i in span], axis=1)
        gain = gain + gain_part(block, rows, slice(g.start * odev, g.stop * odev))
    gain = gain / (members - 1)

    for x in range(2):
        ghigh, glow = halves(gain[x * mdev:(x + 1) * mdev])
        gboth = jnp.concatenate([ghigh, glow], axis=0)

        def update(i, c, x=x, ghigh=ghigh, gboth=gboth):
            lanes = pl.ds(pl.multiple_of(i * width, width), width)
            top = nn(gboth, sh[x, :, lanes])
            out[x, :, lanes] = zs[x, mine, lanes] + (top[:mdev] + top[mdev:] + nn(ghigh, sl[x, :, lanes]))
            return c

        lax.fori_loop(0, slab // width, update, 0)

    awaited(r.at[pl.ds(0, planes - 2)], ssem.at[S_OUT])
    awaited(fr.at[pl.ds(0, space_count - 1)], ssem.at[S_FORC])
    awaited(r.at[pl.ds(0, planes - 2)], ssem.at[S_BACK])
    awaited(ab.at[0, pl.ds(0, members - mdev)], ssem.at[S_OBS])
    awaited(e0.at[pl.ds(0, 2 * REACH)], ssem.at[S_RHS])
    awaited(ab.at[pl.ds(0, REACH)], ssem.at[S_BAND])
    awaited(ab.at[pl.ds(0, REACH)], ssem.at[S_PAIR])
    awaited(bb.at[pl.ds(0, space_count - 1)], ssem.at[S_BOUND])
    for e in range(ITERS - 1):
        awaited(ex.at[e, pl.ds(0, 2 * REACH)], ssem.at[S_DIR + e])
    for hop in range(HOPS):
        for at in (S_RIGHT, S_LEFT):
            awaited(zs.at[0, pl.ds(0, mdev), :], ssem.at[at + hop])


def shards(ensemble, forcing, obs_cell, obs_value, obs_var, obs_noise):
    mdev, pdev, slab = ensemble.shape
    odev = obs_cell.shape[0]
    space_count = lax.axis_size("space")
    mem_count = lax.axis_size("mem")
    members = mdev * mem_count
    planes = pdev * space_count
    band = SLOTS * odev

    def call(*args):
        return kernel(space_count, mem_count, *args)

    vmem = pl.BlockSpec(memory_space=pltpu.VMEM)
    analysis = pl.pallas_call(
        call,
        out_shape=jax.ShapeDtypeStruct((pdev, mdev, slab), f32),
        in_specs=[vmem] * 6,
        out_specs=vmem,
        scratch_shapes=[
            pltpu.VMEM((planes, mdev // 2, 128), f32),
            pltpu.VMEM((planes, mdev // 2, 128), f32),
            pltpu.VMEM((space_count, pdev, 128), f32),
            pltpu.VMEM((pdev, members, slab), f32),
            pltpu.VMEM((pdev, members, slab), bf16),
            pltpu.VMEM((pdev, members, slab), bf16),
            pltpu.VMEM((pdev * slab, odev), bf16),
            pltpu.VMEM((SLOTS, members, odev), f32),
            pltpu.VMEM((members, band), bf16),
            pltpu.VMEM((members, band), bf16),
            pltpu.VMEM((SLOTS, mdev + 8, odev), f32),
            pltpu.VMEM((ITERS - 1, SLOTS, mdev, odev), f32),
            pltpu.VMEM((space_count, 8, odev), f32),
            pltpu.VMEM((odev, band), bf16),
            pltpu.VMEM((odev, band), bf16),
            pltpu.VMEM((2 * mdev, 2 * REACH * odev), bf16),
            pltpu.SemaphoreType.DMA((SENDS,)),
            pltpu.SemaphoreType.DMA((RECVS,)),
            pltpu.SemaphoreType.DMA((3,)),
        ],
        compiler_params=pltpu.CompilerParams(
            collective_id=0, has_side_effects=True, vmem_limit_bytes=32 * 1024 * 1024),
        name="cycle",
    )(
        jnp.transpose(ensemble, (1, 0, 2)), forcing, obs_cell[None, :], obs_value[None, :], obs_var[None, :],
        obs_noise,
    )
    return jnp.transpose(analysis, (1, 0, 2))


def solution(mesh):
    placed = (
        P("mem", "space", None),
        P("space", None),
        P("space"),
        P("space"),
        P("space"),
        P("mem", "space"),
    )
    return jax.shard_map(
        shards, mesh=mesh, in_specs=placed, out_specs=P("mem", "space", None), check_vma=False
    )
```

```python
import jax
import jax.numpy as jnp
from jax import lax
from jax.experimental import pallas as pl
from jax.experimental.pallas import tpu as pltpu
from jax.sharding import PartitionSpec as P

FSTEPS = 4
ITERS = 6
LOC = 16
REACH = 8
SLOTS = 2 * REACH + 1
MESH = pl.DeviceIdType.MESH
AWAY = (4, -4, 6, -6, 2, -2, 8, -8)
STEPS = (
    (2, 2), (2, 1), (1, 2), (2, 3), (3, 2), (1, 1), (3, 3), (1, 3),
    (3, 1), (2, 0), (0, 2), (1, 0), (0, 1), (3, 0), (0, 3), (0, 0),
)
f32 = jnp.float32
bf16 = jnp.bfloat16

HOPS = 7
R_OUT, R_FORC, R_BACK, R_BOUND = range(4)
R_RHS = 4
R_DIR = R_RHS + 2 * REACH
R_OBS = R_DIR + ITERS - 1
R_BAND = R_OBS + 8
R_RIGHT = R_BAND + SLOTS
R_LEFT = R_RIGHT + HOPS
RECVS = R_LEFT + HOPS
S_OUT, S_FORC, S_BACK, S_OBS, S_RHS, S_BAND, S_PAIR, S_BOUND = range(8)
S_DIR = 8
S_RIGHT = S_DIR + ITERS - 1
S_LEFT = S_RIGHT + HOPS
SENDS = S_LEFT + HOPS

NT = (((1,), (1,)), ((), ()))


def nn(a, b):
    return jnp.dot(a, b, preferred_element_type=f32)


def nt(a, b):
    return lax.dot_general(a, b, NT, preferred_element_type=f32)


def halves(x):
    high = x.astype(bf16)
    return high, (x - high.astype(f32)).astype(bf16)


def awaited(ref, sem):
    pltpu.make_async_copy(ref, ref, sem).wait()


def kernel(
    space_count, mem_count,
    ens, forc, cell, value, var, noise,
    out,
    r, t, fr, zs, sh, sl, oh, ab, ah, al, e0, ex, bb, ch, cl, dh,
    ssem, rsem, lsem,
):
    me_s = lax.axis_index("space")
    me_m = lax.axis_index("mem")
    members = ab.shape[1]
    mdev = noise.shape[0]
    planes = r.shape[0]
    half = mdev // 2
    odev = cell.shape[1]
    slab = ens.shape[2]

    def chunk_of(index):
        return lax.div(index, 2), lax.rem(index, 2)

    def other(base, step, count):
        return lax.rem(base + step, count)

    my_c, my_h = chunk_of(me_s)
    side_y = 4
    side_x = space_count // 2 // side_y
    others = []
    for dx, dy in STEPS:
        chip = lax.rem(lax.div(my_c, side_y) + dx, side_x) * side_y + lax.rem(lax.rem(my_c, side_y) + dy, side_y)
        others.append(2 * chip + (1 - my_h))
        if (dx, dy) != (0, 0):
            others.append(2 * chip + my_h)

    barrier = pltpu.get_barrier_semaphore()

    def greet_space(i, c):
        pl.semaphore_signal(barrier, inc=1, device_id={"space": other(me_s, i, space_count)}, device_id_type=MESH)
        return c

    def greet_mem(i, c):
        pl.semaphore_signal(barrier, inc=1, device_id={"mem": other(me_m, i, mem_count)}, device_id_type=MESH)
        return c

    lax.fori_loop(1, space_count, greet_space, 0)
    lax.fori_loop(1, mem_count, greet_mem, 0)

    own_out = pltpu.make_async_copy(
        ens.at[:, pl.ds(pl.multiple_of(my_h * half, half), half), pl.ds(pl.multiple_of(my_c * 128, 128), 128)],
        r.at[pl.ds(me_s * 2, 2)], lsem.at[0])
    own_forc = pltpu.make_async_copy(
        forc.at[:, pl.ds(pl.multiple_of(my_c * 128, 128), 128)], fr.at[me_s], lsem.at[1])
    own_out.start()
    own_forc.start()

    pl.semaphore_wait(barrier, space_count + mem_count - 2)

    for to in others:
        tc, th = chunk_of(to)
        cells = pl.ds(pl.multiple_of(tc * 128, 128), 128)
        pltpu.make_async_remote_copy(
            src_ref=forc.at[:, cells], dst_ref=fr.at[me_s],
            send_sem=ssem.at[S_FORC], recv_sem=rsem.at[R_FORC],
            device_id={"space": to}, device_id_type=MESH).start()
        pltpu.make_async_remote_copy(
            src_ref=ens.at[:, pl.ds(pl.multiple_of(th * half, half), half), cells],
            dst_ref=r.at[pl.ds(me_s * 2, 2)],
            send_sem=ssem.at[S_OUT], recv_sem=rsem.at[R_OUT],
            device_id={"space": to}, device_id_type=MESH).start()

    cells_here = cell[...] - me_s * (2 * slab)

    def one_hot(i, c):
        rows = lax.broadcasted_iota(jnp.int32, (256, odev), 0) + i * 256
        oh[pl.ds(pl.multiple_of(i * 256, 256), 256), :] = jnp.where(rows == cells_here, 1.0, 0.0).astype(bf16)
        return c

    lax.fori_loop(0, 2 * slab // 256, one_hot, 0)

    own_out.wait()
    own_forc.wait()
    awaited(r.at[pl.ds(0, planes - 2)], rsem.at[R_OUT])
    awaited(fr.at[pl.ds(0, space_count - 1)], rsem.at[R_FORC])

    def advance(src, dst):
        def group(g, carry):
            two, one, now = carry
            for i in range(8):
                x = g * 8 + i
                ahead = src[lax.rem(x + 1, planes)]
                force = fr[g * 4 + i // 2, pl.ds(i % 2, 1), :]
                dst[x] = now + 0.05 * ((ahead - two) * one - now + force)
                two, one, now = one, now, ahead
            return two, one, now

        lax.fori_loop(0, planes // 8, group, (src[planes - 2], src[planes - 1], src[0]))

    for step in range(FSTEPS // 2):
        advance(r, t)
        advance(t, r)

    mine = pl.ds(pl.multiple_of(me_m * mdev, mdev), mdev)
    my_rows = pl.ds(pl.multiple_of(me_m * mdev + my_h * half, half), half)
    my_cells = pl.ds(pl.multiple_of(my_c * 128, 128), 128)

    for to in others:
        pltpu.make_async_remote_copy(
            src_ref=r.at[pl.ds(to * 2, 2)], dst_ref=zs.at[:, my_rows, my_cells],
            send_sem=ssem.at[S_BACK], recv_sem=rsem.at[R_BACK],
            device_id={"space": to}, device_id_type=MESH).start()
    own_back = pltpu.make_async_copy(r.at[pl.ds(me_s * 2, 2)], zs.at[:, my_rows, my_cells], lsem.at[2])
    own_back.start()
    own_back.wait()
    awaited(r.at[pl.ds(0, planes - 2)], rsem.at[R_BACK])

    observed = jnp.zeros((3 * mdev, odev), f32)
    for x in range(2):
        block = zs[x, mine, :]
        first = block.astype(bf16)
        rest = block - first.astype(f32)
        second = rest.astype(bf16)
        third = (rest - second.astype(f32)).astype(bf16)
        pieces = jnp.concatenate([first, second, third], axis=0)
        observed = observed + nn(pieces, oh[x * slab:(x + 1) * slab, :])
    observed = observed[:mdev] + observed[mdev:2 * mdev] + observed[2 * mdev:]
    ab[REACH, mine, :] = observed

    def send_obs(i, c):
        pltpu.make_async_remote_copy(
            src_ref=ab.at[REACH, mine], dst_ref=ab.at[REACH, mine],
            send_sem=ssem.at[S_OBS], recv_sem=rsem.at[R_OBS + i],
            device_id={"mem": other(me_m, i, mem_count)}, device_id_type=MESH).start()
        return c

    lax.fori_loop(1, mem_count, send_obs, 0)

    right = other(me_m, 1, mem_count)
    left = other(me_m, mem_count - 1, mem_count)

    def relay(hop):
        for way in (1, -1):
            origin = lax.rem(me_m + mem_count - way * (hop // 2), mem_count)
            x = hop % 2 if way > 0 else 1 - hop % 2
            ref = zs.at[x, pl.ds(pl.multiple_of(origin * mdev, mdev), mdev), :]
            pltpu.make_async_remote_copy(
                src_ref=ref, dst_ref=ref,
                send_sem=ssem.at[(S_RIGHT if way > 0 else S_LEFT) + hop],
                recv_sem=rsem.at[(R_RIGHT if way > 0 else R_LEFT) + hop],
                device_id={"mem": right if way > 0 else left}, device_id_type=MESH).start()

    def relayed(hop):
        for base in (R_RIGHT, R_LEFT):
            awaited(zs.at[0, pl.ds(0, mdev), :], rsem.at[base + hop])

    plane_row = jnp.floor(cell[...].astype(f32) / slab)
    rhs = jnp.sqrt(var[...]) * noise[...] + value[...] - observed
    own = 2 * REACH
    e0[own, :mdev, :] = rhs
    e0[own, mdev:, :] = jnp.broadcast_to(plane_row, (8, odev))

    turn = 1 - 2 * my_h
    partner = {"space": me_s + turn}
    out_of_reach = REACH - 1 - my_h
    band_to = [{"space": lax.rem(me_s + away + space_count, space_count)} for away in AWAY]

    def spread(at, send, recv):
        def copy(there, to):
            pltpu.make_async_remote_copy(
                src_ref=at(own), dst_ref=at(there), send_sem=ssem.at[send], recv_sem=rsem.at[recv + there],
                device_id=to, device_id_type=MESH).start()

        for i, to in enumerate(band_to):
            copy(i ^ 1, to)
        copy(REACH + out_of_reach, partner)

    def hand_over(at, send, recv):
        def copy(i):
            pltpu.make_async_remote_copy(
                src_ref=at(i), dst_ref=at(REACH + i), send_sem=ssem.at[send], recv_sem=rsem.at[recv + REACH + i],
                device_id=partner, device_id_type=MESH).start()

        for i in range(REACH - 2):
            awaited(at(i), rsem.at[recv + i])
            copy(i)
        for i in range(REACH - 2, REACH):
            awaited(at(i), rsem.at[recv + i])
        copy(2 * REACH - 3 - out_of_reach)

    def handed(at, recv):
        for i in range(REACH, 2 * REACH):
            awaited(at(i), rsem.at[recv + i])

    def rhs_at(i):
        return e0.at[i]

    spread(rhs_at, S_RHS, R_RHS)

    near = (1, -1, 4, -4)
    chips_at = {chips: {"space": lax.rem(me_s + 2 * chips + space_count, space_count)}
                for chips in near}

    def piece_rows(step):
        origin = lax.rem(me_m + mem_count - step, mem_count)
        return pl.ds(pl.multiple_of(origin * mdev, mdev), mdev)

    def piece_send(slot, there, rows, chips):
        pltpu.make_async_remote_copy(
            src_ref=ab.at[slot, rows], dst_ref=ab.at[there, rows],
            send_sem=ssem.at[S_BAND], recv_sem=rsem.at[R_BAND + there],
            device_id=chips_at[chips], device_id_type=MESH).start()

    def to_chips(step):
        rows = piece_rows(step)
        for chips in near:
            piece_send(REACH, REACH - 2 * chips, rows, chips)

    def piece_here(step):
        awaited(ab.at[REACH, pl.ds(0, mdev)], rsem.at[R_OBS + step])

    to_chips(0)
    relay(0)
    relay(1)
    for step in (1, 7, 2, 6, 3, 5, 4):
        piece_here(step)
        to_chips(step)
    hand_over(rhs_at, S_RHS, R_RHS)

    def pair_send(e):
        pltpu.make_async_remote_copy(
            src_ref=ab.at[REACH + turn * e], dst_ref=ab.at[REACH + turn * (e - 1)],
            send_sem=ssem.at[S_PAIR], recv_sem=rsem.at[R_BAND + REACH + turn * (e - 1)],
            device_id=partner, device_id_type=MESH).start()

    def slot_here(j):
        awaited(ab.at[0], rsem.at[R_BAND + j])

    pair_send(0)

    def anomalies(j):
        raw = ab[j]
        return raw - jnp.sum(raw, axis=0, keepdims=True) / members

    anom_t = anomalies(REACH).T
    th, tl = halves(anom_t)
    both_t = jnp.concatenate([th, tl], axis=0)
    own_plane = jnp.broadcast_to(plane_row, (odev, odev)).T
    own_var = jnp.broadcast_to(var[...], (odev, odev)).T
    diagonal = (lax.broadcasted_iota(jnp.int32, (odev, odev), 0) == lax.broadcasted_iota(jnp.int32, (odev, odev), 1))
    diag_var = jnp.where(diagonal, own_var, 0.0)

    def taper(a, b):
        spread = jnp.abs(a - b)
        spread = jnp.minimum(spread, planes - spread)
        return jnp.maximum(0.0, 1.0 - spread / LOC)

    def rows_of(j, place, total, more=None):
        lanes = pl.ds(pl.multiple_of(place * odev, odev), odev)
        high, low = halves(anomalies(j))
        ah[:, lanes] = high
        al[:, lanes] = low
        gram = nn(both_t, high)
        gram = gram[:odev] + gram[odev:] + nn(th, low)
        block = taper(own_plane, e0[place, pl.ds(mdev, 1), :]) * gram / (members - 1)
        if more is not None:
            block = block + more
        chigh, clow = halves(block)
        ch[:, lanes] = chigh
        cl[:, lanes] = clow
        return total + jnp.abs(block)

    total = rows_of(REACH, own, jnp.zeros((odev, odev), f32), diag_var)

    for side in (1, -1):
        slot = REACH + 2 * side
        slot_here(slot)
        for chips in (-side, 4 * side):
            piece_send(slot, slot - 2 * chips, slice(None), chips)
    pair_send(2)
    pair_send(-2)
    handed(rhs_at, R_RHS)

    def pick(i, table):
        value = table[0]
        for k in range(1, len(table)):
            value = jnp.where(i == k, table[k], value)
        return value

    def place(rank, negative):
        return 2 * rank + my_h + negative - 2 * my_h * negative

    def slot_rows(e, rank, negative, total):
        return rows_of(REACH + turn * e, place(rank, negative), total)

    def partner_rows(e, rank, negative, total):
        return rows_of(REACH + turn * (1 - e), REACH + place(rank, 1 - negative), total)

    total = slot_rows(2, 2, 0, total)
    total = slot_rows(-2, 2, 1, total)

    def two_slots(i, total):
        e = pick(i, (8, 4, -4, 6, -6))
        f = pick(i, (0, 2, -2, 8, 4))
        slot_here(REACH + turn * e)
        pair_send(e)
        slot_here(REACH + turn * (1 - f))
        total = slot_rows(e, pick(i, (3, 0, 0, 1, 1)), pick(i, (0, 0, 1, 0, 1)), total)
        return partner_rows(f, pick(i, (3, 2, 2, 3, 0)), pick(i, (1, 0, 1, 0, 0)), total)

    total = lax.fori_loop(0, 1, two_slots, total)
    relayed(0)
    relay(2)
    total = lax.fori_loop(1, 5, two_slots, total)
    slot_here(REACH - turn * REACH)
    slot_here(REACH + turn * (1 + 4))
    total = slot_rows(-REACH, 3, 1, total)
    total = partner_rows(-4, 0, 1, total)
    slot_here(REACH + turn * (1 - 6))
    slot_here(REACH + turn * (1 + 6))
    total = partner_rows(6, 1, 0, total)
    total = partner_rows(-6, 1, 1, total)

    def part(block, lanes):
        high, low = halves(block)
        top = nt(jnp.concatenate([high, low], axis=0), ch[:, lanes])
        return top[:mdev] + top[mdev:] + nt(high, cl[:, lanes])

    own_lanes = slice(own * odev, (own + 1) * odev)
    lanes_out = slice(0, own * odev)

    def exchange(e, block):
        ex[e, own] = block

        def copy(there, to):
            pltpu.make_async_remote_copy(
                src_ref=ex.at[e, own], dst_ref=ex.at[e, there],
                send_sem=ssem.at[S_DIR + e], recv_sem=rsem.at[R_DIR + e],
                device_id=to, device_id_type=MESH).start()

        for i, to in enumerate(band_to):
            copy(i ^ 1, to)
            if i < REACH - 2:
                copy(REACH + (i ^ 1), {"space": lax.rem(me_s + AWAY[i] + turn + space_count, space_count)})
        copy(3 * REACH - 3 - out_of_reach,
             {"space": lax.rem(me_s - (REACH - 1) * turn + space_count, space_count)})
        copy(REACH + out_of_reach, partner)

    def arrived(e):
        awaited(ex.at[e, pl.ds(0, own)], rsem.at[R_DIR + e])
        return lambda i: ex[e, i]

    def image_of(block, values_of):
        image = part(block, own_lanes)
        values = values_of()
        for i in range(own):
            high, low = halves(values(i))
            dh[:mdev, i * odev:(i + 1) * odev] = high
            dh[mdev:, i * odev:(i + 1) * odev] = low
        top = nt(dh[...], ch[:, lanes_out])
        return image + (top[:mdev] + top[mdev:] + nt(dh[:mdev, :], cl[:, lanes_out]))

    row_max = jnp.max(jnp.sum(total, axis=1, keepdims=True), axis=0, keepdims=True)
    var_min = jnp.min(var[...], axis=1, keepdims=True)
    is_upper = lax.broadcasted_iota(jnp.int32, (8, odev), 0) < 4
    bb[me_s] = jnp.where(is_upper, row_max, -var_min)

    for to in others:
        pltpu.make_async_remote_copy(
            src_ref=bb.at[me_s], dst_ref=bb.at[me_s],
            send_sem=ssem.at[S_BOUND], recv_sem=rsem.at[R_BOUND],
            device_id={"space": to}, device_id_type=MESH).start()

    first_image = image_of(rhs, lambda: lambda i: e0[i, pl.ds(0, mdev), :])
    exchange(0, first_image)
    relayed(1)
    relay(3)
    second_image = image_of(first_image, lambda: arrived(0))

    awaited(bb.at[pl.ds(0, space_count - 1)], rsem.at[R_BOUND])
    bounds = jnp.max(bb[...], axis=0)
    upper = bounds[0:1, :]
    lower = -bounds[4:5, :]
    center = (upper + lower) / 2.0
    radius = (upper - lower) / 2.0
    sigma = center / radius
    rho = 1.0 / sigma
    direction = rhs / center
    weight = direction
    residual = rhs - first_image / center
    rho_next = 1.0 / (2.0 * sigma - rho)
    keep, take = rho_next * rho, 2.0 * rho_next / radius
    image = keep * (first_image / center) + take * (first_image - second_image / center)
    direction = keep * direction + take * residual
    rho = rho_next
    weight = weight + direction

    for e in range(1, ITERS - 2):
        residual = residual - image
        rho_next = 1.0 / (2.0 * sigma - rho)
        direction = rho_next * rho * direction + 2.0 * rho_next / radius * residual
        rho = rho_next
        weight = weight + direction
        exchange(e, direction)
        relayed(e + 1)
        relay(e + 3)
        image = image_of(direction, lambda e=e: arrived(e))
    residual = residual - image
    rho_next = 1.0 / (2.0 * sigma - rho)
    direction = rho_next * rho * direction + 2.0 * rho_next / radius * residual
    weight = weight + direction
    last = ITERS - 2
    exchange(last, weight)

    relayed(HOPS - 2)
    relayed(HOPS - 1)
    width = 512

    def split_states(i, c):
        x = lax.div(i, slab // width)
        lanes = pl.ds(pl.multiple_of(lax.rem(i, slab // width) * width, width), width)
        states = zs[x, :, lanes]
        high, low = halves(states - jnp.sum(states, axis=0, keepdims=True) / members)
        sh[x, :, lanes] = high
        sl[x, :, lanes] = low
        return c

    lax.fori_loop(0, 2 * slab // width, split_states, 0)

    base = me_s.astype(f32) * 2.0

    def gain_part(block, row, lanes):
        wide = jnp.concatenate([block * taper(base, row), block * taper(base + 1.0, row)], axis=0)
        high, low = halves(wide)
        top = nt(jnp.concatenate([high, low], axis=0), ah[:, lanes])
        return top[:2 * mdev] + top[2 * mdev:] + nt(high, al[:, lanes])

    gain = gain_part(weight, plane_row, own_lanes)
    values = arrived(last)
    for g in (slice(0, REACH), slice(REACH, own)):
        span = range(g.start, g.stop)
        rows = jnp.concatenate([e0[i, pl.ds(mdev, 1), :] for i in span], axis=1)
        block = jnp.concatenate([values(i) for i in span], axis=1)
        gain = gain + gain_part(block, rows, slice(g.start * odev, g.stop * odev))
    gain = gain / (members - 1)

    for x in range(2):
        ghigh, glow = halves(gain[x * mdev:(x + 1) * mdev])
        gboth = jnp.concatenate([ghigh, glow], axis=0)

        wide = 1024

        def update(i, c, x=x, ghigh=ghigh, gboth=gboth):
            lanes = pl.ds(pl.multiple_of(i * wide, wide), wide)
            top = nn(gboth, sh[x, :, lanes])
            out[x, :, lanes] = zs[x, mine, lanes] + (top[:mdev] + top[mdev:] + nn(ghigh, sl[x, :, lanes]))
            return c

        lax.fori_loop(0, slab // wide, update, 0)

    awaited(r.at[pl.ds(0, planes - 2)], ssem.at[S_OUT])
    awaited(fr.at[pl.ds(0, space_count - 1)], ssem.at[S_FORC])
    awaited(r.at[pl.ds(0, planes - 2)], ssem.at[S_BACK])
    awaited(ab.at[0, pl.ds(0, members - mdev)], ssem.at[S_OBS])
    awaited(e0.at[pl.ds(0, 2 * REACH)], ssem.at[S_RHS])
    awaited(ab.at[pl.ds(0, REACH)], ssem.at[S_BAND])
    awaited(ab.at[pl.ds(0, REACH)], ssem.at[S_PAIR])
    awaited(bb.at[pl.ds(0, space_count - 1)], ssem.at[S_BOUND])
    for e in range(ITERS - 1):
        awaited(ex.at[e, pl.ds(0, 2 * REACH)], ssem.at[S_DIR + e])
    for hop in range(HOPS):
        for at in (S_RIGHT, S_LEFT):
            awaited(zs.at[0, pl.ds(0, mdev), :], ssem.at[at + hop])


def shards(ensemble, forcing, obs_cell, obs_value, obs_var, obs_noise):
    mdev, pdev, slab = ensemble.shape
    odev = obs_cell.shape[0]
    space_count = lax.axis_size("space")
    mem_count = lax.axis_size("mem")
    members = mdev * mem_count
    planes = pdev * space_count
    band = SLOTS * odev

    def call(*args):
        return kernel(space_count, mem_count, *args)

    vmem = pl.BlockSpec(memory_space=pltpu.VMEM)
    analysis = pl.pallas_call(
        call,
        out_shape=jax.ShapeDtypeStruct((pdev, mdev, slab), f32),
        in_specs=[vmem] * 6,
        out_specs=vmem,
        scratch_shapes=[
            pltpu.VMEM((planes, mdev // 2, 128), f32),
            pltpu.VMEM((planes, mdev // 2, 128), f32),
            pltpu.VMEM((space_count, pdev, 128), f32),
            pltpu.VMEM((pdev, members, slab), f32),
            pltpu.VMEM((pdev, members, slab), bf16),
            pltpu.VMEM((pdev, members, slab), bf16),
            pltpu.VMEM((pdev * slab, odev), bf16),
            pltpu.VMEM((SLOTS, members, odev), f32),
            pltpu.VMEM((members, band), bf16),
            pltpu.VMEM((members, band), bf16),
            pltpu.VMEM((SLOTS, mdev + 8, odev), f32),
            pltpu.VMEM((ITERS - 1, SLOTS, mdev, odev), f32),
            pltpu.VMEM((space_count, 8, odev), f32),
            pltpu.VMEM((odev, band), bf16),
            pltpu.VMEM((odev, band), bf16),
            pltpu.VMEM((2 * mdev, 2 * REACH * odev), bf16),
            pltpu.SemaphoreType.DMA((SENDS,)),
            pltpu.SemaphoreType.DMA((RECVS,)),
            pltpu.SemaphoreType.DMA((3,)),
        ],
        compiler_params=pltpu.CompilerParams(
            collective_id=0, has_side_effects=True, vmem_limit_bytes=32 * 1024 * 1024),
        name="cycle",
    )(
        jnp.transpose(ensemble, (1, 0, 2)), forcing, obs_cell[None, :], obs_value[None, :], obs_var[None, :],
        obs_noise,
    )
    return jnp.transpose(analysis, (1, 0, 2))


def solution(mesh):
    placed = (
        P("mem", "space", None),
        P("space", None),
        P("space"),
        P("space"),
        P("space"),
        P("mem", "space"),
    )
    return jax.shard_map(
        shards, mesh=mesh, in_specs=placed, out_specs=P("mem", "space", None), check_vma=False
    )
```

```python
import jax
import jax.numpy as jnp
from jax import lax
from jax.experimental import pallas as pl
from jax.experimental.pallas import tpu as pltpu
from jax.sharding import PartitionSpec as P

FSTEPS = 4
ITERS = 6
LOC = 16
REACH = 8
SLOTS = 2 * REACH + 1
MESH = pl.DeviceIdType.MESH
AWAY = (4, -4, 6, -6, 2, -2, 8, -8)
STEPS = (
    (2, 2), (2, 1), (1, 2), (2, 3), (3, 2), (1, 1), (3, 3), (1, 3),
    (3, 1), (2, 0), (0, 2), (1, 0), (0, 1), (3, 0), (0, 3), (0, 0),
)
f32 = jnp.float32
bf16 = jnp.bfloat16

HOPS = 7
R_OUT, R_FORC, R_BACK, R_BOUND = range(4)
R_RHS = 4
R_DIR = R_RHS + 2 * REACH
R_OBS = R_DIR + ITERS - 1
R_BAND = R_OBS + 8
R_RIGHT = R_BAND + SLOTS
R_LEFT = R_RIGHT + HOPS
RECVS = R_LEFT + HOPS
S_OUT, S_FORC, S_BACK, S_OBS, S_RHS, S_BAND, S_PAIR, S_BOUND = range(8)
S_DIR = 8
S_RIGHT = S_DIR + ITERS - 1
S_LEFT = S_RIGHT + HOPS
SENDS = S_LEFT + HOPS

NT = (((1,), (1,)), ((), ()))


def nn(a, b):
    return jnp.dot(a, b, preferred_element_type=f32)


def nt(a, b):
    return lax.dot_general(a, b, NT, preferred_element_type=f32)


def halves(x):
    high = x.astype(bf16)
    return high, (x - high.astype(f32)).astype(bf16)


def awaited(ref, sem):
    pltpu.make_async_copy(ref, ref, sem).wait()


def kernel(
    space_count, mem_count,
    ens, forc, cell, value, var, noise,
    out,
    r, t, fr, zs, sh, sl, oh, ab, ah, al, e0, ex, bb, ch, cl, dh,
    ssem, rsem, lsem,
):
    me_s = lax.axis_index("space")
    me_m = lax.axis_index("mem")
    members = ab.shape[1]
    mdev = noise.shape[0]
    planes = r.shape[0]
    half = mdev // 2
    odev = cell.shape[1]
    slab = ens.shape[2]

    def chunk_of(index):
        return lax.div(index, 2), lax.rem(index, 2)

    def other(base, step, count):
        return lax.rem(base + step, count)

    my_c, my_h = chunk_of(me_s)
    side_y = 4
    side_x = space_count // 2 // side_y
    others = []
    for dx, dy in STEPS:
        chip = lax.rem(lax.div(my_c, side_y) + dx, side_x) * side_y + lax.rem(lax.rem(my_c, side_y) + dy, side_y)
        others.append(2 * chip + (1 - my_h))
        if (dx, dy) != (0, 0):
            others.append(2 * chip + my_h)

    barrier = pltpu.get_barrier_semaphore()

    def greet_space(i, c):
        pl.semaphore_signal(barrier, inc=1, device_id={"space": other(me_s, i, space_count)}, device_id_type=MESH)
        return c

    def greet_mem(i, c):
        pl.semaphore_signal(barrier, inc=1, device_id={"mem": other(me_m, i, mem_count)}, device_id_type=MESH)
        return c

    lax.fori_loop(1, space_count, greet_space, 0)
    lax.fori_loop(1, mem_count, greet_mem, 0)

    own_out = pltpu.make_async_copy(
        ens.at[:, pl.ds(pl.multiple_of(my_h * half, half), half), pl.ds(pl.multiple_of(my_c * 128, 128), 128)],
        r.at[pl.ds(me_s * 2, 2)], lsem.at[0])
    own_forc = pltpu.make_async_copy(
        forc.at[:, pl.ds(pl.multiple_of(my_c * 128, 128), 128)], fr.at[me_s], lsem.at[1])
    own_out.start()
    own_forc.start()

    pl.semaphore_wait(barrier, space_count + mem_count - 2)

    for to in others:
        tc, th = chunk_of(to)
        cells = pl.ds(pl.multiple_of(tc * 128, 128), 128)
        pltpu.make_async_remote_copy(
            src_ref=forc.at[:, cells], dst_ref=fr.at[me_s],
            send_sem=ssem.at[S_FORC], recv_sem=rsem.at[R_FORC],
            device_id={"space": to}, device_id_type=MESH).start()
        pltpu.make_async_remote_copy(
            src_ref=ens.at[:, pl.ds(pl.multiple_of(th * half, half), half), cells],
            dst_ref=r.at[pl.ds(me_s * 2, 2)],
            send_sem=ssem.at[S_OUT], recv_sem=rsem.at[R_OUT],
            device_id={"space": to}, device_id_type=MESH).start()

    cells_here = cell[...] - me_s * (2 * slab)

    def one_hot(i, c):
        rows = lax.broadcasted_iota(jnp.int32, (256, odev), 0) + i * 256
        oh[pl.ds(pl.multiple_of(i * 256, 256), 256), :] = jnp.where(rows == cells_here, 1.0, 0.0).astype(bf16)
        return c

    lax.fori_loop(0, 2 * slab // 256, one_hot, 0)

    own_out.wait()
    own_forc.wait()
    awaited(r.at[pl.ds(0, planes - 2)], rsem.at[R_OUT])
    awaited(fr.at[pl.ds(0, space_count - 1)], rsem.at[R_FORC])

    def advance(src, dst):
        def group(g, carry):
            two, one, now = carry
            for i in range(8):
                x = g * 8 + i
                ahead = src[lax.rem(x + 1, planes)]
                force = fr[g * 4 + i // 2, pl.ds(i % 2, 1), :]
                dst[x] = now + 0.05 * ((ahead - two) * one - now + force)
                two, one, now = one, now, ahead
            return two, one, now

        lax.fori_loop(0, planes // 8, group, (src[planes - 2], src[planes - 1], src[0]))

    for step in range(FSTEPS // 2):
        advance(r, t)
        advance(t, r)

    mine = pl.ds(pl.multiple_of(me_m * mdev, mdev), mdev)
    my_rows = pl.ds(pl.multiple_of(me_m * mdev + my_h * half, half), half)
    my_cells = pl.ds(pl.multiple_of(my_c * 128, 128), 128)

    for to in others:
        pltpu.make_async_remote_copy(
            src_ref=r.at[pl.ds(to * 2, 2)], dst_ref=zs.at[:, my_rows, my_cells],
            send_sem=ssem.at[S_BACK], recv_sem=rsem.at[R_BACK],
            device_id={"space": to}, device_id_type=MESH).start()
    own_back = pltpu.make_async_copy(r.at[pl.ds(me_s * 2, 2)], zs.at[:, my_rows, my_cells], lsem.at[2])
    own_back.start()
    own_back.wait()
    awaited(r.at[pl.ds(0, planes - 2)], rsem.at[R_BACK])

    observed = jnp.zeros((3 * mdev, odev), f32)
    for x in range(2):
        block = zs[x, mine, :]
        first = block.astype(bf16)
        rest = block - first.astype(f32)
        second = rest.astype(bf16)
        third = (rest - second.astype(f32)).astype(bf16)
        pieces = jnp.concatenate([first, second, third], axis=0)
        observed = observed + nn(pieces, oh[x * slab:(x + 1) * slab, :])
    observed = observed[:mdev] + observed[mdev:2 * mdev] + observed[2 * mdev:]
    ab[REACH, mine, :] = observed

    def send_obs(i, c):
        pltpu.make_async_remote_copy(
            src_ref=ab.at[REACH, mine], dst_ref=ab.at[REACH, mine],
            send_sem=ssem.at[S_OBS], recv_sem=rsem.at[R_OBS + i],
            device_id={"mem": other(me_m, i, mem_count)}, device_id_type=MESH).start()
        return c

    lax.fori_loop(1, mem_count, send_obs, 0)

    right = other(me_m, 1, mem_count)
    left = other(me_m, mem_count - 1, mem_count)

    def relay(hop):
        for way in (1, -1):
            origin = lax.rem(me_m + mem_count - way * (hop // 2), mem_count)
            x = hop % 2 if way > 0 else 1 - hop % 2
            ref = zs.at[x, pl.ds(pl.multiple_of(origin * mdev, mdev), mdev), :]
            pltpu.make_async_remote_copy(
                src_ref=ref, dst_ref=ref,
                send_sem=ssem.at[(S_RIGHT if way > 0 else S_LEFT) + hop],
                recv_sem=rsem.at[(R_RIGHT if way > 0 else R_LEFT) + hop],
                device_id={"mem": right if way > 0 else left}, device_id_type=MESH).start()

    def relayed(hop):
        for base in (R_RIGHT, R_LEFT):
            awaited(zs.at[0, pl.ds(0, mdev), :], rsem.at[base + hop])

    plane_row = jnp.floor(cell[...].astype(f32) / slab)
    rhs = jnp.sqrt(var[...]) * noise[...] + value[...] - observed
    own = 2 * REACH
    e0[own, :mdev, :] = rhs
    e0[own, mdev:, :] = jnp.broadcast_to(plane_row, (8, odev))

    turn = 1 - 2 * my_h
    partner = {"space": me_s + turn}
    out_of_reach = REACH - 1 - my_h
    band_to = [{"space": lax.rem(me_s + away + space_count, space_count)} for away in AWAY]

    def spread(at, send, recv):
        def copy(there, to):
            pltpu.make_async_remote_copy(
                src_ref=at(own), dst_ref=at(there), send_sem=ssem.at[send], recv_sem=rsem.at[recv + there],
                device_id=to, device_id_type=MESH).start()

        for i, to in enumerate(band_to):
            copy(i ^ 1, to)
        copy(REACH + out_of_reach, partner)

    def hand_over(at, send, recv):
        def copy(i):
            pltpu.make_async_remote_copy(
                src_ref=at(i), dst_ref=at(REACH + i), send_sem=ssem.at[send], recv_sem=rsem.at[recv + REACH + i],
                device_id=partner, device_id_type=MESH).start()

        for i in range(REACH - 2):
            awaited(at(i), rsem.at[recv + i])
            copy(i)
        for i in range(REACH - 2, REACH):
            awaited(at(i), rsem.at[recv + i])
        copy(2 * REACH - 3 - out_of_reach)

    def handed(at, recv):
        for i in range(REACH, 2 * REACH):
            awaited(at(i), rsem.at[recv + i])

    def rhs_at(i):
        return e0.at[i]

    spread(rhs_at, S_RHS, R_RHS)

    near = (1, -1, 4, -4)
    chips_at = {chips: {"space": lax.rem(me_s + 2 * chips + space_count, space_count)}
                for chips in near}

    def piece_rows(step):
        origin = lax.rem(me_m + mem_count - step, mem_count)
        return pl.ds(pl.multiple_of(origin * mdev, mdev), mdev)

    def piece_send(slot, there, rows, chips):
        pltpu.make_async_remote_copy(
            src_ref=ab.at[slot, rows], dst_ref=ab.at[there, rows],
            send_sem=ssem.at[S_BAND], recv_sem=rsem.at[R_BAND + there],
            device_id=chips_at[chips], device_id_type=MESH).start()

    def to_chips(step):
        rows = piece_rows(step)
        for chips in near:
            piece_send(REACH, REACH - 2 * chips, rows, chips)

    def piece_here(step):
        awaited(ab.at[REACH, pl.ds(0, mdev)], rsem.at[R_OBS + step])

    to_chips(0)
    relay(0)
    relay(1)
    for step in (1, 7, 2, 6, 3, 5, 4):
        piece_here(step)
        to_chips(step)
    hand_over(rhs_at, S_RHS, R_RHS)

    def pair_send(e):
        pltpu.make_async_remote_copy(
            src_ref=ab.at[REACH + turn * e], dst_ref=ab.at[REACH + turn * (e - 1)],
            send_sem=ssem.at[S_PAIR], recv_sem=rsem.at[R_BAND + REACH + turn * (e - 1)],
            device_id=partner, device_id_type=MESH).start()

    def slot_here(j):
        awaited(ab.at[0], rsem.at[R_BAND + j])

    pair_send(0)

    def anomalies(j):
        raw = ab[j]
        return raw - jnp.sum(raw, axis=0, keepdims=True) / members

    anom_t = anomalies(REACH).T
    th, tl = halves(anom_t)
    both_t = jnp.concatenate([th, tl], axis=0)
    own_plane = jnp.broadcast_to(plane_row, (odev, odev)).T
    own_var = jnp.broadcast_to(var[...], (odev, odev)).T
    diagonal = (lax.broadcasted_iota(jnp.int32, (odev, odev), 0) == lax.broadcasted_iota(jnp.int32, (odev, odev), 1))
    diag_var = jnp.where(diagonal, own_var, 0.0)

    def taper(a, b):
        spread = jnp.abs(a - b)
        spread = jnp.minimum(spread, planes - spread)
        return jnp.maximum(0.0, 1.0 - spread / LOC)

    def rows_of(j, place, total, more=None):
        lanes = pl.ds(pl.multiple_of(place * odev, odev), odev)
        high, low = halves(anomalies(j))
        ah[:, lanes] = high
        al[:, lanes] = low
        gram = nn(both_t, high)
        gram = gram[:odev] + gram[odev:] + nn(th, low)
        block = taper(own_plane, e0[place, pl.ds(mdev, 1), :]) * gram / (members - 1)
        if more is not None:
            block = block + more
        chigh, clow = halves(block)
        ch[:, lanes] = chigh
        cl[:, lanes] = clow
        return total + jnp.abs(block)

    total = rows_of(REACH, own, jnp.zeros((odev, odev), f32), diag_var)

    for side in (1, -1):
        slot = REACH + 2 * side
        slot_here(slot)
        piece_send(slot, slot + 2 * side, slice(None), -side)
        edge = lax.rem(my_c, side_y) == (side_y - 1 if side > 0 else 0)
        given = jnp.where(edge, REACH, slot)
        chips = jnp.where(edge, -3 * side, 4 * side)
        there = given - 2 * chips
        pltpu.make_async_remote_copy(
            src_ref=ab.at[given], dst_ref=ab.at[there],
            send_sem=ssem.at[S_BAND], recv_sem=rsem.at[R_BAND + there],
            device_id={"space": lax.rem(me_s + 2 * chips + space_count, space_count)}, device_id_type=MESH).start()
    pair_send(2)
    pair_send(-2)
    handed(rhs_at, R_RHS)

    def pick(i, table):
        value = table[0]
        for k in range(1, len(table)):
            value = jnp.where(i == k, table[k], value)
        return value

    def place(rank, negative):
        return 2 * rank + my_h + negative - 2 * my_h * negative

    def slot_rows(e, rank, negative, total):
        return rows_of(REACH + turn * e, place(rank, negative), total)

    def partner_rows(e, rank, negative, total):
        return rows_of(REACH + turn * (1 - e), REACH + place(rank, 1 - negative), total)

    total = slot_rows(2, 2, 0, total)
    total = slot_rows(-2, 2, 1, total)

    def two_slots(i, total):
        e = pick(i, (8, 4, -4, 6, -6))
        f = pick(i, (0, 2, -2, 8, 4))
        slot_here(REACH + turn * e)
        pair_send(e)
        slot_here(REACH + turn * (1 - f))
        total = slot_rows(e, pick(i, (3, 0, 0, 1, 1)), pick(i, (0, 0, 1, 0, 1)), total)
        return partner_rows(f, pick(i, (3, 2, 2, 3, 0)), pick(i, (1, 0, 1, 0, 0)), total)

    total = lax.fori_loop(0, 1, two_slots, total)
    relayed(0)
    relay(2)
    total = lax.fori_loop(1, 5, two_slots, total)
    slot_here(REACH - turn * REACH)
    slot_here(REACH + turn * (1 + 4))
    total = slot_rows(-REACH, 3, 1, total)
    total = partner_rows(-4, 0, 1, total)
    slot_here(REACH + turn * (1 - 6))
    slot_here(REACH + turn * (1 + 6))
    total = partner_rows(6, 1, 0, total)
    total = partner_rows(-6, 1, 1, total)

    def part(block, lanes):
        high, low = halves(block)
        top = nt(jnp.concatenate([high, low], axis=0), ch[:, lanes])
        return top[:mdev] + top[mdev:] + nt(high, cl[:, lanes])

    own_lanes = slice(own * odev, (own + 1) * odev)
    lanes_out = slice(0, own * odev)

    def exchange(e, block):
        ex[e, own] = block

        def copy(there, to):
            pltpu.make_async_remote_copy(
                src_ref=ex.at[e, own], dst_ref=ex.at[e, there],
                send_sem=ssem.at[S_DIR + e], recv_sem=rsem.at[R_DIR + e],
                device_id=to, device_id_type=MESH).start()

        for i, to in enumerate(band_to):
            copy(i ^ 1, to)
            if i < REACH - 2:
                copy(REACH + (i ^ 1), {"space": lax.rem(me_s + AWAY[i] + turn + space_count, space_count)})
        copy(3 * REACH - 3 - out_of_reach,
             {"space": lax.rem(me_s - (REACH - 1) * turn + space_count, space_count)})
        copy(REACH + out_of_reach, partner)

    def arrived(e):
        awaited(ex.at[e, pl.ds(0, own)], rsem.at[R_DIR + e])
        return lambda i: ex[e, i]

    def image_of(block, values_of):
        image = part(block, own_lanes)
        values = values_of()
        for i in range(own):
            high, low = halves(values(i))
            dh[:mdev, i * odev:(i + 1) * odev] = high
            dh[mdev:, i * odev:(i + 1) * odev] = low
        top = nt(dh[...], ch[:, lanes_out])
        return image + (top[:mdev] + top[mdev:] + nt(dh[:mdev, :], cl[:, lanes_out]))

    row_max = jnp.max(jnp.sum(total, axis=1, keepdims=True), axis=0, keepdims=True)
    var_min = jnp.min(var[...], axis=1, keepdims=True)
    is_upper = lax.broadcasted_iota(jnp.int32, (8, odev), 0) < 4
    bb[me_s] = jnp.where(is_upper, row_max, -var_min)

    for to in others:
        pltpu.make_async_remote_copy(
            src_ref=bb.at[me_s], dst_ref=bb.at[me_s],
            send_sem=ssem.at[S_BOUND], recv_sem=rsem.at[R_BOUND],
            device_id={"space": to}, device_id_type=MESH).start()

    first_image = image_of(rhs, lambda: lambda i: e0[i, pl.ds(0, mdev), :])
    exchange(0, first_image)
    relayed(1)
    relay(3)
    second_image = image_of(first_image, lambda: arrived(0))

    awaited(bb.at[pl.ds(0, space_count - 1)], rsem.at[R_BOUND])
    bounds = jnp.max(bb[...], axis=0)
    upper = bounds[0:1, :]
    lower = -bounds[4:5, :]
    center = (upper + lower) / 2.0
    radius = (upper - lower) / 2.0
    sigma = center / radius
    rho = 1.0 / sigma
    direction = rhs / center
    weight = direction
    residual = rhs - first_image / center
    rho_next = 1.0 / (2.0 * sigma - rho)
    keep, take = rho_next * rho, 2.0 * rho_next / radius
    image = keep * (first_image / center) + take * (first_image - second_image / center)
    direction = keep * direction + take * residual
    rho = rho_next
    weight = weight + direction

    for e in range(1, ITERS - 2):
        residual = residual - image
        rho_next = 1.0 / (2.0 * sigma - rho)
        direction = rho_next * rho * direction + 2.0 * rho_next / radius * residual
        rho = rho_next
        weight = weight + direction
        exchange(e, direction)
        relayed(e + 1)
        relay(e + 3)
        image = image_of(direction, lambda e=e: arrived(e))
    residual = residual - image
    rho_next = 1.0 / (2.0 * sigma - rho)
    direction = rho_next * rho * direction + 2.0 * rho_next / radius * residual
    weight = weight + direction
    last = ITERS - 2
    exchange(last, weight)

    relayed(HOPS - 2)
    relayed(HOPS - 1)
    width = 512

    def split_states(i, c):
        x = lax.div(i, slab // width)
        lanes = pl.ds(pl.multiple_of(lax.rem(i, slab // width) * width, width), width)
        states = zs[x, :, lanes]
        high, low = halves(states - jnp.sum(states, axis=0, keepdims=True) / members)
        sh[x, :, lanes] = high
        sl[x, :, lanes] = low
        return c

    lax.fori_loop(0, 2 * slab // width, split_states, 0)

    base = me_s.astype(f32) * 2.0

    def gain_part(block, row, lanes):
        wide = jnp.concatenate([block * taper(base, row), block * taper(base + 1.0, row)], axis=0)
        high, low = halves(wide)
        top = nt(jnp.concatenate([high, low], axis=0), ah[:, lanes])
        return top[:2 * mdev] + top[2 * mdev:] + nt(high, al[:, lanes])

    gain = gain_part(weight, plane_row, own_lanes)
    values = arrived(last)
    for g in (slice(0, REACH), slice(REACH, own)):
        span = range(g.start, g.stop)
        rows = jnp.concatenate([e0[i, pl.ds(mdev, 1), :] for i in span], axis=1)
        block = jnp.concatenate([values(i) for i in span], axis=1)
        gain = gain + gain_part(block, rows, slice(g.start * odev, g.stop * odev))
    gain = gain / (members - 1)

    for x in range(2):
        ghigh, glow = halves(gain[x * mdev:(x + 1) * mdev])
        gboth = jnp.concatenate([ghigh, glow], axis=0)

        wide = 1024

        def update(i, c, x=x, ghigh=ghigh, gboth=gboth):
            lanes = pl.ds(pl.multiple_of(i * wide, wide), wide)
            top = nn(gboth, sh[x, :, lanes])
            out[x, :, lanes] = zs[x, mine, lanes] + (top[:mdev] + top[mdev:] + nn(ghigh, sl[x, :, lanes]))
            return c

        lax.fori_loop(0, slab // wide, update, 0)

    awaited(r.at[pl.ds(0, planes - 2)], ssem.at[S_OUT])
    awaited(fr.at[pl.ds(0, space_count - 1)], ssem.at[S_FORC])
    awaited(r.at[pl.ds(0, planes - 2)], ssem.at[S_BACK])
    awaited(ab.at[0, pl.ds(0, members - mdev)], ssem.at[S_OBS])
    awaited(e0.at[pl.ds(0, 2 * REACH)], ssem.at[S_RHS])
    awaited(ab.at[pl.ds(0, REACH)], ssem.at[S_BAND])
    awaited(ab.at[pl.ds(0, REACH)], ssem.at[S_PAIR])
    awaited(bb.at[pl.ds(0, space_count - 1)], ssem.at[S_BOUND])
    for e in range(ITERS - 1):
        awaited(ex.at[e, pl.ds(0, 2 * REACH)], ssem.at[S_DIR + e])
    for hop in range(HOPS):
        for at in (S_RIGHT, S_LEFT):
            awaited(zs.at[0, pl.ds(0, mdev), :], ssem.at[at + hop])


def shards(ensemble, forcing, obs_cell, obs_value, obs_var, obs_noise):
    mdev, pdev, slab = ensemble.shape
    odev = obs_cell.shape[0]
    space_count = lax.axis_size("space")
    mem_count = lax.axis_size("mem")
    members = mdev * mem_count
    planes = pdev * space_count
    band = SLOTS * odev

    def call(*args):
        return kernel(space_count, mem_count, *args)

    vmem = pl.BlockSpec(memory_space=pltpu.VMEM)
    analysis = pl.pallas_call(
        call,
        out_shape=jax.ShapeDtypeStruct((pdev, mdev, slab), f32),
        in_specs=[vmem] * 6,
        out_specs=vmem,
        scratch_shapes=[
            pltpu.VMEM((planes, mdev // 2, 128), f32),
            pltpu.VMEM((planes, mdev // 2, 128), f32),
            pltpu.VMEM((space_count, pdev, 128), f32),
            pltpu.VMEM((pdev, members, slab), f32),
            pltpu.VMEM((pdev, members, slab), bf16),
            pltpu.VMEM((pdev, members, slab), bf16),
            pltpu.VMEM((pdev * slab, odev), bf16),
            pltpu.VMEM((SLOTS, members, odev), f32),
            pltpu.VMEM((members, band), bf16),
            pltpu.VMEM((members, band), bf16),
            pltpu.VMEM((SLOTS, mdev + 8, odev), f32),
            pltpu.VMEM((ITERS - 1, SLOTS, mdev, odev), f32),
            pltpu.VMEM((space_count, 8, odev), f32),
            pltpu.VMEM((odev, band), bf16),
            pltpu.VMEM((odev, band), bf16),
            pltpu.VMEM((2 * mdev, 2 * REACH * odev), bf16),
            pltpu.SemaphoreType.DMA((SENDS,)),
            pltpu.SemaphoreType.DMA((RECVS,)),
            pltpu.SemaphoreType.DMA((3,)),
        ],
        compiler_params=pltpu.CompilerParams(
            collective_id=0, has_side_effects=True, vmem_limit_bytes=32 * 1024 * 1024),
        name="cycle",
    )(
        jnp.transpose(ensemble, (1, 0, 2)), forcing, obs_cell[None, :], obs_value[None, :], obs_var[None, :],
        obs_noise,
    )
    return jnp.transpose(analysis, (1, 0, 2))


def solution(mesh):
    placed = (
        P("mem", "space", None),
        P("space", None),
        P("space"),
        P("space"),
        P("space"),
        P("mem", "space"),
    )
    return jax.shard_map(
        shards, mesh=mesh, in_specs=placed, out_specs=P("mem", "space", None), check_vma=False
    )
```

```python
import jax
import jax.numpy as jnp
from jax import lax
from jax.experimental import pallas as pl
from jax.experimental.pallas import tpu as pltpu
from jax.sharding import PartitionSpec as P

FSTEPS = 4
ITERS = 6
LOC = 16
REACH = 8
SLOTS = 2 * REACH + 1
MESH = pl.DeviceIdType.MESH
AWAY = (4, -4, 6, -6, 2, -2, 8, -8)
STEPS = (
    (2, 2), (2, 1), (1, 2), (2, 3), (3, 2), (1, 1), (3, 3), (1, 3),
    (3, 1), (2, 0), (0, 2), (1, 0), (0, 1), (3, 0), (0, 3), (0, 0),
)
f32 = jnp.float32
bf16 = jnp.bfloat16

HOPS = 7
R_OUT, R_FORC, R_BACK, R_BOUND = range(4)
R_RHS = 4
R_DIR = R_RHS + 2 * REACH
R_OBS = R_DIR + ITERS - 1
R_BAND = R_OBS + 8
R_RIGHT = R_BAND + SLOTS
R_LEFT = R_RIGHT + HOPS
RECVS = R_LEFT + HOPS
S_OUT, S_FORC, S_BACK, S_OBS, S_RHS, S_BAND, S_PAIR, S_BOUND = range(8)
S_DIR = 8
S_RIGHT = S_DIR + ITERS - 1
S_LEFT = S_RIGHT + HOPS
SENDS = S_LEFT + HOPS

NT = (((1,), (1,)), ((), ()))


def nn(a, b):
    return jnp.dot(a, b, preferred_element_type=f32)


def nt(a, b):
    return lax.dot_general(a, b, NT, preferred_element_type=f32)


def halves(x):
    high = x.astype(bf16)
    return high, (x - high.astype(f32)).astype(bf16)


def awaited(ref, sem):
    pltpu.make_async_copy(ref, ref, sem).wait()


def kernel(
    space_count, mem_count,
    ens, forc, cell, value, var, noise,
    out,
    r, t, fr, zs, sh, sl, oh, ab, ah, al, e0, ex, bb, ch, cl, dh,
    ssem, rsem, lsem,
):
    me_s = lax.axis_index("space")
    me_m = lax.axis_index("mem")
    members = ab.shape[1]
    mdev = noise.shape[0]
    planes = r.shape[0]
    half = mdev // 2
    odev = cell.shape[1]
    slab = ens.shape[2]

    def chunk_of(index):
        return lax.div(index, 2), lax.rem(index, 2)

    def other(base, step, count):
        return lax.rem(base + step, count)

    my_c, my_h = chunk_of(me_s)
    side_y = 4
    side_x = space_count // 2 // side_y
    others = []
    for dx, dy in STEPS:
        chip = lax.rem(lax.div(my_c, side_y) + dx, side_x) * side_y + lax.rem(lax.rem(my_c, side_y) + dy, side_y)
        others.append(2 * chip + (1 - my_h))
        if (dx, dy) != (0, 0):
            others.append(2 * chip + my_h)

    barrier = pltpu.get_barrier_semaphore()

    def greet_space(i, c):
        pl.semaphore_signal(barrier, inc=1, device_id={"space": other(me_s, i, space_count)}, device_id_type=MESH)
        return c

    def greet_mem(i, c):
        pl.semaphore_signal(barrier, inc=1, device_id={"mem": other(me_m, i, mem_count)}, device_id_type=MESH)
        return c

    lax.fori_loop(1, space_count, greet_space, 0)
    lax.fori_loop(1, mem_count, greet_mem, 0)

    own_out = pltpu.make_async_copy(
        ens.at[:, pl.ds(pl.multiple_of(my_h * half, half), half), pl.ds(pl.multiple_of(my_c * 128, 128), 128)],
        r.at[pl.ds(me_s * 2, 2)], lsem.at[0])
    own_forc = pltpu.make_async_copy(
        forc.at[:, pl.ds(pl.multiple_of(my_c * 128, 128), 128)], fr.at[me_s], lsem.at[1])
    own_out.start()
    own_forc.start()

    pl.semaphore_wait(barrier, space_count + mem_count - 2)

    for to in others:
        tc, th = chunk_of(to)
        cells = pl.ds(pl.multiple_of(tc * 128, 128), 128)
        pltpu.make_async_remote_copy(
            src_ref=forc.at[:, cells], dst_ref=fr.at[me_s],
            send_sem=ssem.at[S_FORC], recv_sem=rsem.at[R_FORC],
            device_id={"space": to}, device_id_type=MESH).start()
        pltpu.make_async_remote_copy(
            src_ref=ens.at[:, pl.ds(pl.multiple_of(th * half, half), half), cells],
            dst_ref=r.at[pl.ds(me_s * 2, 2)],
            send_sem=ssem.at[S_OUT], recv_sem=rsem.at[R_OUT],
            device_id={"space": to}, device_id_type=MESH).start()

    cells_here = cell[...] - me_s * (2 * slab)

    def one_hot(i, c):
        rows = lax.broadcasted_iota(jnp.int32, (256, odev), 0) + i * 256
        oh[pl.ds(pl.multiple_of(i * 256, 256), 256), :] = jnp.where(rows == cells_here, 1.0, 0.0).astype(bf16)
        return c

    lax.fori_loop(0, 2 * slab // 256, one_hot, 0)

    own_out.wait()
    own_forc.wait()
    awaited(r.at[pl.ds(0, planes - 2)], rsem.at[R_OUT])
    awaited(fr.at[pl.ds(0, space_count - 1)], rsem.at[R_FORC])

    def advance(src, dst):
        def group(g, carry):
            two, one, now = carry
            for i in range(8):
                x = g * 8 + i
                ahead = src[lax.rem(x + 1, planes)]
                force = fr[g * 4 + i // 2, pl.ds(i % 2, 1), :]
                dst[x] = now + 0.05 * ((ahead - two) * one - now + force)
                two, one, now = one, now, ahead
            return two, one, now

        lax.fori_loop(0, planes // 8, group, (src[planes - 2], src[planes - 1], src[0]))

    for step in range(FSTEPS // 2):
        advance(r, t)
        advance(t, r)

    mine = pl.ds(pl.multiple_of(me_m * mdev, mdev), mdev)
    my_rows = pl.ds(pl.multiple_of(me_m * mdev + my_h * half, half), half)
    my_cells = pl.ds(pl.multiple_of(my_c * 128, 128), 128)

    for to in others:
        pltpu.make_async_remote_copy(
            src_ref=r.at[pl.ds(to * 2, 2)], dst_ref=zs.at[:, my_rows, my_cells],
            send_sem=ssem.at[S_BACK], recv_sem=rsem.at[R_BACK],
            device_id={"space": to}, device_id_type=MESH).start()
    own_back = pltpu.make_async_copy(r.at[pl.ds(me_s * 2, 2)], zs.at[:, my_rows, my_cells], lsem.at[2])
    own_back.start()
    own_back.wait()
    awaited(r.at[pl.ds(0, planes - 2)], rsem.at[R_BACK])

    observed = jnp.zeros((3 * mdev, odev), f32)
    for x in range(2):
        block = zs[x, mine, :]
        first = block.astype(bf16)
        rest = block - first.astype(f32)
        second = rest.astype(bf16)
        third = (rest - second.astype(f32)).astype(bf16)
        pieces = jnp.concatenate([first, second, third], axis=0)
        observed = observed + nn(pieces, oh[x * slab:(x + 1) * slab, :])
    observed = observed[:mdev] + observed[mdev:2 * mdev] + observed[2 * mdev:]
    ab[REACH, mine, :] = observed

    def send_obs(i, c):
        pltpu.make_async_remote_copy(
            src_ref=ab.at[REACH, mine], dst_ref=ab.at[REACH, mine],
            send_sem=ssem.at[S_OBS], recv_sem=rsem.at[R_OBS + i],
            device_id={"mem": other(me_m, i, mem_count)}, device_id_type=MESH).start()
        return c

    lax.fori_loop(1, mem_count, send_obs, 0)

    right = other(me_m, 1, mem_count)
    left = other(me_m, mem_count - 1, mem_count)

    def relay(hop):
        for way in (1, -1):
            origin = lax.rem(me_m + mem_count - way * (hop // 2), mem_count)
            x = hop % 2 if way > 0 else 1 - hop % 2
            ref = zs.at[x, pl.ds(pl.multiple_of(origin * mdev, mdev), mdev), :]
            pltpu.make_async_remote_copy(
                src_ref=ref, dst_ref=ref,
                send_sem=ssem.at[(S_RIGHT if way > 0 else S_LEFT) + hop],
                recv_sem=rsem.at[(R_RIGHT if way > 0 else R_LEFT) + hop],
                device_id={"mem": right if way > 0 else left}, device_id_type=MESH).start()

    def relayed(hop):
        for base in (R_RIGHT, R_LEFT):
            awaited(zs.at[0, pl.ds(0, mdev), :], rsem.at[base + hop])

    plane_row = jnp.floor(cell[...].astype(f32) / slab)
    rhs = jnp.sqrt(var[...]) * noise[...] + value[...] - observed
    own = 2 * REACH
    e0[own, :mdev, :] = rhs
    e0[own, mdev:, :] = jnp.broadcast_to(plane_row, (8, odev))

    turn = 1 - 2 * my_h
    partner = {"space": me_s + turn}
    out_of_reach = REACH - 1 - my_h
    band_to = [{"space": lax.rem(me_s + away + space_count, space_count)} for away in AWAY]

    def spread(at, send, recv):
        def copy(there, to):
            pltpu.make_async_remote_copy(
                src_ref=at(own), dst_ref=at(there), send_sem=ssem.at[send], recv_sem=rsem.at[recv + there],
                device_id=to, device_id_type=MESH).start()

        for i, to in enumerate(band_to):
            copy(i ^ 1, to)
        copy(REACH + out_of_reach, partner)

    def hand_over(at, send, recv):
        def copy(i):
            pltpu.make_async_remote_copy(
                src_ref=at(i), dst_ref=at(REACH + i), send_sem=ssem.at[send], recv_sem=rsem.at[recv + REACH + i],
                device_id=partner, device_id_type=MESH).start()

        for i in range(REACH - 2):
            awaited(at(i), rsem.at[recv + i])
            copy(i)
        for i in range(REACH - 2, REACH):
            awaited(at(i), rsem.at[recv + i])
        copy(2 * REACH - 3 - out_of_reach)

    def handed(at, recv):
        for i in range(REACH, 2 * REACH):
            awaited(at(i), rsem.at[recv + i])

    def rhs_at(i):
        return e0.at[i]

    spread(rhs_at, S_RHS, R_RHS)

    near = (1, -1, 4, -4)
    chips_at = {chips: {"space": lax.rem(me_s + 2 * chips + space_count, space_count)}
                for chips in near}

    def piece_rows(step):
        origin = lax.rem(me_m + mem_count - step, mem_count)
        return pl.ds(pl.multiple_of(origin * mdev, mdev), mdev)

    def piece_send(slot, there, rows, chips):
        pltpu.make_async_remote_copy(
            src_ref=ab.at[slot, rows], dst_ref=ab.at[there, rows],
            send_sem=ssem.at[S_BAND], recv_sem=rsem.at[R_BAND + there],
            device_id=chips_at[chips], device_id_type=MESH).start()

    def to_chips(step):
        rows = piece_rows(step)
        for chips in near:
            piece_send(REACH, REACH - 2 * chips, rows, chips)

    def piece_here(step):
        awaited(ab.at[REACH, pl.ds(0, mdev)], rsem.at[R_OBS + step])

    to_chips(0)
    relay(0)
    relay(1)
    for step in (1, 7, 2, 6, 3, 5, 4):
        piece_here(step)
        to_chips(step)
    hand_over(rhs_at, S_RHS, R_RHS)

    def pair_send(e):
        pltpu.make_async_remote_copy(
            src_ref=ab.at[REACH + turn * e], dst_ref=ab.at[REACH + turn * (e - 1)],
            send_sem=ssem.at[S_PAIR], recv_sem=rsem.at[R_BAND + REACH + turn * (e - 1)],
            device_id=partner, device_id_type=MESH).start()

    def slot_here(j):
        awaited(ab.at[0], rsem.at[R_BAND + j])

    pair_send(0)

    def anomalies(j):
        raw = ab[j]
        return raw - jnp.sum(raw, axis=0, keepdims=True) / members

    anom_t = anomalies(REACH).T
    th, tl = halves(anom_t)
    both_t = jnp.concatenate([th, tl], axis=0)
    own_plane = jnp.broadcast_to(plane_row, (odev, odev)).T
    own_var = jnp.broadcast_to(var[...], (odev, odev)).T
    diagonal = (lax.broadcasted_iota(jnp.int32, (odev, odev), 0) == lax.broadcasted_iota(jnp.int32, (odev, odev), 1))
    diag_var = jnp.where(diagonal, own_var, 0.0)

    def taper(a, b):
        spread = jnp.abs(a - b)
        spread = jnp.minimum(spread, planes - spread)
        return jnp.maximum(0.0, 1.0 - spread / LOC)

    def rows_of(j, place, total, more=None):
        lanes = pl.ds(pl.multiple_of(place * odev, odev), odev)
        high, low = halves(anomalies(j))
        ah[:, lanes] = high
        al[:, lanes] = low
        gram = nn(both_t, high)
        gram = gram[:odev] + gram[odev:] + nn(th, low)
        block = taper(own_plane, e0[place, pl.ds(mdev, 1), :]) * gram / (members - 1)
        if more is not None:
            block = block + more
        chigh, clow = halves(block)
        ch[:, lanes] = chigh
        cl[:, lanes] = clow
        return total + jnp.abs(block)

    total = rows_of(REACH, own, jnp.zeros((odev, odev), f32), diag_var)

    def pass_on(given, chips):
        there = given - 2 * chips
        pltpu.make_async_remote_copy(
            src_ref=ab.at[given], dst_ref=ab.at[there],
            send_sem=ssem.at[S_BAND], recv_sem=rsem.at[R_BAND + there],
            device_id={"space": lax.rem(me_s + 2 * chips + space_count, space_count)}, device_id_type=MESH).start()

    my_y = lax.rem(my_c, side_y)
    first_side = jnp.where(my_y == side_y - 1, -1, 1)
    for side in (first_side, -first_side):
        slot = REACH + 2 * side
        slot_here(slot)
        pass_on(slot, -side)
        edge = my_y == jnp.where(side > 0, side_y - 1, 0)
        pass_on(jnp.where(edge, REACH, slot), jnp.where(edge, -3 * side, 4 * side))
    pair_send(2)
    pair_send(-2)
    handed(rhs_at, R_RHS)

    def pick(i, table):
        value = table[0]
        for k in range(1, len(table)):
            value = jnp.where(i == k, table[k], value)
        return value

    def place(rank, negative):
        return 2 * rank + my_h + negative - 2 * my_h * negative

    def slot_rows(e, rank, negative, total):
        return rows_of(REACH + turn * e, place(rank, negative), total)

    def partner_rows(e, rank, negative, total):
        return rows_of(REACH + turn * (1 - e), REACH + place(rank, 1 - negative), total)

    total = slot_rows(2, 2, 0, total)
    total = slot_rows(-2, 2, 1, total)

    def two_slots(i, total):
        e = pick(i, (8, 4, -4, 6, -6))
        f = pick(i, (0, 2, -2, 8, 4))
        slot_here(REACH + turn * e)
        pair_send(e)
        slot_here(REACH + turn * (1 - f))
        total = slot_rows(e, pick(i, (3, 0, 0, 1, 1)), pick(i, (0, 0, 1, 0, 1)), total)
        return partner_rows(f, pick(i, (3, 2, 2, 3, 0)), pick(i, (1, 0, 1, 0, 0)), total)

    total = lax.fori_loop(0, 1, two_slots, total)
    relayed(0)
    relay(2)
    total = lax.fori_loop(1, 5, two_slots, total)
    slot_here(REACH - turn * REACH)
    slot_here(REACH + turn * (1 + 4))
    total = slot_rows(-REACH, 3, 1, total)
    total = partner_rows(-4, 0, 1, total)
    slot_here(REACH + turn * (1 - 6))
    slot_here(REACH + turn * (1 + 6))
    total = partner_rows(6, 1, 0, total)
    total = partner_rows(-6, 1, 1, total)

    def part(block, lanes):
        high, low = halves(block)
        top = nt(jnp.concatenate([high, low], axis=0), ch[:, lanes])
        return top[:mdev] + top[mdev:] + nt(high, cl[:, lanes])

    own_lanes = slice(own * odev, (own + 1) * odev)
    lanes_out = slice(0, own * odev)

    def exchange(e, block):
        ex[e, own] = block

        def copy(there, to):
            pltpu.make_async_remote_copy(
                src_ref=ex.at[e, own], dst_ref=ex.at[e, there],
                send_sem=ssem.at[S_DIR + e], recv_sem=rsem.at[R_DIR + e],
                device_id=to, device_id_type=MESH).start()

        for i, to in enumerate(band_to):
            copy(i ^ 1, to)
            if i < REACH - 2:
                copy(REACH + (i ^ 1), {"space": lax.rem(me_s + AWAY[i] + turn + space_count, space_count)})
        copy(3 * REACH - 3 - out_of_reach,
             {"space": lax.rem(me_s - (REACH - 1) * turn + space_count, space_count)})
        copy(REACH + out_of_reach, partner)

    def arrived(e):
        awaited(ex.at[e, pl.ds(0, own)], rsem.at[R_DIR + e])
        return lambda i: ex[e, i]

    def image_of(block, values_of):
        image = part(block, own_lanes)
        values = values_of()
        for i in range(own):
            high, low = halves(values(i))
            dh[:mdev, i * odev:(i + 1) * odev] = high
            dh[mdev:, i * odev:(i + 1) * odev] = low
        top = nt(dh[...], ch[:, lanes_out])
        return image + (top[:mdev] + top[mdev:] + nt(dh[:mdev, :], cl[:, lanes_out]))

    row_max = jnp.max(jnp.sum(total, axis=1, keepdims=True), axis=0, keepdims=True)
    var_min = jnp.min(var[...], axis=1, keepdims=True)
    is_upper = lax.broadcasted_iota(jnp.int32, (8, odev), 0) < 4
    bb[me_s] = jnp.where(is_upper, row_max, -var_min)

    for to in others:
        pltpu.make_async_remote_copy(
            src_ref=bb.at[me_s], dst_ref=bb.at[me_s],
            send_sem=ssem.at[S_BOUND], recv_sem=rsem.at[R_BOUND],
            device_id={"space": to}, device_id_type=MESH).start()

    first_image = image_of(rhs, lambda: lambda i: e0[i, pl.ds(0, mdev), :])
    exchange(0, first_image)
    relayed(1)
    relay(3)
    second_image = image_of(first_image, lambda: arrived(0))

    awaited(bb.at[pl.ds(0, space_count - 1)], rsem.at[R_BOUND])
    bounds = jnp.max(bb[...], axis=0)
    upper = bounds[0:1, :]
    lower = -bounds[4:5, :]
    center = (upper + lower) / 2.0
    radius = (upper - lower) / 2.0
    sigma = center / radius
    rho = 1.0 / sigma
    direction = rhs / center
    weight = direction
    residual = rhs - first_image / center
    rho_next = 1.0 / (2.0 * sigma - rho)
    keep, take = rho_next * rho, 2.0 * rho_next / radius
    image = keep * (first_image / center) + take * (first_image - second_image / center)
    direction = keep * direction + take * residual
    rho = rho_next
    weight = weight + direction

    for e in range(1, ITERS - 2):
        residual = residual - image
        rho_next = 1.0 / (2.0 * sigma - rho)
        direction = rho_next * rho * direction + 2.0 * rho_next / radius * residual
        rho = rho_next
        weight = weight + direction
        exchange(e, direction)
        relayed(e + 1)
        relay(e + 3)
        image = image_of(direction, lambda e=e: arrived(e))
    residual = residual - image
    rho_next = 1.0 / (2.0 * sigma - rho)
    direction = rho_next * rho * direction + 2.0 * rho_next / radius * residual
    weight = weight + direction
    last = ITERS - 2
    exchange(last, weight)

    relayed(HOPS - 2)
    relayed(HOPS - 1)
    width = 512

    def split_states(i, c):
        x = lax.div(i, slab // width)
        lanes = pl.ds(pl.multiple_of(lax.rem(i, slab // width) * width, width), width)
        states = zs[x, :, lanes]
        high, low = halves(states - jnp.sum(states, axis=0, keepdims=True) / members)
        sh[x, :, lanes] = high
        sl[x, :, lanes] = low
        return c

    lax.fori_loop(0, 2 * slab // width, split_states, 0)

    base = me_s.astype(f32) * 2.0

    def gain_part(block, row, lanes):
        wide = jnp.concatenate([block * taper(base, row), block * taper(base + 1.0, row)], axis=0)
        high, low = halves(wide)
        top = nt(jnp.concatenate([high, low], axis=0), ah[:, lanes])
        return top[:2 * mdev] + top[2 * mdev:] + nt(high, al[:, lanes])

    gain = gain_part(weight, plane_row, own_lanes)
    values = arrived(last)
    for g in (slice(0, REACH), slice(REACH, own)):
        span = range(g.start, g.stop)
        rows = jnp.concatenate([e0[i, pl.ds(mdev, 1), :] for i in span], axis=1)
        block = jnp.concatenate([values(i) for i in span], axis=1)
        gain = gain + gain_part(block, rows, slice(g.start * odev, g.stop * odev))
    gain = gain / (members - 1)

    for x in range(2):
        ghigh, glow = halves(gain[x * mdev:(x + 1) * mdev])
        gboth = jnp.concatenate([ghigh, glow], axis=0)

        wide = 1024

        def update(i, c, x=x, ghigh=ghigh, gboth=gboth):
            lanes = pl.ds(pl.multiple_of(i * wide, wide), wide)
            top = nn(gboth, sh[x, :, lanes])
            out[x, :, lanes] = zs[x, mine, lanes] + (top[:mdev] + top[mdev:] + nn(ghigh, sl[x, :, lanes]))
            return c

        lax.fori_loop(0, slab // wide, update, 0)

    awaited(r.at[pl.ds(0, planes - 2)], ssem.at[S_OUT])
    awaited(fr.at[pl.ds(0, space_count - 1)], ssem.at[S_FORC])
    awaited(r.at[pl.ds(0, planes - 2)], ssem.at[S_BACK])
    awaited(ab.at[0, pl.ds(0, members - mdev)], ssem.at[S_OBS])
    awaited(e0.at[pl.ds(0, 2 * REACH)], ssem.at[S_RHS])
    awaited(ab.at[pl.ds(0, REACH)], ssem.at[S_BAND])
    awaited(ab.at[pl.ds(0, REACH)], ssem.at[S_PAIR])
    awaited(bb.at[pl.ds(0, space_count - 1)], ssem.at[S_BOUND])
    for e in range(ITERS - 1):
        awaited(ex.at[e, pl.ds(0, 2 * REACH)], ssem.at[S_DIR + e])
    for hop in range(HOPS):
        for at in (S_RIGHT, S_LEFT):
            awaited(zs.at[0, pl.ds(0, mdev), :], ssem.at[at + hop])


def shards(ensemble, forcing, obs_cell, obs_value, obs_var, obs_noise):
    mdev, pdev, slab = ensemble.shape
    odev = obs_cell.shape[0]
    space_count = lax.axis_size("space")
    mem_count = lax.axis_size("mem")
    members = mdev * mem_count
    planes = pdev * space_count
    band = SLOTS * odev

    def call(*args):
        return kernel(space_count, mem_count, *args)

    vmem = pl.BlockSpec(memory_space=pltpu.VMEM)
    analysis = pl.pallas_call(
        call,
        out_shape=jax.ShapeDtypeStruct((pdev, mdev, slab), f32),
        in_specs=[vmem] * 6,
        out_specs=vmem,
        scratch_shapes=[
            pltpu.VMEM((planes, mdev // 2, 128), f32),
            pltpu.VMEM((planes, mdev // 2, 128), f32),
            pltpu.VMEM((space_count, pdev, 128), f32),
            pltpu.VMEM((pdev, members, slab), f32),
            pltpu.VMEM((pdev, members, slab), bf16),
            pltpu.VMEM((pdev, members, slab), bf16),
            pltpu.VMEM((pdev * slab, odev), bf16),
            pltpu.VMEM((SLOTS, members, odev), f32),
            pltpu.VMEM((members, band), bf16),
            pltpu.VMEM((members, band), bf16),
            pltpu.VMEM((SLOTS, mdev + 8, odev), f32),
            pltpu.VMEM((ITERS - 1, SLOTS, mdev, odev), f32),
            pltpu.VMEM((space_count, 8, odev), f32),
            pltpu.VMEM((odev, band), bf16),
            pltpu.VMEM((odev, band), bf16),
            pltpu.VMEM((2 * mdev, 2 * REACH * odev), bf16),
            pltpu.SemaphoreType.DMA((SENDS,)),
            pltpu.SemaphoreType.DMA((RECVS,)),
            pltpu.SemaphoreType.DMA((3,)),
        ],
        compiler_params=pltpu.CompilerParams(
            collective_id=0, has_side_effects=True, vmem_limit_bytes=32 * 1024 * 1024),
        name="cycle",
    )(
        jnp.transpose(ensemble, (1, 0, 2)), forcing, obs_cell[None, :], obs_value[None, :], obs_var[None, :],
        obs_noise,
    )
    return jnp.transpose(analysis, (1, 0, 2))


def solution(mesh):
    placed = (
        P("mem", "space", None),
        P("space", None),
        P("space"),
        P("space"),
        P("space"),
        P("mem", "space"),
    )
    return jax.shard_map(
        shards, mesh=mesh, in_specs=placed, out_specs=P("mem", "space", None), check_vma=False
    )
```

```python
import jax
import jax.numpy as jnp
from jax import lax
from jax.experimental import pallas as pl
from jax.experimental.pallas import tpu as pltpu
from jax.sharding import PartitionSpec as P

FSTEPS = 4
ITERS = 6
LOC = 16
REACH = 8
SLOTS = 2 * REACH + 1
MESH = pl.DeviceIdType.MESH
AWAY = (4, -4, 6, -6, 2, -2, 8, -8)
STEPS = (
    (2, 2), (2, 1), (1, 2), (2, 3), (3, 2), (1, 1), (3, 3), (1, 3),
    (3, 1), (2, 0), (0, 2), (1, 0), (0, 1), (3, 0), (0, 3), (0, 0),
)
f32 = jnp.float32
bf16 = jnp.bfloat16

HOPS = 7
R_OUT, R_FORC, R_BACK, R_BOUND = range(4)
R_RHS = 4
R_DIR = R_RHS + 2 * REACH
R_OBS = R_DIR + ITERS - 1
R_BAND = R_OBS + 8
R_RIGHT = R_BAND + SLOTS
R_LEFT = R_RIGHT + HOPS
RECVS = R_LEFT + HOPS
S_OUT, S_FORC, S_BACK, S_OBS, S_RHS, S_BAND, S_PAIR, S_BOUND = range(8)
S_DIR = 8
S_RIGHT = S_DIR + ITERS - 1
S_LEFT = S_RIGHT + HOPS
SENDS = S_LEFT + HOPS

NT = (((1,), (1,)), ((), ()))


def nn(a, b):
    return jnp.dot(a, b, preferred_element_type=f32)


def nt(a, b):
    return lax.dot_general(a, b, NT, preferred_element_type=f32)


def halves(x):
    high = x.astype(bf16)
    return high, (x - high.astype(f32)).astype(bf16)


def awaited(ref, sem):
    pltpu.make_async_copy(ref, ref, sem).wait()


def kernel(
    space_count, mem_count,
    ens, forc, cell, value, var, noise,
    out,
    r, t, fr, zs, sh, sl, oh, ab, ah, al, e0, ex, bb, ch, cl, dh,
    ssem, rsem, lsem,
):
    me_s = lax.axis_index("space")
    me_m = lax.axis_index("mem")
    members = ab.shape[1]
    mdev = noise.shape[0]
    planes = r.shape[0]
    half = mdev // 2
    odev = cell.shape[1]
    slab = ens.shape[2]

    def chunk_of(index):
        return lax.div(index, 2), lax.rem(index, 2)

    def other(base, step, count):
        return lax.rem(base + step, count)

    my_c, my_h = chunk_of(me_s)
    side_y = 4
    side_x = space_count // 2 // side_y
    others = []
    for dx, dy in STEPS:
        chip = lax.rem(lax.div(my_c, side_y) + dx, side_x) * side_y + lax.rem(lax.rem(my_c, side_y) + dy, side_y)
        others.append(2 * chip + (1 - my_h))
        if (dx, dy) != (0, 0):
            others.append(2 * chip + my_h)

    barrier = pltpu.get_barrier_semaphore()

    def greet_space(i, c):
        pl.semaphore_signal(barrier, inc=1, device_id={"space": other(me_s, i, space_count)}, device_id_type=MESH)
        return c

    def greet_mem(i, c):
        pl.semaphore_signal(barrier, inc=1, device_id={"mem": other(me_m, i, mem_count)}, device_id_type=MESH)
        return c

    lax.fori_loop(1, space_count, greet_space, 0)
    lax.fori_loop(1, mem_count, greet_mem, 0)

    own_out = pltpu.make_async_copy(
        ens.at[:, pl.ds(pl.multiple_of(my_h * half, half), half), pl.ds(pl.multiple_of(my_c * 128, 128), 128)],
        r.at[pl.ds(me_s * 2, 2)], lsem.at[0])
    own_forc = pltpu.make_async_copy(
        forc.at[:, pl.ds(pl.multiple_of(my_c * 128, 128), 128)], fr.at[me_s], lsem.at[1])
    own_out.start()
    own_forc.start()

    pl.semaphore_wait(barrier, space_count + mem_count - 2)

    for to in others:
        tc, th = chunk_of(to)
        cells = pl.ds(pl.multiple_of(tc * 128, 128), 128)
        pltpu.make_async_remote_copy(
            src_ref=forc.at[:, cells], dst_ref=fr.at[me_s],
            send_sem=ssem.at[S_FORC], recv_sem=rsem.at[R_FORC],
            device_id={"space": to}, device_id_type=MESH).start()
        pltpu.make_async_remote_copy(
            src_ref=ens.at[:, pl.ds(pl.multiple_of(th * half, half), half), cells],
            dst_ref=r.at[pl.ds(me_s * 2, 2)],
            send_sem=ssem.at[S_OUT], recv_sem=rsem.at[R_OUT],
            device_id={"space": to}, device_id_type=MESH).start()

    cells_here = cell[...] - me_s * (2 * slab)

    def one_hot(i, c):
        rows = lax.broadcasted_iota(jnp.int32, (256, odev), 0) + i * 256
        oh[pl.ds(pl.multiple_of(i * 256, 256), 256), :] = jnp.where(rows == cells_here, 1.0, 0.0).astype(bf16)
        return c

    lax.fori_loop(0, 2 * slab // 256, one_hot, 0)

    own_out.wait()
    own_forc.wait()
    awaited(r.at[pl.ds(0, planes - 2)], rsem.at[R_OUT])
    awaited(fr.at[pl.ds(0, space_count - 1)], rsem.at[R_FORC])

    def advance(src, dst):
        def group(g, carry):
            two, one, now = carry
            for i in range(8):
                x = g * 8 + i
                ahead = src[lax.rem(x + 1, planes)]
                force = fr[g * 4 + i // 2, pl.ds(i % 2, 1), :]
                dst[x] = now + 0.05 * ((ahead - two) * one - now + force)
                two, one, now = one, now, ahead
            return two, one, now

        lax.fori_loop(0, planes // 8, group, (src[planes - 2], src[planes - 1], src[0]))

    for step in range(FSTEPS // 2):
        advance(r, t)
        advance(t, r)

    mine = pl.ds(pl.multiple_of(me_m * mdev, mdev), mdev)
    my_rows = pl.ds(pl.multiple_of(me_m * mdev + my_h * half, half), half)
    my_cells = pl.ds(pl.multiple_of(my_c * 128, 128), 128)

    for to in others:
        pltpu.make_async_remote_copy(
            src_ref=r.at[pl.ds(to * 2, 2)], dst_ref=zs.at[:, my_rows, my_cells],
            send_sem=ssem.at[S_BACK], recv_sem=rsem.at[R_BACK],
            device_id={"space": to}, device_id_type=MESH).start()
    own_back = pltpu.make_async_copy(r.at[pl.ds(me_s * 2, 2)], zs.at[:, my_rows, my_cells], lsem.at[2])
    own_back.start()
    own_back.wait()
    awaited(r.at[pl.ds(0, planes - 2)], rsem.at[R_BACK])

    observed = jnp.zeros((3 * mdev, odev), f32)
    for x in range(2):
        block = zs[x, mine, :]
        first = block.astype(bf16)
        rest = block - first.astype(f32)
        second = rest.astype(bf16)
        third = (rest - second.astype(f32)).astype(bf16)
        pieces = jnp.concatenate([first, second, third], axis=0)
        observed = observed + nn(pieces, oh[x * slab:(x + 1) * slab, :])
    observed = observed[:mdev] + observed[mdev:2 * mdev] + observed[2 * mdev:]
    ab[REACH, mine, :] = observed

    for i in (4, 3, 5, 2, 6, 1, 7):
        pltpu.make_async_remote_copy(
            src_ref=ab.at[REACH, mine], dst_ref=ab.at[REACH, mine],
            send_sem=ssem.at[S_OBS], recv_sem=rsem.at[R_OBS + i],
            device_id={"mem": other(me_m, i, mem_count)}, device_id_type=MESH).start()

    right = other(me_m, 1, mem_count)
    left = other(me_m, mem_count - 1, mem_count)

    def relay(hop):
        for way in (1, -1):
            origin = lax.rem(me_m + mem_count - way * (hop // 2), mem_count)
            x = hop % 2 if way > 0 else 1 - hop % 2
            ref = zs.at[x, pl.ds(pl.multiple_of(origin * mdev, mdev), mdev), :]
            pltpu.make_async_remote_copy(
                src_ref=ref, dst_ref=ref,
                send_sem=ssem.at[(S_RIGHT if way > 0 else S_LEFT) + hop],
                recv_sem=rsem.at[(R_RIGHT if way > 0 else R_LEFT) + hop],
                device_id={"mem": right if way > 0 else left}, device_id_type=MESH).start()

    def relayed(hop):
        for base in (R_RIGHT, R_LEFT):
            awaited(zs.at[0, pl.ds(0, mdev), :], rsem.at[base + hop])

    plane_row = jnp.floor(cell[...].astype(f32) / slab)
    rhs = jnp.sqrt(var[...]) * noise[...] + value[...] - observed
    own = 2 * REACH
    e0[own, :mdev, :] = rhs
    e0[own, mdev:, :] = jnp.broadcast_to(plane_row, (8, odev))

    turn = 1 - 2 * my_h
    partner = {"space": me_s + turn}
    out_of_reach = REACH - 1 - my_h
    band_to = [{"space": lax.rem(me_s + away + space_count, space_count)} for away in AWAY]

    def spread(at, send, recv):
        def copy(there, to):
            pltpu.make_async_remote_copy(
                src_ref=at(own), dst_ref=at(there), send_sem=ssem.at[send], recv_sem=rsem.at[recv + there],
                device_id=to, device_id_type=MESH).start()

        for i, to in enumerate(band_to):
            copy(i ^ 1, to)
        copy(REACH + out_of_reach, partner)

    def hand_over(at, send, recv):
        def copy(i):
            pltpu.make_async_remote_copy(
                src_ref=at(i), dst_ref=at(REACH + i), send_sem=ssem.at[send], recv_sem=rsem.at[recv + REACH + i],
                device_id=partner, device_id_type=MESH).start()

        for i in range(REACH - 2):
            awaited(at(i), rsem.at[recv + i])
            copy(i)
        for i in range(REACH - 2, REACH):
            awaited(at(i), rsem.at[recv + i])
        copy(2 * REACH - 3 - out_of_reach)

    def handed(at, recv):
        for i in range(REACH, 2 * REACH):
            awaited(at(i), rsem.at[recv + i])

    def rhs_at(i):
        return e0.at[i]

    spread(rhs_at, S_RHS, R_RHS)

    near = (1, -1, 4, -4)
    chips_at = {chips: {"space": lax.rem(me_s + 2 * chips + space_count, space_count)}
                for chips in near}

    def piece_rows(step):
        origin = lax.rem(me_m + mem_count - step, mem_count)
        return pl.ds(pl.multiple_of(origin * mdev, mdev), mdev)

    def piece_send(slot, there, rows, chips):
        pltpu.make_async_remote_copy(
            src_ref=ab.at[slot, rows], dst_ref=ab.at[there, rows],
            send_sem=ssem.at[S_BAND], recv_sem=rsem.at[R_BAND + there],
            device_id=chips_at[chips], device_id_type=MESH).start()

    def to_chips(step):
        rows = piece_rows(step)
        for chips in near:
            piece_send(REACH, REACH - 2 * chips, rows, chips)

    def piece_here(step):
        awaited(ab.at[REACH, pl.ds(0, mdev)], rsem.at[R_OBS + step])

    to_chips(0)
    relay(0)
    relay(1)
    for step in (1, 7, 2, 6, 3, 5, 4):
        piece_here(step)
        to_chips(step)
    hand_over(rhs_at, S_RHS, R_RHS)

    def pair_send(e):
        pltpu.make_async_remote_copy(
            src_ref=ab.at[REACH + turn * e], dst_ref=ab.at[REACH + turn * (e - 1)],
            send_sem=ssem.at[S_PAIR], recv_sem=rsem.at[R_BAND + REACH + turn * (e - 1)],
            device_id=partner, device_id_type=MESH).start()

    def slot_here(j):
        awaited(ab.at[0], rsem.at[R_BAND + j])

    pair_send(0)

    def anomalies(j):
        raw = ab[j]
        return raw - jnp.sum(raw, axis=0, keepdims=True) / members

    anom_t = anomalies(REACH).T
    th, tl = halves(anom_t)
    both_t = jnp.concatenate([th, tl], axis=0)
    own_plane = jnp.broadcast_to(plane_row, (odev, odev)).T
    own_var = jnp.broadcast_to(var[...], (odev, odev)).T
    diagonal = (lax.broadcasted_iota(jnp.int32, (odev, odev), 0) == lax.broadcasted_iota(jnp.int32, (odev, odev), 1))
    diag_var = jnp.where(diagonal, own_var, 0.0)

    def taper(a, b):
        spread = jnp.abs(a - b)
        spread = jnp.minimum(spread, planes - spread)
        return jnp.maximum(0.0, 1.0 - spread / LOC)

    def rows_of(j, place, total, more=None):
        lanes = pl.ds(pl.multiple_of(place * odev, odev), odev)
        high, low = halves(anomalies(j))
        ah[:, lanes] = high
        al[:, lanes] = low
        gram = nn(both_t, high)
        gram = gram[:odev] + gram[odev:] + nn(th, low)
        block = taper(own_plane, e0[place, pl.ds(mdev, 1), :]) * gram / (members - 1)
        if more is not None:
            block = block + more
        chigh, clow = halves(block)
        ch[:, lanes] = chigh
        cl[:, lanes] = clow
        return total + jnp.abs(block)

    total = rows_of(REACH, own, jnp.zeros((odev, odev), f32), diag_var)

    def pass_on(given, chips):
        there = given - 2 * chips
        pltpu.make_async_remote_copy(
            src_ref=ab.at[given], dst_ref=ab.at[there],
            send_sem=ssem.at[S_BAND], recv_sem=rsem.at[R_BAND + there],
            device_id={"space": lax.rem(me_s + 2 * chips + space_count, space_count)}, device_id_type=MESH).start()

    my_y = lax.rem(my_c, side_y)
    first_side = jnp.where(my_y == side_y - 1, -1, 1)
    for side in (first_side, -first_side):
        slot = REACH + 2 * side
        slot_here(slot)
        pass_on(slot, -side)
        edge = my_y == jnp.where(side > 0, side_y - 1, 0)
        pass_on(jnp.where(edge, REACH, slot), jnp.where(edge, -3 * side, 4 * side))
    pair_send(2)
    pair_send(-2)
    handed(rhs_at, R_RHS)

    def pick(i, table):
        value = table[0]
        for k in range(1, len(table)):
            value = jnp.where(i == k, table[k], value)
        return value

    def place(rank, negative):
        return 2 * rank + my_h + negative - 2 * my_h * negative

    def slot_rows(e, rank, negative, total):
        return rows_of(REACH + turn * e, place(rank, negative), total)

    def partner_rows(e, rank, negative, total):
        return rows_of(REACH + turn * (1 - e), REACH + place(rank, 1 - negative), total)

    total = slot_rows(2, 2, 0, total)
    total = slot_rows(-2, 2, 1, total)

    def two_slots(i, total):
        e = pick(i, (8, 4, -4, 6, -6))
        f = pick(i, (0, 2, -2, 8, 4))
        slot_here(REACH + turn * e)
        pair_send(e)
        slot_here(REACH + turn * (1 - f))
        total = slot_rows(e, pick(i, (3, 0, 0, 1, 1)), pick(i, (0, 0, 1, 0, 1)), total)
        return partner_rows(f, pick(i, (3, 2, 2, 3, 0)), pick(i, (1, 0, 1, 0, 0)), total)

    total = lax.fori_loop(0, 1, two_slots, total)
    relayed(0)
    relay(2)
    total = lax.fori_loop(1, 5, two_slots, total)
    slot_here(REACH - turn * REACH)
    slot_here(REACH + turn * (1 + 4))
    total = slot_rows(-REACH, 3, 1, total)
    total = partner_rows(-4, 0, 1, total)
    slot_here(REACH + turn * (1 - 6))
    slot_here(REACH + turn * (1 + 6))
    total = partner_rows(6, 1, 0, total)
    total = partner_rows(-6, 1, 1, total)

    def part(block, lanes):
        high, low = halves(block)
        top = nt(jnp.concatenate([high, low], axis=0), ch[:, lanes])
        return top[:mdev] + top[mdev:] + nt(high, cl[:, lanes])

    own_lanes = slice(own * odev, (own + 1) * odev)
    lanes_out = slice(0, own * odev)

    def exchange(e, block):
        ex[e, own] = block

        def copy(there, to):
            pltpu.make_async_remote_copy(
                src_ref=ex.at[e, own], dst_ref=ex.at[e, there],
                send_sem=ssem.at[S_DIR + e], recv_sem=rsem.at[R_DIR + e],
                device_id=to, device_id_type=MESH).start()

        for i, to in enumerate(band_to):
            copy(i ^ 1, to)
            if i < REACH - 2:
                copy(REACH + (i ^ 1), {"space": lax.rem(me_s + AWAY[i] + turn + space_count, space_count)})
        copy(3 * REACH - 3 - out_of_reach,
             {"space": lax.rem(me_s - (REACH - 1) * turn + space_count, space_count)})
        copy(REACH + out_of_reach, partner)

    def arrived(e):
        awaited(ex.at[e, pl.ds(0, own)], rsem.at[R_DIR + e])
        return lambda i: ex[e, i]

    def image_of(block, values_of):
        image = part(block, own_lanes)
        values = values_of()
        for i in range(own):
            high, low = halves(values(i))
            dh[:mdev, i * odev:(i + 1) * odev] = high
            dh[mdev:, i * odev:(i + 1) * odev] = low
        top = nt(dh[...], ch[:, lanes_out])
        return image + (top[:mdev] + top[mdev:] + nt(dh[:mdev, :], cl[:, lanes_out]))

    row_max = jnp.max(jnp.sum(total, axis=1, keepdims=True), axis=0, keepdims=True)
    var_min = jnp.min(var[...], axis=1, keepdims=True)
    is_upper = lax.broadcasted_iota(jnp.int32, (8, odev), 0) < 4
    bb[me_s] = jnp.where(is_upper, row_max, -var_min)

    for to in others:
        pltpu.make_async_remote_copy(
            src_ref=bb.at[me_s], dst_ref=bb.at[me_s],
            send_sem=ssem.at[S_BOUND], recv_sem=rsem.at[R_BOUND],
            device_id={"space": to}, device_id_type=MESH).start()

    first_image = image_of(rhs, lambda: lambda i: e0[i, pl.ds(0, mdev), :])
    exchange(0, first_image)
    relayed(1)
    relay(3)
    second_image = image_of(first_image, lambda: arrived(0))

    awaited(bb.at[pl.ds(0, space_count - 1)], rsem.at[R_BOUND])
    bounds = jnp.max(bb[...], axis=0)
    upper = bounds[0:1, :]
    lower = -bounds[4:5, :]
    center = (upper + lower) / 2.0
    radius = (upper - lower) / 2.0
    sigma = center / radius
    rho = 1.0 / sigma
    direction = rhs / center
    weight = direction
    residual = rhs - first_image / center
    rho_next = 1.0 / (2.0 * sigma - rho)
    keep, take = rho_next * rho, 2.0 * rho_next / radius
    image = keep * (first_image / center) + take * (first_image - second_image / center)
    direction = keep * direction + take * residual
    rho = rho_next
    weight = weight + direction

    for e in range(1, ITERS - 2):
        residual = residual - image
        rho_next = 1.0 / (2.0 * sigma - rho)
        direction = rho_next * rho * direction + 2.0 * rho_next / radius * residual
        rho = rho_next
        weight = weight + direction
        exchange(e, direction)
        relayed(e + 1)
        relay(e + 3)
        image = image_of(direction, lambda e=e: arrived(e))
    residual = residual - image
    rho_next = 1.0 / (2.0 * sigma - rho)
    direction = rho_next * rho * direction + 2.0 * rho_next / radius * residual
    weight = weight + direction
    last = ITERS - 2
    exchange(last, weight)

    relayed(HOPS - 2)
    relayed(HOPS - 1)
    width = 512

    def split_states(i, c):
        x = lax.div(i, slab // width)
        lanes = pl.ds(pl.multiple_of(lax.rem(i, slab // width) * width, width), width)
        states = zs[x, :, lanes]
        high, low = halves(states - jnp.sum(states, axis=0, keepdims=True) / members)
        sh[x, :, lanes] = high
        sl[x, :, lanes] = low
        return c

    lax.fori_loop(0, 2 * slab // width, split_states, 0)

    base = me_s.astype(f32) * 2.0

    def gain_part(block, row, lanes):
        wide = jnp.concatenate([block * taper(base, row), block * taper(base + 1.0, row)], axis=0)
        high, low = halves(wide)
        top = nt(jnp.concatenate([high, low], axis=0), ah[:, lanes])
        return top[:2 * mdev] + top[2 * mdev:] + nt(high, al[:, lanes])

    gain = gain_part(weight, plane_row, own_lanes)
    values = arrived(last)
    for g in (slice(0, REACH), slice(REACH, own)):
        span = range(g.start, g.stop)
        rows = jnp.concatenate([e0[i, pl.ds(mdev, 1), :] for i in span], axis=1)
        block = jnp.concatenate([values(i) for i in span], axis=1)
        gain = gain + gain_part(block, rows, slice(g.start * odev, g.stop * odev))
    gain = gain / (members - 1)

    for x in range(2):
        ghigh, glow = halves(gain[x * mdev:(x + 1) * mdev])
        gboth = jnp.concatenate([ghigh, glow], axis=0)

        wide = 1024

        def update(i, c, x=x, ghigh=ghigh, gboth=gboth):
            lanes = pl.ds(pl.multiple_of(i * wide, wide), wide)
            top = nn(gboth, sh[x, :, lanes])
            out[x, :, lanes] = zs[x, mine, lanes] + (top[:mdev] + top[mdev:] + nn(ghigh, sl[x, :, lanes]))
            return c

        lax.fori_loop(0, slab // wide, update, 0)

    awaited(r.at[pl.ds(0, planes - 2)], ssem.at[S_OUT])
    awaited(fr.at[pl.ds(0, space_count - 1)], ssem.at[S_FORC])
    awaited(r.at[pl.ds(0, planes - 2)], ssem.at[S_BACK])
    awaited(ab.at[0, pl.ds(0, members - mdev)], ssem.at[S_OBS])
    awaited(e0.at[pl.ds(0, 2 * REACH)], ssem.at[S_RHS])
    awaited(ab.at[pl.ds(0, REACH)], ssem.at[S_BAND])
    awaited(ab.at[pl.ds(0, REACH)], ssem.at[S_PAIR])
    awaited(bb.at[pl.ds(0, space_count - 1)], ssem.at[S_BOUND])
    for e in range(ITERS - 1):
        awaited(ex.at[e, pl.ds(0, 2 * REACH)], ssem.at[S_DIR + e])
    for hop in range(HOPS):
        for at in (S_RIGHT, S_LEFT):
            awaited(zs.at[0, pl.ds(0, mdev), :], ssem.at[at + hop])


def shards(ensemble, forcing, obs_cell, obs_value, obs_var, obs_noise):
    mdev, pdev, slab = ensemble.shape
    odev = obs_cell.shape[0]
    space_count = lax.axis_size("space")
    mem_count = lax.axis_size("mem")
    members = mdev * mem_count
    planes = pdev * space_count
    band = SLOTS * odev

    def call(*args):
        return kernel(space_count, mem_count, *args)

    vmem = pl.BlockSpec(memory_space=pltpu.VMEM)
    analysis = pl.pallas_call(
        call,
        out_shape=jax.ShapeDtypeStruct((pdev, mdev, slab), f32),
        in_specs=[vmem] * 6,
        out_specs=vmem,
        scratch_shapes=[
            pltpu.VMEM((planes, mdev // 2, 128), f32),
            pltpu.VMEM((planes, mdev // 2, 128), f32),
            pltpu.VMEM((space_count, pdev, 128), f32),
            pltpu.VMEM((pdev, members, slab), f32),
            pltpu.VMEM((pdev, members, slab), bf16),
            pltpu.VMEM((pdev, members, slab), bf16),
            pltpu.VMEM((pdev * slab, odev), bf16),
            pltpu.VMEM((SLOTS, members, odev), f32),
            pltpu.VMEM((members, band), bf16),
            pltpu.VMEM((members, band), bf16),
            pltpu.VMEM((SLOTS, mdev + 8, odev), f32),
            pltpu.VMEM((ITERS - 1, SLOTS, mdev, odev), f32),
            pltpu.VMEM((space_count, 8, odev), f32),
            pltpu.VMEM((odev, band), bf16),
            pltpu.VMEM((odev, band), bf16),
            pltpu.VMEM((2 * mdev, 2 * REACH * odev), bf16),
            pltpu.SemaphoreType.DMA((SENDS,)),
            pltpu.SemaphoreType.DMA((RECVS,)),
            pltpu.SemaphoreType.DMA((3,)),
        ],
        compiler_params=pltpu.CompilerParams(
            collective_id=0, has_side_effects=True, vmem_limit_bytes=32 * 1024 * 1024),
        name="cycle",
    )(
        jnp.transpose(ensemble, (1, 0, 2)), forcing, obs_cell[None, :], obs_value[None, :], obs_var[None, :],
        obs_noise,
    )
    return jnp.transpose(analysis, (1, 0, 2))


def solution(mesh):
    placed = (
        P("mem", "space", None),
        P("space", None),
        P("space"),
        P("space"),
        P("space"),
        P("mem", "space"),
    )
    return jax.shard_map(
        shards, mesh=mesh, in_specs=placed, out_specs=P("mem", "space", None), check_vma=False
    )
```
